32 devices in a mesh: rows: 4 (over y, x), wide: 8 (over z, core).
Axes of the slice: x: 2, y: 2, z: 4, core: 2. Of those that a mesh axis runs over, the one named last changes fastest.
Arguments:
- tokens: bfloat16 [16, 1024, 1024], P('rows', 'wide'), may hold values from -6 to 6
- segments: int32 [16, 1024], P('rows'), may hold values from 0 to 15, never falling along the last dimension, each value on 1 to 128 neighbouring positions
- w_qkv: bfloat16 [2, 1024, 3072], replicated, may hold values from -0.1875 to 0.1875
- b_qkv: float32 [2, 3072], replicated, may hold values from -3 to 3
- w_out: bfloat16 [2, 1024, 1024], replicated, may hold values from -1 to 1
- b_out: float32 [2, 1024], replicated, may hold values from -3 to 3
- norm_gain: float32 [2, 2, 1024], replicated, may hold values from 0.5 to 1.5
- norm_bias: float32 [2, 2, 1024], replicated, may hold values from -2 to 2
- w_up: bfloat16 [2, 4096, 1024], P(None, 'wide'), may hold values from -0.1875 to 0.1875
- b_up: bfloat16 [2, 4096], P(None, 'wide'), may hold values from -3 to 3
- w_down: bfloat16 [2, 4096, 1024], P(None, 'wide'), may hold values from -0.09375 to 0.09375
- b_down: float32 [2, 1024], replicated, may hold values from -2 to 2
- prefix: bfloat16 [2, 2, 64, 1024], replicated, may hold values from -6 to 6
- cotangent: bfloat16 [16, 1024, 1024], P('rows', 'wide'), may hold values from -6 to 6
Outputs:
- output: bfloat16 [16, 1024, 1024], P('rows', 'wide')
- grad_tokens: float32 [16, 1024, 1024], P('rows', 'wide')
- grad_prefix: float32 [2, 2, 64, 1024], replicated
The draws below stay inside these ranges and needn't reach their ends.
Inputs may be any that keep to these rules, and one draw needn't show every extreme that they name: `segments`: along each row the pair ids never fall, each pair covers 1 to 128 consecutive positions, and some pair covers exactly 128.
All inputs are finite; a program needn't handle non-finite values.
Results may differ from the reference program's by a relative error of at most 0.02.
Values may be sent and summed in bfloat16 or wider, within the bound.
A program may use at most 320 MiB of HBM per device.

```python
import math
import jax
import jax.numpy as jnp
import numpy as np
from jax import lax

D = 1024
FF = 4096
HEADS = 16
PREFIX = 64
PAIR_MAX = 128
LAYERS = 2
TOK_DEV = 128
ROWS = 16
LEN = 1024
PAIRS = 16


def levels(stream_key, shape, cuts, low, top_value):
    level = 1.0
    for axis_at, blocks in cuts:
        heights = jax.random.uniform(jax.random.fold_in(jax.random.fold_in(stream_key, 6), axis_at), (blocks,), jnp.float32, low / len(cuts), top_value / len(cuts))
        level = level * jnp.repeat(jnp.exp(heights), shape[axis_at] // blocks).reshape((-1,) + (1,) * (len(shape) - 1 - axis_at))
    return level


def profile(count, total, bound, lean):
    weights = [(1 << 20) // math.isqrt(standing ** lean) + 1 for standing in range(2, count + 1)]
    spare, counts = total - bound - (count - 1), [1] * (count - 1)
    while spare > 0:
        candidates = [i for i in range(count - 1) if counts[i] < bound]
        mass, remaining = sum([weights[i] for i in candidates]), spare
        for i in candidates:
            extra = min(bound - counts[i], max(1, remaining * weights[i] // mass), spare)
            counts[i] = counts[i] + extra
            spare = spare - extra
    return np.array([bound] + counts)


def ragged(own_key, count, total, most, lean):
    if count == 2:
        one = jax.random.randint(own_key, (), max(1, total - most), min(most, total - 1) + 1)
        return jnp.stack([one, total - one])
    lengths = jnp.asarray(profile(count, total, most, lean), jnp.int32)
    twos = (count - 1) // 2
    donor, sink = lengths[1:1 + 2 * twos:2], lengths[2:2 + 2 * twos:2]
    room = jnp.minimum(donor - 1, most - sink)
    passed = jax.random.randint(jax.random.fold_in(own_key, 1), (twos,), 0, 1 << 20) % (room + 1)
    lengths = lengths.at[1:1 + 2 * twos:2].set(donor - passed).at[2:2 + 2 * twos:2].set(sink + passed)
    return lengths[jax.random.permutation(jax.random.fold_in(own_key, 2), count)]


def noise(stream_key, dims, scale, limit, split=(), kind=jnp.bfloat16):
    level = levels(stream_key, dims, split, -0.22, 0.18) if split else 1.0
    values = jax.random.normal(stream_key, dims, jnp.float32) * scale * level
    return jnp.minimum(jnp.maximum(values, -limit), limit).astype(kind)


def setup_inputs(seed: int = 0) -> dict:
    seeds = jax.random.split(jax.random.key(seed), 15)
    return {
        "tokens": noise(seeds[0], (ROWS, LEN, D), 1.0, 6.0, ((0, 4), (1, 8))),
        "segments": jax.vmap(lambda own: jnp.searchsorted(jnp.cumsum(ragged(own, PAIRS, LEN, PAIR_MAX, 2)), jnp.arange(LEN), side="right"))(jax.random.split(seeds[1], ROWS)).reshape((ROWS, LEN)).astype(jnp.int32),
        "w_qkv": noise(seeds[2], (LAYERS, D, 3 * D), D ** -0.5, 0.1875),
        "b_qkv": noise(seeds[3], (LAYERS, 3 * D), 0.5, 3.0, (), jnp.float32),
        "w_out": noise(seeds[4], (LAYERS, D, D), (D // 32) ** -0.5, 1.0),
        "b_out": noise(seeds[5], (LAYERS, D), 0.5, 3.0, (), jnp.float32),
        "norm_gain": jnp.clip(1.0 + 0.1 * jax.random.normal(seeds[6], (LAYERS, 2, D), jnp.float32), 0.5, 1.5),
        "norm_bias": noise(seeds[7], (LAYERS, 2, D), 0.3, 2.0, (), jnp.float32),
        "w_up": noise(seeds[8], (LAYERS, FF, D), D ** -0.5, 0.1875, ((1, 8),)),
        "b_up": noise(seeds[9], (LAYERS, FF), 0.5, 3.0, ((1, 8),)),
        "w_down": noise(seeds[10], (LAYERS, FF, D), FF ** -0.5, 0.09375, ((1, 8),)),
        "b_down": noise(seeds[11], (LAYERS, D), 0.3, 2.0, (), jnp.float32),
        "prefix": noise(seeds[12], (LAYERS, 2, PREFIX, D), 1.0, 6.0),
        "cotangent": noise(seeds[13], (ROWS, LEN, D), 1.0, 6.0, ((0, 4), (1, 8))),
    }


@jax.custom_vjp
def low(v):
    return lax.optimization_barrier(v.astype(jnp.bfloat16)).astype(jnp.float32)

@jax.custom_vjp
def low_back(v):
    return v

def low_keep(v):
    return (low(v), None)

def low_pass(kept, grad):
    return (grad,)

def back_keep(v):
    return (v, None)

def back_low(kept, grad):
    return (low(grad),)
low.defvjp(low_keep, low_pass)
low_back.defvjp(back_keep, back_low)
precise = lax.Precision.HIGHEST

def normalize(values, gain, shift):
    center = values - lax.optimization_barrier(jnp.mean(values, axis=-1, keepdims=True))
    spread = lax.optimization_barrier(jnp.mean(center * center, axis=-1, keepdims=True))
    return center * lax.rsqrt(spread + 1e-05) * gain + shift

def gelu_exact(values):
    return jax.nn.gelu(values, approximate=False)

def attend_block(query_rows, key_rows, value_rows, prefix_keys, prefix_values, query_ids, key_ids):
    head_size = query_rows.shape[1] // HEADS
    block_rows = query_rows.shape[0]
    all_keys = jnp.concatenate([prefix_keys, key_rows], 0).reshape(-1, HEADS, head_size)
    all_values = jnp.concatenate([prefix_values, value_rows], 0).reshape(-1, HEADS, head_size)
    queries = query_rows.reshape(block_rows, HEADS, head_size)
    scores = jnp.einsum('qhe,khe->hkq', queries, all_keys, precision=precise) * (1.0 / math.sqrt(head_size))
    scores = low_back(scores)
    visible = jnp.concatenate([jnp.ones((prefix_keys.shape[0], block_rows), dtype=bool), key_ids[:, None] == query_ids[None, :]], 0)
    scores = jnp.where(visible[None], scores, -1e+30)
    top_score = lax.optimization_barrier(jnp.max(scores, axis=1, keepdims=True))
    exp_scores = jnp.exp(scores - top_score)
    probs = low(exp_scores / lax.optimization_barrier(jnp.sum(exp_scores, axis=1, keepdims=True)))
    context = jnp.einsum('hkq,khe->qhe', probs, all_values, precision=precise)
    return context.reshape(block_rows, -1)

def one_layer(hidden, prefix_pair, seg_ids, layer_weights):
    wq_all, bq_all, wo_mat, bo_vec, gains, shifts, wu_mat, bu_vec, wd_mat, bd_vec = layer_weights
    length, model_width = hidden.shape
    rim_rows = PAIR_MAX
    block_rows = TOK_DEV
    span = block_rows + 2 * rim_rows
    qkv_all = low(low_back(jnp.dot(low(hidden), wq_all, precision=precise) + bq_all))
    queries = qkv_all[:, :model_width]
    keys_pad = jnp.pad(qkv_all[:, model_width:2 * model_width], ((rim_rows, rim_rows), (0, 0)))
    values_pad = jnp.pad(qkv_all[:, 2 * model_width:], ((rim_rows, rim_rows), (0, 0)))
    ids_pad = jnp.pad(seg_ids, (rim_rows, rim_rows), constant_values=-1)

    def per_block(block_index):
        offset = block_index * block_rows
        return attend_block(lax.dynamic_slice_in_dim(queries, offset, block_rows, 0), lax.dynamic_slice_in_dim(keys_pad, offset, span, 0), lax.dynamic_slice_in_dim(values_pad, offset, span, 0), prefix_pair[0], prefix_pair[1], lax.dynamic_slice_in_dim(seg_ids, offset, block_rows, 0), lax.dynamic_slice_in_dim(ids_pad, offset, span, 0))
    context = lax.map(jax.checkpoint(per_block), jnp.arange(length // block_rows, dtype=jnp.int32))
    context = low(low_back(context.reshape(length, model_width)))
    attention = low_back(jnp.dot(context, wo_mat, precision=precise) + bo_vec)
    normed = normalize(hidden + attention, gains[0], shifts[0])
    pre_act = low_back(jnp.dot(low(normed), wu_mat.T, precision=precise) + bu_vec)
    act_low = low(gelu_exact(pre_act))
    ffn_out = low_back(jnp.dot(act_low, wd_mat, precision=precise) + bd_vec)
    return normalize(normed + ffn_out, gains[1], shifts[1])

def reference(tokens, segments, w_qkv, b_qkv, w_out, b_out, norm_gain, norm_bias, w_up, b_up, w_down, b_down, prefix, cotangent):
    weights = (w_qkv.astype(jnp.float32), b_qkv, w_out.astype(jnp.float32), b_out, norm_gain, norm_bias, w_up.astype(jnp.float32), b_up.astype(jnp.float32), w_down.astype(jnp.float32), b_down)

    def forward(sequence, prefix_vals, seg_ids):
        for layer_index in range(LAYERS):
            sequence = one_layer(sequence, prefix_vals[layer_index], seg_ids, [member[layer_index] for member in weights])
        return sequence

    def per_row(grad_total, inputs):
        sequence, seg_ids, cot_row = inputs
        result, pullback = jax.vjp(lambda first_arg, second_arg: forward(first_arg, second_arg, seg_ids), sequence.astype(jnp.float32), prefix.astype(jnp.float32))
        grad_row, grad_pref = pullback(cot_row.astype(jnp.float32))
        return (grad_total + grad_pref, (result.astype(jnp.bfloat16), grad_row))
    grad_total, (outputs, grads) = lax.scan(per_row, jnp.zeros(prefix.shape, jnp.float32), (tokens, segments, cotangent))
    return (outputs, grads, grad_total)
```

```python
import math

import jax
import jax.numpy as jnp
from jax import lax
from jax.experimental import pallas as pl
from jax.experimental.pallas import tpu as pltpu
from jax.sharding import PartitionSpec as P

HEADS = 16
PAIR_MAX = 128
LAYERS = 2


def extended(block, sides, width):
    for axis, dim in sides:
        count = lax.axis_size(axis)
        forward = [(i, i + 1) for i in range(count - 1)]
        backward = [(target, source) for source, target in forward]
        low = lax.ppermute(
            lax.slice_in_dim(block, block.shape[dim] - width, None, axis=dim), axis, forward
        )
        high = lax.ppermute(lax.slice_in_dim(block, 0, width, axis=dim), axis, backward)
        block = jnp.concatenate([low, block, high], axis=dim)
    return block


def normalize(values, gain, shift):
    center = values - jnp.mean(values, axis=-1, keepdims=True)
    spread = jnp.mean(center * center, axis=-1, keepdims=True)
    return center * lax.rsqrt(spread + 1e-05) * gain + shift


def gelu_exact(values):
    return jax.nn.gelu(values, approximate=False)


def gelu_back(pre_values, grad_values):
    return jax.vjp(gelu_exact, pre_values)[1](grad_values)[0]


def norm_grad(values, gain, shift, grad_values):
    return jax.vjp(lambda inner: normalize(inner, gain, shift), values)[1](grad_values)[0]


def multiply(left, right):
    return jnp.dot(left, right, preferred_element_type=jnp.float32)


def multiply_back(left, right):
    return lax.dot_general(
        left, right, (((1,), (1,)), ((), ())), preferred_element_type=jnp.float32
    )


MESH = pl.DeviceIdType.MESH


class Gather:
    def __init__(self, shards, full, sems):
        self.shards = shards
        self.full = full
        self.send_sem, self.zs, self.xs, self.ys, self.ds, self.cz, self.cx, self.cy, self.cd, self.cown, self.own = sems
        self.row = lax.axis_index("rows")
        wide = lax.axis_index("wide")
        self.z, self.core = lax.div(wide, 2), lax.rem(wide, 2)
        self.shard_rows = shards[0].shape[1]
        self.unit_rows = self.shard_rows // 4
        self.row_x = self.row + 1 - 2 * lax.rem(self.row, 2)
        self.row_y = lax.rem(self.row + 2, 4)
        self.row_d = 3 - self.row

    def peer(self, kind):
        wide = self.z * 2 + self.core
        if kind == "x":
            return (self.row_x, wide)
        if kind == "y":
            return (self.row_y, wide)
        if kind == "core":
            return (self.row, self.z * 2 + 1 - self.core)
        if kind == "right":
            return (self.row, wide + 2)
        return (self.row, wide - 2)

    def unit(self, layer, member, z, core, quarter):
        start = (z * 2 + core) * self.shard_rows + quarter * self.unit_rows
        return self.full.at[layer, member, pl.ds(pl.multiple_of(start, self.unit_rows), self.unit_rows)]

    def shard(self, layer, member, z, core):
        start = (z * 2 + core) * self.shard_rows
        return self.full.at[layer, member, pl.ds(pl.multiple_of(start, self.shard_rows), self.shard_rows)]

    def barrier(self):
        sem = pltpu.get_barrier_semaphore()
        for kind in ("x", "y", "core"):
            pl.semaphore_signal(sem, inc=1, device_id=self.peer(kind), device_id_type=MESH)

        @pl.when(self.z < 3)
        def _():
            pl.semaphore_signal(sem, inc=1, device_id=self.peer("right"), device_id_type=MESH)

        @pl.when(self.z > 0)
        def _():
            pl.semaphore_signal(sem, inc=1, device_id=self.peer("left"), device_id_type=MESH)

        pl.semaphore_wait(sem, 3 + jnp.minimum(self.z, 1) + jnp.minimum(3 - self.z, 1))

    def copy(self, src, dst, recv, kind):
        return pltpu.make_async_remote_copy(
            src_ref=src, dst_ref=dst, send_sem=self.send_sem, recv_sem=recv,
            device_id=self.peer(kind), device_id_type=MESH,
        )

    def start(self, layer):
        for member in range(2):
            shard = self.shards[member].at[layer]
            mine = shard.at[pl.ds(pl.multiple_of(self.row * self.unit_rows, self.unit_rows), self.unit_rows)]
            here = self.unit(layer, member, self.z, self.core, self.row)

            @pl.when(self.z < 3)
            def _():
                self.copy(mine, here, self.zs.at[layer, member, 0, 0], "right").start()

            @pl.when(self.z > 0)
            def _():
                self.copy(mine, here, self.zs.at[layer, member, 0, 1], "left").start()

        for member in range(2):
            shard = self.shards[member].at[layer]
            place = self.shard(layer, member, self.z, self.core)
            pltpu.make_async_copy(shard, place, self.own.at[layer, member]).start()
            self.copy(shard, place, self.cown.at[layer, member], "core").start()

    def slots(self, body):
        for step in range(3):
            for side in range(2):
                origin = self.z - 1 - step if side == 0 else self.z + 1 + step
                inside = origin >= 0 if side == 0 else origin < 4

                @pl.when(inside)
                def _():
                    body(step, side, origin)

    def on_z(self, layer, step, side, origin):
        for member in range(2):
            unit = self.unit(layer, member, origin, self.core, self.row)
            self.copy(unit, unit, self.zs.at[layer, member, step, side], "x").wait_recv()
            if step < 2:
                more = self.z < 3 if side == 0 else self.z > 0

                @pl.when(more)
                def _():
                    self.copy(unit, unit, self.zs.at[layer, member, step + 1, side], "right" if side == 0 else "left").start()

            self.copy(unit, unit, self.xs.at[layer, member, step, side], "x").start()
            self.copy(unit, unit, self.ys.at[layer, member, step, side], "y").start()
            self.copy(unit, unit, self.cz.at[layer, member, step, side], "core").start()

    def on_xy(self, layer, step, side, origin):
        for member in range(2):
            unit = self.unit(layer, member, origin, self.core, self.row_x)
            self.copy(unit, unit, self.xs.at[layer, member, step, side], "x").wait_recv()
            if member == 0:
                self.copy(unit, unit, self.ds.at[layer, member, step, side], "y").start()
            self.copy(unit, unit, self.cx.at[layer, member, step, side], "core").start()
            unit = self.unit(layer, member, origin, self.core, self.row_y)
            self.copy(unit, unit, self.ys.at[layer, member, step, side], "y").wait_recv()
            if member == 1:
                self.copy(unit, unit, self.ds.at[layer, member, step, side], "x").start()
            self.copy(unit, unit, self.cy.at[layer, member, step, side], "core").start()

    def on_d(self, layer, step, side, origin):
        for member in range(2):
            unit = self.unit(layer, member, origin, self.core, self.row_d)
            self.copy(unit, unit, self.ds.at[layer, member, step, side], "x").wait_recv()
            self.copy(unit, unit, self.cd.at[layer, member, step, side], "core").start()

    def on_core(self, layer, step, side, origin):
        for member in range(2):
            for sem, quarter in ((self.cz, self.row), (self.cx, self.row_x), (self.cy, self.row_y), (self.cd, self.row_d)):
                unit = self.unit(layer, member, origin, 1 - self.core, quarter)
                self.copy(unit, unit, sem.at[layer, member, step, side], "core").wait_recv()

    def on_own(self, layer):
        for member in range(2):
            place = self.shard(layer, member, self.z, self.core)
            pltpu.make_async_copy(self.shards[member].at[layer], place, self.own.at[layer, member]).wait()
            place = self.shard(layer, member, self.z, 1 - self.core)
            self.copy(place, place, self.cown.at[layer, member], "core").wait_recv()

    def drain(self, layer):
        def wait(units):
            span = self.full.at[layer, 0, pl.ds(0, units * self.unit_rows)]
            self.copy(span, span, self.own.at[layer, 0], "core").wait_send()

        for member in range(2):
            wait(4)
            @pl.when(self.z < 3)
            def _():
                wait(1)
            @pl.when(self.z > 0)
            def _():
                wait(1)

        def slot(step, side, origin):
            if step < 2:
                more = self.z < 3 if side == 0 else self.z > 0
                @pl.when(more)
                def _():
                    wait(2)
            wait(2 * 3 + 2 * 2 + 2 + 2)

        self.slots(slot)


GATHER_SEMS = (
    [pltpu.SemaphoreType.DMA] + [pltpu.SemaphoreType.DMA((2, 2, 3, 2))] * 8 + [pltpu.SemaphoreType.DMA((2, 2))] * 2
)


def gather_kernel(up_ref, down_ref, out_ref, full, out_sem, *sems):
    g = Gather((up_ref, down_ref), full, sems)
    g.barrier()
    layers = up_ref.shape[0]
    for layer in range(layers):
        g.start(layer)
    for layer in range(layers):
        g.slots(lambda step, side, origin: g.on_z(layer, step, side, origin))
        g.slots(lambda step, side, origin: g.on_xy(layer, step, side, origin))
        g.slots(lambda step, side, origin: g.on_d(layer, step, side, origin))
        g.on_own(layer)
        g.slots(lambda step, side, origin: g.on_core(layer, step, side, origin))
        pltpu.make_async_copy(full.at[layer], out_ref.at[layer], out_sem.at[layer]).start()
        g.drain(layer)
    for layer in range(layers):
        pltpu.make_async_copy(full.at[layer], out_ref.at[layer], out_sem.at[layer]).wait()


def gathered(w_up, w_down):
    layers, rows, width = w_up.shape
    count = lax.axis_size("wide")
    if count != 8 or lax.axis_size("rows") != 4:
        both = [lax.all_gather(w, "wide", axis=1, tiled=True) for w in (w_up, w_down)]
        return jnp.stack(both, axis=1)
    return pl.pallas_call(
        gather_kernel,
        out_shape=jax.ShapeDtypeStruct((layers, 2, count * rows, width), w_up.dtype),
        in_specs=[pl.BlockSpec(memory_space=pl.ANY)] * 2,
        out_specs=pl.BlockSpec(memory_space=pl.ANY),
        scratch_shapes=[pltpu.VMEM((layers, 2, count * rows, width), w_up.dtype), pltpu.SemaphoreType.DMA((2,))] + GATHER_SEMS,
        compiler_params=pltpu.CompilerParams(collective_id=0, has_side_effects=True, vmem_limit_bytes=48 << 20),
    )(w_up, w_down)


def local(
    tokens,
    segments,
    w_qkv,
    b_qkv,
    w_out,
    b_out,
    norm_gain,
    norm_bias,
    w_up,
    b_up,
    w_down,
    b_down,
    prefix,
    cotangent,
):
    seqs_here, tok_here, model_width = tokens.shape
    rows_here = seqs_here * tok_here
    head_count = HEADS
    head_size = model_width // head_count
    score_scale = 1.0 / math.sqrt(head_size)
    rim_rows = PAIR_MAX
    prefix_len = prefix.shape[2]
    position = lax.axis_index("wide") * tok_here
    padded_ids = jnp.pad(segments, ((0, 0), (rim_rows, rim_rows)), constant_values=-1)
    query_ids = lax.dynamic_slice_in_dim(segments, position, tok_here, 1)
    window_ids = lax.dynamic_slice_in_dim(padded_ids, position, tok_here + 2 * rim_rows, 1)
    prefix_mask = jnp.ones((seqs_here, prefix_len, tok_here), dtype=bool)
    visible = jnp.concatenate(
        [prefix_mask, window_ids[:, :, None] == query_ids[:, None, :]], axis=1
    )[:, None]

    def split_heads(values):
        return values.reshape(seqs_here, values.shape[1], head_count, head_size)

    def with_prefix(layer_index, member, window_part):
        fixed_rows = jnp.broadcast_to(
            prefix[layer_index, member][None], (seqs_here, prefix_len, model_width)
        )
        return split_heads(jnp.concatenate([fixed_rows, window_part], axis=1))

    def score_block(queries, key_all):
        scores = (
            jnp.einsum("sqhe,skhe->shkq", queries, key_all, preferred_element_type=jnp.float32)
            * score_scale
        )
        return jnp.where(visible, scores, -1e30)

    hidden = tokens.astype(jnp.float32).reshape(rows_here, model_width)
    stored = []
    both = gathered(w_up, w_down)
    bias_all = lax.all_gather(b_up, "wide", axis=1, tiled=True)
    for layer_index in range(LAYERS):
        qkv_all = multiply(hidden.astype(jnp.bfloat16), w_qkv[layer_index]) + b_qkv[layer_index]
        qkv_low = qkv_all.astype(jnp.bfloat16).reshape(seqs_here, tok_here, 3 * model_width)
        queries = split_heads(qkv_low[:, :, :model_width])
        window = extended(qkv_low[:, :, model_width:], (("wide", 1),), rim_rows)
        key_all = with_prefix(layer_index, 0, window[:, :, :model_width])
        value_all = with_prefix(layer_index, 1, window[:, :, model_width:])
        scores = score_block(queries, key_all)
        top_score = jnp.max(scores, axis=2, keepdims=True)
        exp_scores = jnp.exp(scores - top_score)
        denominator = jnp.sum(exp_scores, axis=2, keepdims=True)
        probs_low = (exp_scores / denominator).astype(jnp.bfloat16)
        log_total = top_score + jnp.log(denominator)
        context = jnp.einsum(
            "shkq,skhe->sqhe", probs_low, value_all, preferred_element_type=jnp.float32
        )
        context_low = context.astype(jnp.bfloat16).reshape(rows_here, model_width)
        attention = multiply(context_low, w_out[layer_index]) + b_out[layer_index]
        pre_norm = hidden + attention
        normed = normalize(pre_norm, norm_gain[layer_index, 0], norm_bias[layer_index, 0])
        normed_low = normed.astype(jnp.bfloat16)
        up_rows, down_rows, bias_rows = both[layer_index, 0], both[layer_index, 1], bias_all[layer_index]
        pre_rows = multiply_back(normed_low, up_rows) + bias_rows.astype(jnp.float32)
        ffn_out = multiply(gelu_exact(pre_rows).astype(jnp.bfloat16), down_rows)
        kept_ffn = ()
        second_in = normed + ffn_out + b_down[layer_index]
        stored.append(
            (queries, key_all, value_all, log_total, pre_norm, normed_low, second_in, kept_ffn)
        )
        hidden = normalize(second_in, norm_gain[layer_index, 1], norm_bias[layer_index, 1])
    output = hidden.astype(jnp.bfloat16).reshape(seqs_here, tok_here, model_width)
    grad_hidden = cotangent.astype(jnp.float32).reshape(rows_here, model_width)
    prefix_grads = [None] * LAYERS
    for layer_index in reversed(range(LAYERS)):
        queries, key_all, value_all, log_total, pre_norm, normed_low, second_in, kept_ffn = stored[
            layer_index
        ]
        grad_sum2 = norm_grad(
            second_in, norm_gain[layer_index, 1], norm_bias[layer_index, 1], grad_hidden
        )
        grad_ffn_low = grad_sum2.astype(jnp.bfloat16)
        back_up_rows, back_down_rows, back_bias_rows = both[layer_index, 0], both[layer_index, 1], bias_all[layer_index]
        back_pre_rows = multiply_back(normed_low, back_up_rows) + back_bias_rows.astype(jnp.float32)
        grad_rows = gelu_back(back_pre_rows, multiply_back(grad_ffn_low, back_down_rows)).astype(
            jnp.bfloat16
        )
        grad_from_ffn = multiply(grad_rows, back_up_rows)
        grad_normed = grad_sum2 + grad_from_ffn
        grad_sum1 = norm_grad(
            pre_norm, norm_gain[layer_index, 0], norm_bias[layer_index, 0], grad_normed
        )
        grad_attn_low = grad_sum1.astype(jnp.bfloat16)
        grad_context = multiply_back(grad_attn_low, w_out[layer_index]).astype(jnp.bfloat16)
        grad_context = split_heads(grad_context.reshape(seqs_here, tok_here, model_width))
        scores = score_block(queries, key_all)
        probs = jnp.exp(scores - log_total)
        probs_low = probs.astype(jnp.bfloat16)
        grad_probs = jnp.einsum(
            "sqhe,skhe->shkq", grad_context, value_all, preferred_element_type=jnp.float32
        )
        row_dot = jnp.sum(probs * grad_probs, axis=2, keepdims=True)
        grad_scores = (probs * (grad_probs - row_dot)).astype(jnp.bfloat16)
        grad_queries = (
            jnp.einsum("shkq,skhe->sqhe", grad_scores, key_all, preferred_element_type=jnp.float32)
            * score_scale
        )
        grad_keys = (
            jnp.einsum("shkq,sqhe->skhe", grad_scores, queries, preferred_element_type=jnp.float32)
            * score_scale
        )
        grad_values = jnp.einsum(
            "shkq,sqhe->skhe", probs_low, grad_context, preferred_element_type=jnp.float32
        )
        key_count = grad_keys.shape[1]
        grad_keys = grad_keys.reshape(seqs_here, key_count, model_width)
        grad_values = grad_values.reshape(seqs_here, key_count, model_width)
        prefix_grads[layer_index] = jnp.stack(
            [
                jnp.sum(grad_keys[:, :prefix_len], axis=0),
                jnp.sum(grad_values[:, :prefix_len], axis=0),
            ],
            axis=0,
        )
        grad_window = jnp.concatenate(
            [grad_keys[:, prefix_len:], grad_values[:, prefix_len:]], axis=2
        )
        grad_kv = grad_window[:, rim_rows : rim_rows + tok_here]
        rim_grads = jnp.concatenate(
            [grad_window[:, :rim_rows], grad_window[:, rim_rows + tok_here :]], axis=1
        )
        returned = extended(rim_grads.astype(jnp.bfloat16), (("wide", 1),), rim_rows).astype(
            rim_grads.dtype
        )
        grad_kv = grad_kv + returned[:, :rim_rows]
        grad_kv = grad_kv + returned[:, 3 * rim_rows :]
        grad_qkv = jnp.concatenate(
            [grad_queries.reshape(seqs_here, tok_here, model_width), grad_kv], axis=2
        )
        grad_qkv = grad_qkv.astype(jnp.bfloat16).reshape(rows_here, 3 * model_width)
        grad_hidden = grad_sum1 + multiply_back(grad_qkv, w_qkv[layer_index])
    grad_prefix = lax.psum(jnp.stack(prefix_grads, axis=0), ("rows", "wide"))
    return (output, grad_hidden.reshape(seqs_here, tok_here, model_width), grad_prefix)


def solution(mesh):
    return jax.shard_map(
        local,
        mesh=mesh,
        in_specs=(
            P("rows", "wide", None),
            P("rows", None),
            P(),
            P(),
            P(),
            P(),
            P(),
            P(),
            P(None, "wide", None),
            P(None, "wide"),
            P(None, "wide", None),
            P(),
            P(),
            P("rows", "wide", None),
        ),
        out_specs=(P("rows", "wide", None), P("rows", "wide", None), P()),
        check_vma=False,
    )
```

```python
import functools
import math

import jax
import jax.numpy as jnp
from jax import lax
from jax.experimental import pallas as pl
from jax.experimental.pallas import tpu as pltpu
from jax.sharding import PartitionSpec as P

HEADS = 16
PAIR_MAX = 128
MESH = pl.DeviceIdType.MESH
LANES = 128
SPAN = 1024
ROOT_HALF = math.sqrt(0.5)


def multiply(left, right):
    return jnp.dot(left, right, preferred_element_type=jnp.float32)


def multiply_back(left, right):
    return lax.dot_general(left, right, (((1,), (1,)), ((), ())), preferred_element_type=jnp.float32)


def multiply_first(left, right):
    return lax.dot_general(left, right, (((0,), (0,)), ((), ())), preferred_element_type=jnp.float32)


def two_heads(rows):
    half = rows.shape[1] // 2
    lane = lax.broadcasted_iota(jnp.int32, rows.shape, 1)
    nothing = jnp.zeros_like(rows)
    return jnp.concatenate([jnp.where(lane < half, rows, nothing), jnp.where(lane >= half, rows, nothing)], axis=0)


def own_heads(columns):
    half, count = columns.shape[0] // 2, columns.shape[1] // 2
    place = lax.broadcasted_iota(jnp.int32, (columns.shape[0], count), 0)
    return jnp.where(place < half, columns[:, :count], columns[:, count:]).T


def attend(blocks, rows, rim, pair, q_ref, k_ref, v_ref, prefix_ref, hide_ref, context_ref, lse_ref):
    lanes = pl.ds(pl.multiple_of(pair * 128, 128), 128)
    prefix_keys, prefix_values = prefix_ref[0, :, lanes], prefix_ref[1, :, lanes]
    for block in range(blocks):
        here = pl.ds(block * rows, rows)
        window = pl.ds(block * rows, rows + 2 * rim)
        queries = two_heads(q_ref[here, lanes])
        hide = hide_ref[block]
        fixed = multiply_back(prefix_keys, queries)
        near = multiply_back(k_ref[window, lanes], queries) + jnp.concatenate([hide, hide], axis=1)
        top = jnp.maximum(jnp.max(fixed, axis=0, keepdims=True), jnp.max(near, axis=0, keepdims=True))
        fixed, near = jnp.exp(fixed - top), jnp.exp(near - top)
        total = jnp.sum(fixed, axis=0, keepdims=True) + jnp.sum(near, axis=0, keepdims=True)
        share = 1.0 / total
        columns = multiply_first(prefix_values, fixed.astype(jnp.bfloat16)) + multiply_first(
            v_ref[window, lanes], near.astype(jnp.bfloat16)
        )
        context_ref[here, lanes] = own_heads(columns * share).astype(jnp.bfloat16)
        lse_ref[pair * blocks + block] = top + jnp.log(total)


def attend_back(blocks, rows, rim, pair, q_ref, k_ref, v_ref, prefix_ref, hide_ref, lse_ref, grad_ref, dq_ref, dk_ref, dv_ref, dp_ref, scale):
    lanes = pl.ds(pl.multiple_of(pair * 128, 128), 128)
    prefix_keys, prefix_values = prefix_ref[0, :, lanes], prefix_ref[1, :, lanes]
    for block in range(blocks):
        here = pl.ds(block * rows, rows)
        window = pl.ds(block * rows, rows + 2 * rim)
        queries = two_heads(q_ref[here, lanes])
        grads = two_heads(grad_ref[here, lanes])
        hide = hide_ref[block]
        keys, values = k_ref[window, lanes], v_ref[window, lanes]
        lse = lse_ref[pair * blocks + block]
        fixed = jnp.exp(multiply_back(prefix_keys, queries) - lse)
        near = jnp.exp(multiply_back(keys, queries) + jnp.concatenate([hide, hide], axis=1) - lse)
        grad_fixed = multiply_back(prefix_values, grads)
        grad_near = multiply_back(values, grads)
        dots = jnp.sum(fixed * grad_fixed, axis=0, keepdims=True) + jnp.sum(near * grad_near, axis=0, keepdims=True)
        grad_fixed = (fixed * (grad_fixed - dots)).astype(jnp.bfloat16)
        grad_near = (near * (grad_near - dots)).astype(jnp.bfloat16)
        fixed, near = fixed.astype(jnp.bfloat16), near.astype(jnp.bfloat16)
        columns = multiply_first(prefix_keys, grad_fixed) + multiply_first(keys, grad_near)
        dq_ref[here, lanes] = (own_heads(columns) * scale).astype(jnp.bfloat16)
        new_keys, new_values = multiply(grad_near, queries), multiply(near, grads)
        fixed_keys, fixed_values = multiply(grad_fixed, queries), multiply(fixed, grads)
        old = pl.ds(block * rows, 2 * rim)
        fresh = pl.ds(block * rows + 2 * rim, rows)
        if block == 0:
            dk_ref[window, lanes], dv_ref[window, lanes] = new_keys, new_values
            dp_ref[0, :, lanes], dp_ref[1, :, lanes] = fixed_keys, fixed_values
        else:
            dk_ref[old, lanes] += new_keys[: 2 * rim]
            dv_ref[old, lanes] += new_values[: 2 * rim]
            dk_ref[fresh, lanes], dv_ref[fresh, lanes] = new_keys[2 * rim :], new_values[2 * rim :]
            dp_ref[0, :, lanes] += fixed_keys
            dp_ref[1, :, lanes] += fixed_values


def gelu_pair(values):
    size = jnp.abs(values) * ROOT_HALF
    bell = jnp.exp(values * values * -0.5)
    t = 1.0 / (1.0 + 0.3275911 * size)
    series = ((((1.061405429 * t - 1.453152027) * t + 1.421413741) * t - 0.284496736) * t + 0.254829592) * t
    tail = 0.5 * series * bell
    below = jnp.where(values < 0, tail, 1.0 - tail)
    return values * below, below + values * bell * (1.0 / math.sqrt(2.0 * math.pi))


def normalize(values):
    center = values - jnp.mean(values, axis=-1, keepdims=True)
    scale = lax.rsqrt(jnp.mean(center * center, axis=-1, keepdims=True) + 1e-05)
    return center * scale, scale


def norm_grad(grad, unit, scale, gain):
    inner = grad * gain
    first = jnp.mean(inner, axis=-1, keepdims=True)
    second = jnp.mean(inner * unit, axis=-1, keepdims=True)
    return scale * (inner - first - unit * second)


def each(count, step, body):
    @pl.loop(0, count)
    def _(i):
        body(pl.ds(pl.multiple_of(i * step, step), step))


class Place:
    def __init__(self, seqs, tok):
        self.seqs, self.tok, self.rows = seqs, tok, seqs * tok
        self.wide_size = lax.axis_size("wide")
        self.parts = self.wide_size // seqs
        self.row, self.wide = lax.axis_index("rows"), lax.axis_index("wide")
        self.seq, self.part = lax.div(self.wide, self.parts), lax.rem(self.wide, self.parts)

    def others(self, body):
        @pl.loop(1, self.wide_size)
        def _(step):
            body(lax.rem(self.wide + step, self.wide_size))

    def barrier(self, more):
        sem = pltpu.get_barrier_semaphore()
        self.others(lambda other: pl.semaphore_signal(sem, inc=1, device_id=(self.row, other), device_id_type=MESH))
        for row in more:
            pl.semaphore_signal(sem, inc=1, device_id=(row, self.wide), device_id_type=MESH)
        pl.semaphore_wait(sem, self.wide_size - 1 + len(more))

    def remote(self, src, dst, send, recv, device):
        return pltpu.make_async_remote_copy(
            src_ref=src, dst_ref=dst, send_sem=send, recv_sem=recv, device_id=device, device_id_type=MESH
        )

    def send_out(self, parts, target, send, recv, own):
        block = lax.rem(self.wide, self.seqs)
        for s in range(self.seqs):
            goal = s * self.parts + lax.div(self.wide, self.seqs)

            @pl.when(goal != self.wide)
            def _():
                self.remote(parts(s), target(block), send, recv.at[block], (self.row, goal)).start()

            @pl.when(goal == self.wide)
            def _():
                pltpu.make_async_copy(parts(s), target(block), own).start()

    def sent_out(self, parts, target, send, recv, own):
        block = lax.rem(self.wide, self.seqs)
        for s in range(self.seqs):
            goal = s * self.parts + lax.div(self.wide, self.seqs)

            @pl.when(goal != self.wide)
            def _():
                self.remote(parts(s), target(block), send, recv.at[block], (self.row, goal)).wait_send()

    def got_out(self, parts, target, send, recv, own):
        for b in range(self.seqs):
            source = self.part * self.seqs + b

            @pl.when(source != self.wide)
            def _():
                self.remote(parts(0), target(b), send, recv.at[b], (self.row, self.wide)).wait_recv()

            @pl.when(source == self.wide)
            def _():
                pltpu.make_async_copy(parts(0), target(b), own).wait()

    def send_home_block(self, b, part, target, send, recv, own):
        goal = self.part * self.seqs + b

        @pl.when(goal != self.wide)
        def _():
            self.remote(part, target(self.seq), send, recv.at[self.seq], (self.row, goal)).start()

        @pl.when(goal == self.wide)
        def _():
            pltpu.make_async_copy(part, target(self.seq), own).start()

    def sent_home(self, part, target, send, recv):
        for b in range(self.seqs):
            goal = self.part * self.seqs + b

            @pl.when(goal != self.wide)
            def _():
                self.remote(part, target(self.seq), send, recv.at[self.seq], (self.row, goal)).wait_send()

    def got_home(self, s, part, target, send, recv, own):
        source = s * self.parts + lax.div(self.wide, self.seqs)

        @pl.when(source != self.wide)
        def _():
            self.remote(part, target(s), send, recv.at[s], (self.row, self.wide)).wait_recv()

        @pl.when(source == self.wide)
        def _():
            pltpu.make_async_copy(part, target(s), own).wait()


class Gather:
    def __init__(self, shards, full, sems):
        self.shards = shards
        self.full = full
        self.send_sem, self.zs, self.xs, self.ys, self.ds, self.cz, self.cx, self.cy, self.cd, self.cown, self.own = sems
        self.row = lax.axis_index("rows")
        self.wide = lax.axis_index("wide")
        self.z, self.core = lax.div(self.wide, 2), lax.rem(self.wide, 2)
        self.shard_rows = shards[0].shape[1]
        self.unit_rows = self.shard_rows // 4
        self.row_x = self.row + 1 - 2 * lax.rem(self.row, 2)
        self.row_y = lax.rem(self.row + 2, 4)
        self.row_d = 3 - self.row

    def unit(self, layer, member, z, core, quarter):
        start = (z * 2 + core) * self.shard_rows + quarter * self.unit_rows
        return self.full.at[layer, member, pl.ds(pl.multiple_of(start, self.unit_rows), self.unit_rows)]

    def shard(self, layer, member, z, core):
        start = (z * 2 + core) * self.shard_rows
        return self.full.at[layer, member, pl.ds(pl.multiple_of(start, self.shard_rows), self.shard_rows)]

    def copy(self, src, dst, recv, kind):
        if kind == "x":
            device = (self.row_x, self.wide)
        elif kind == "y":
            device = (self.row_y, self.wide)
        elif kind == "core":
            device = (self.row, self.z * 2 + 1 - self.core)
        else:
            device = (self.row, self.wide + 2 - 4 * kind)
        return pltpu.make_async_remote_copy(
            src_ref=src, dst_ref=dst, send_sem=self.send_sem, recv_sem=recv, device_id=device, device_id_type=MESH
        )

    def start_z(self, layer):
        for member in range(2):
            start = pl.multiple_of(self.row * self.unit_rows, self.unit_rows)
            mine = self.shards[member].at[layer, pl.ds(start, self.unit_rows)]
            here = self.unit(layer, member, self.z, self.core, self.row)

            @pl.when(self.z < 3)
            def _():
                self.copy(mine, here, self.zs.at[layer, member, 0, 0], 0).start()

            @pl.when(self.z > 0)
            def _():
                self.copy(mine, here, self.zs.at[layer, member, 0, 1], 1).start()

    def start_core(self, layer):
        for member in range(2):
            place = self.shard(layer, member, self.z, self.core)
            pltpu.make_async_copy(self.shards[member].at[layer], place, self.own.at[layer, member]).start()
            self.copy(self.shards[member].at[layer], place, self.cown.at[layer, member], "core").start()

    def slot(self, i):
        near = jnp.minimum(self.z, 3 - self.z)
        far_side = 1 - lax.div(self.z, 2)
        both = jnp.minimum(lax.div(i, jnp.maximum(2 * near, 1)), 1) + (1 - jnp.minimum(near, 1))
        both = 1 - jnp.minimum(both, 1)
        step = both * lax.div(i, 2) + (1 - both) * (i - near)
        side = both * lax.rem(i, 2) + (1 - both) * far_side
        return step, side, self.z + (1 + step) * (2 * side - 1)

    def on_z(self, layer, i):
        step, side, origin = self.slot(i)
        for member in range(2):
            unit = self.unit(layer, member, origin, self.core, self.row)
            self.copy(unit, unit, self.zs.at[layer, member, step, side], "x").wait_recv()
            target = self.z + 1 - 2 * side

            @pl.when((target >= 0) & (target < 4))
            def _():
                self.copy(unit, unit, self.zs.at[layer, member, step + 1, side], side).start()

            self.copy(unit, unit, self.xs.at[layer, member, step, side], "x").start()
            self.copy(unit, unit, self.ys.at[layer, member, step, side], "y").start()
            self.copy(unit, unit, self.cz.at[layer, member, step, side], "core").start()

    def on_xy(self, layer, i):
        step, side, origin = self.slot(i)
        for member in range(2):
            unit = self.unit(layer, member, origin, self.core, self.row_x)
            self.copy(unit, unit, self.xs.at[layer, member, step, side], "x").wait_recv()
            if member == 0:
                self.copy(unit, unit, self.ds.at[layer, member, step, side], "y").start()
            self.copy(unit, unit, self.cx.at[layer, member, step, side], "core").start()
            unit = self.unit(layer, member, origin, self.core, self.row_y)
            self.copy(unit, unit, self.ys.at[layer, member, step, side], "y").wait_recv()
            if member == 1:
                self.copy(unit, unit, self.ds.at[layer, member, step, side], "x").start()
            self.copy(unit, unit, self.cy.at[layer, member, step, side], "core").start()

    def on_d(self, layer, i):
        step, side, origin = self.slot(i)
        for member in range(2):
            unit = self.unit(layer, member, origin, self.core, self.row_d)
            self.copy(unit, unit, self.ds.at[layer, member, step, side], "x").wait_recv()
            self.copy(unit, unit, self.cd.at[layer, member, step, side], "core").start()

    def on_core(self, layer, i):
        step, side, origin = self.slot(i)
        for member in range(2):
            for sem, quarter in ((self.cz, self.row), (self.cx, self.row_x), (self.cy, self.row_y), (self.cd, self.row_d)):
                unit = self.unit(layer, member, origin, 1 - self.core, quarter)
                self.copy(unit, unit, sem.at[layer, member, step, side], "core").wait_recv()

    def on_own(self, layer):
        for member in range(2):
            place = self.shard(layer, member, self.z, self.core)
            pltpu.make_async_copy(self.shards[member].at[layer], place, self.own.at[layer, member]).wait()
            place = self.shard(layer, member, self.z, 1 - self.core)
            self.copy(place, place, self.cown.at[layer, member], "core").wait_recv()

    def drain(self, layers):
        def wait(units):
            span = self.full.at[0, 0, pl.ds(0, units * self.unit_rows)]
            self.copy(span, span, self.own.at[0, 0], "core").wait_send()

        @pl.loop(0, layers)
        def _(layer):
            wait(8)

            @pl.when(self.z < 3)
            def _():
                wait(2)

            @pl.when(self.z > 0)
            def _():
                wait(2)

            @pl.loop(0, 3)
            def _(i):
                step, side, origin = self.slot(i)
                target = self.z + 1 - 2 * side

                @pl.when((target >= 0) & (target < 4))
                def _():
                    wait(2)

                wait(14)


def gather_sems(layers):
    return (
        [pltpu.SemaphoreType.DMA]
        + [pltpu.SemaphoreType.DMA((layers, 2, 3, 2))] * 8
        + [pltpu.SemaphoreType.DMA((layers, 2))] * 2
    )


def forward_kernel(
    fast, seqs, tok, rim,
    tokens, cotangent, w_qkv, w_out, w_up, w_down, full_in,
    hide, b_qkv, b_out, gains, shifts, b_up, b_down, prefix,
    y_low, cot_out, full_out, q_out, k_out, v_out, unit_out, scale_out, slope_out, lse_out,
    full, wqkv, wout, x, low, acc, q, k, v, halo, context, slope, unit1, unit2, scale1, scale2, lse, bias,
    load_sem, store_sem, slope_sem, full_sem, tok_send, tok_recv, tok_own, cot_send, cot_recv, cot_own,
    halo_send, halo_recv, bias_send, bias_recv, bias_own,
    *gather_sem,
):
    layers, width = w_qkv.shape[0], tokens.shape[2]
    place = Place(seqs, tok)
    rows = place.rows
    gather = Gather((w_up, w_down), full, gather_sem) if fast else None
    place.barrier((gather.row_x, gather.row_y) if fast else ())
    own_bias = bias.at[place.wide]

    def load(layer):
        return (
            pltpu.make_async_copy(w_qkv.at[layer], wqkv, load_sem.at[0]),
            pltpu.make_async_copy(w_out.at[layer], wout, load_sem.at[1]),
        )

    def put_bias(other):
        return place.remote(b_up, own_bias, bias_send, bias_recv.at[place.wide], (place.row, other))

    def got_bias(other):
        return place.remote(b_up, bias.at[other], bias_send, bias_recv.at[other], (place.row, other))

    if fast:
        gather.start_z(0)
        gather.start_core(0)
    else:
        pltpu.make_async_copy(full_in, full, full_sem.at[0]).start()
    for copy in load(0):
        copy.start()
    place.others(lambda other: put_bias(other).start())
    pltpu.make_async_copy(b_up, own_bias, bias_own).start()

    tok_args = (lambda s: tokens.at[s], lambda b: low.at[pl.ds(pl.multiple_of(b * tok, tok), tok)], tok_send, tok_recv, tok_own)
    cot_args = (lambda s: cotangent.at[s], lambda b: cot_out.at[pl.ds(pl.multiple_of(b * tok, tok), tok)], cot_send, cot_recv, cot_own)
    events = []
    if fast:
        gather.on_z(0, 0)
        place.send_out(*tok_args)
        gather.on_z(0, 1)
        gather.on_xy(0, 0)
        gather.start_z(1)
        gather.start_core(1)
        gather.on_z(0, 2)
        gather.on_xy(0, 1)
        events = [
            (gather.on_d, 0, 0), (gather.on_xy, 0, 2), (gather.on_z, 1, 0), (gather.on_d, 0, 1), (gather.on_d, 0, 2),
            (gather.on_z, 1, 1), (gather.on_z, 1, 2), (gather.on_xy, 1, 0),
        ]
    else:
        place.send_out(*tok_args)

    def tick(count=1):
        for _ in range(min(count, len(events))):
            event, layer, i = events.pop(0)
            event(layer, i)

    blank = jnp.zeros((rim, width), jnp.bfloat16)

    @pl.when(place.part == 0)
    def _():
        k[pl.ds(0, rim)] = blank
        v[pl.ds(0, rim)] = blank

    @pl.when(place.part == place.parts - 1)
    def _():
        k[pl.ds(rim + rows, rim)] = blank
        v[pl.ds(rim + rows, rim)] = blank

    place.got_out(*tok_args)

    def halo_copy(layer, member, side, wide):
        ref = (k, v)[member]
        return place.remote(
            ref.at[pl.ds((rows, rim)[side], rim)], halo.at[layer, member, side],
            halo_send.at[member, side], halo_recv.at[layer, member, side], (place.row, wide),
        )

    def halos(body, to):
        for side in range(2):
            @pl.when(place.part < place.parts - 1 if (side == 0) == to else place.part > 0)
            def _():
                for member in range(2):
                    body(member, side, jnp.clip(place.wide + (1 - 2 * side), 0, place.wide_size - 1))

    def got_halo(layer, member, side, wide):
        halo_copy(layer, member, side, place.wide).wait_recv()
        (k, v)[member][pl.ds((0, rim + rows)[side], rim)] = halo[layer, member, side]

    def kept(layer):
        return [
            pltpu.make_async_copy(src, dst.at[layer], store_sem.at[i])
            for i, (src, dst) in enumerate(((q, q_out), (k, k_out), (v, v_out)))
        ]

    def kept_norm(layer, which):
        unit, scale = ((unit1, scale1), (unit2, scale2))[which]
        return [
            pltpu.make_async_copy(unit, unit_out.at[layer, which], store_sem.at[3 + which]),
            pltpu.make_async_copy(scale, scale_out.at[layer, which], store_sem.at[5 + which]),
        ]

    half = width // 2
    for layer in range(layers):
        if layer > 0:
            for copy in kept(layer - 1) + kept_norm(layer - 1, 0) + kept_norm(layer - 1, 1):
                copy.wait()
        load(layer)[0].wait()
        for part in (2, 3, 4, 5, 0, 1):
            lanes = pl.ds(part * half, half)
            made = multiply(low[...], wqkv[:, lanes]) + b_qkv[layer, :, lanes]
            kind, side = part // 2, pl.ds((part % 2) * half, half)
            if kind == 0:
                q[:, side] = made.astype(jnp.bfloat16) * (1.0 / math.sqrt(width // HEADS))
            else:
                (k, v)[kind - 1][pl.ds(rim, rows), side] = made.astype(jnp.bfloat16)
            if part == 5:
                tick()
                halos(lambda *at: halo_copy(layer, *at).start(), True)
        if layer + 1 < layers:
            load(layer + 1)[0].start()
        tick()
        halos(lambda *at: got_halo(layer, *at), False)
        halos(lambda *at: halo_copy(layer, *at).wait_send(), True)
        for copy in kept(layer):
            copy.start()

        for first in (0, 4):
            @pl.loop(first, first + 4)
            def _(pair):
                attend(seqs, tok, rim, pair, q, k, v, prefix.at[layer], hide, context, lse.at[layer])

            tick()
        load(layer)[1].wait()
        for part in range(2):
            lanes = pl.ds(part * half, half)
            acc[:, lanes] = multiply(context[...], wout[:, lanes])
        if layer + 1 < layers:
            load(layer + 1)[1].start()
        tick()

        def first_norm(at):
            before = low[at].astype(jnp.float32) if layer == 0 else x[at]
            unit, scale = normalize(before + acc[at] + b_out[layer])
            unit1[at] = unit.astype(jnp.bfloat16)
            scale1[at] = jnp.broadcast_to(scale, (scale.shape[0], LANES))
            normed = unit * gains[layer, 0] + shifts[layer, 0]
            low[at] = normed.astype(jnp.bfloat16)
            acc[at] = normed + b_down[layer]

        each(rows // 64, 64, first_norm)
        for copy in kept_norm(layer, 0):
            copy.start()
        tick()
        if layer == 0:
            pltpu.make_async_copy(b_up, own_bias, bias_own).wait()
            place.others(lambda other: got_bias(other).wait_recv())

            place.others(lambda other: put_bias(other).wait_send())
            if not fast:
                pltpu.make_async_copy(full_in, full, full_sem.at[0]).wait()

        hidden = b_up.shape[1] // layers

        @pl.loop(0, full.shape[2] // SPAN)
        def _(i):
            spot = i
            if fast:
                @pl.when(i == 0)
                def _():
                    gather.on_own(layer)

                @pl.when(i > 0)
                def _():
                    if layer == 1:
                        @pl.when(i > 1)
                        def _():
                            gather.on_xy(1, i - 1)

                        gather.on_d(1, i - 1)
                    gather.on_core(layer, i - 1)

                origin = gather.slot(jnp.maximum(i - 1, 0))[2]
                started = jnp.minimum(i, 1)
                spot = started * origin + (1 - started) * gather.z
            units = pl.ds(pl.multiple_of(spot * SPAN, SPAN), SPAN)
            slot = lax.rem(i, 2)
            step_bias = jnp.concatenate(
                [bias[spot * (SPAN // hidden) + n, :, pl.ds(layer * hidden, hidden)] for n in range(SPAN // hidden)], axis=1
            )

            @pl.when(i > 1)
            def _():
                pltpu.make_async_copy(slope.at[slot], slope_out.at[layer, spot], slope_sem.at[slot]).wait()

            for part in range(2):
                at = pl.ds(part * (rows // 2), rows // 2)
                act, rise = gelu_pair(multiply_back(low[at], full[layer, 0, units]) + step_bias)
                slope[slot, at] = rise.astype(jnp.bfloat16)
                acc[at] += multiply(act.astype(jnp.bfloat16), full[layer, 1, units])
            pltpu.make_async_copy(slope.at[slot], slope_out.at[layer, spot], slope_sem.at[slot]).start()
            if fast:
                pltpu.make_async_copy(full.at[layer, :, units], full_out.at[layer, :, units], full_sem.at[layer]).start()

        for slot in range(2):
            pltpu.make_async_copy(slope.at[slot], slope_out.at[layer, 0], slope_sem.at[slot]).wait()

        def second_norm(at):
            unit, scale = normalize(acc[at])
            unit2[at] = unit.astype(jnp.bfloat16)
            scale2[at] = jnp.broadcast_to(scale, (scale.shape[0], LANES))
            after = unit * gains[layer, 1] + shifts[layer, 1]
            low[at] = after.astype(jnp.bfloat16)
            if layer + 1 < layers:
                x[at] = after

        each(rows // 64, 64, second_norm)
        for copy in kept_norm(layer, 1):
            copy.start()
        if layer == 0:
            place.send_out(*cot_args)
            tick(2)
    last = [pltpu.make_async_copy(low, y_low, store_sem.at[7]), pltpu.make_async_copy(lse, lse_out, store_sem.at[8])]
    for copy in last:
        copy.start()
    place.sent_out(*tok_args)
    place.got_out(*cot_args)
    place.sent_out(*cot_args)
    for copy in last + kept(layers - 1) + kept_norm(layers - 1, 0) + kept_norm(layers - 1, 1):
        copy.wait()
    if fast:
        gather.drain(layers)
        for layer in range(layers):
            pltpu.make_async_copy(full.at[layer], full_out.at[layer], full_sem.at[layer]).wait()


def forward(fast, tokens, cotangent, w_qkv, w_out, w_up, w_down, full_in, hide, b_qkv, b_out, gains, shifts, b_up, b_down, prefix):
    seqs, tok, width = tokens.shape
    layers, rim, rows = w_qkv.shape[0], PAIR_MAX, seqs * tok
    wides = lax.axis_size("wide")
    units = w_up.shape[1] * wides
    low, full_type = jnp.bfloat16, jnp.float32
    spans = units // SPAN
    shape = jax.ShapeDtypeStruct
    dma = pltpu.SemaphoreType.DMA
    scores = (layers, width // LANES * seqs, 1, 2 * tok)
    return pl.pallas_call(
        functools.partial(forward_kernel, fast, seqs, tok, rim),
        out_shape=(
            shape((rows, width), low), shape((rows, width), low), shape((layers, 2, units, width), low),
            shape((layers, rows, width), low), shape((layers, rows + 2 * rim, width), low),
            shape((layers, rows + 2 * rim, width), low), shape((layers, 2, rows, width), low),
            shape((layers, 2, rows, LANES), full_type), shape((layers, spans, rows, SPAN), low), shape(scores, full_type),
        ),
        in_specs=[pl.BlockSpec(memory_space=pl.ANY)] * 7 + [pl.BlockSpec(memory_space=pltpu.VMEM)] * 8,
        out_specs=(pl.BlockSpec(memory_space=pl.ANY),) * 10,
        scratch_shapes=[
            pltpu.VMEM((layers, 2, units, width), low), pltpu.VMEM(w_qkv.shape[1:], low), pltpu.VMEM(w_out.shape[1:], low),
            pltpu.VMEM((rows, width), full_type), pltpu.VMEM((rows, width), low), pltpu.VMEM((rows, width), full_type),
            pltpu.VMEM((rows, width), low), pltpu.VMEM((rows + 2 * rim, width), low), pltpu.VMEM((rows + 2 * rim, width), low),
            pltpu.VMEM((layers, 2, 2, rim, width), low), pltpu.VMEM((rows, width), low), pltpu.VMEM((2, rows, SPAN), low),
            pltpu.VMEM((rows, width), low), pltpu.VMEM((rows, width), low),
            pltpu.VMEM((rows, LANES), full_type), pltpu.VMEM((rows, LANES), full_type),
            pltpu.VMEM(scores, full_type), pltpu.VMEM((wides,) + b_up.shape, full_type),
            dma((2,)), dma((9,)), dma((2,)), dma((layers,)), dma, dma((seqs,)), dma, dma, dma((seqs,)), dma,
            dma((2, 2)), dma((layers, 2, 2)), dma, dma((wides,)), dma,
        ] + (gather_sems(layers) if fast else []),
        compiler_params=pltpu.CompilerParams(collective_id=0, has_side_effects=True, vmem_limit_bytes=67043328),
    )(tokens, cotangent, w_qkv, w_out, w_up, w_down, full_in, hide, b_qkv, b_out, gains, shifts, b_up, b_down, prefix)


def backward_kernel(
    seqs, tok, rim,
    y_low, cot_in, full, w_qkv, w_out, q_in, k_in, v_in, unit_in, scale_in, slope_in,
    lse, hide, gains, prefix,
    out, grads, prefix_grads,
    wqkv, wout, q, k, v, unit1, unit2, scale1, scale2, up, down, slope, cot, acc, low, context, made, dk, dv, edge, edge_in, home,
    load_sem, ffn_sem, out_send, out_recv, out_own, home_send, home_recv, home_own, edge_send, edge_recv, store_sem,
):
    layers, width = w_qkv.shape[0], w_qkv.shape[1]
    place = Place(seqs, tok)
    rows = place.rows
    place.barrier(())
    spans = slope_in.shape[1]

    def out_rows(b):
        return y_low.at[pl.ds(b * tok, tok)]

    out_args = (lambda s: out.at[s], out_send, out_recv)
    for b in range(seqs):
        place.send_home_block(b, out_rows(b), *out_args, out_own)

    cot_copy = pltpu.make_async_copy(cot_in, cot, load_sem.at[layers, 0])
    cot_copy.start()

    def loads(layer):
        pairs = (
            (unit_in.at[layer, 1], unit2), (scale_in.at[layer, 1], scale2), (unit_in.at[layer, 0], unit1),
            (scale_in.at[layer, 0], scale1), (w_out.at[layer], wout), (q_in.at[layer], q), (k_in.at[layer], k),
            (v_in.at[layer], v), (w_qkv.at[layer], wqkv),
        )
        return [pltpu.make_async_copy(src, dst.at[layer % 2], load_sem.at[layer, i]) for i, (src, dst) in enumerate(pairs)]

    def ffn_loads(layer, i):
        slot = lax.rem(i, 2)
        units = pl.ds(pl.multiple_of(i * SPAN, SPAN), SPAN)
        return [
            pltpu.make_async_copy(full.at[layer, 1, units], down.at[slot], ffn_sem.at[slot, 0]),
            pltpu.make_async_copy(slope_in.at[layer, i], slope.at[slot], ffn_sem.at[slot, 1]),
            pltpu.make_async_copy(full.at[layer, 0, units], up.at[slot], ffn_sem.at[slot, 2]),
        ]

    order = list(reversed(range(layers)))
    for copy in loads(order[0])[:2]:
        copy.start()
    for i in range(2):
        for copy in ffn_loads(order[0], i):
            copy.start()
    for copy in loads(order[0])[2:]:
        copy.start()
    half = width // 2
    for layer in order:
        here = layer % 2
        mine = loads(layer)
        if layer == order[0]:
            cot_copy.wait()
        if layer > 0:
            for copy in loads(layer - 1):
                copy.start()
        mine[0].wait()
        mine[1].wait()

        def second_norm(at):
            grad = cot[at].astype(jnp.float32) if layer == order[0] else acc[at]
            grad = norm_grad(grad, unit2[here, at].astype(jnp.float32), scale2[here, at, :1], gains[layer, 1])
            acc[at] = grad
            low[at] = grad.astype(jnp.bfloat16)

        each(rows // 64, 64, second_norm)

        @pl.loop(0, spans)
        def _(i):
            slot = lax.rem(i, 2)
            for copy in ffn_loads(layer, i):
                copy.wait()
            for part in range(2):
                at = pl.ds(part * (rows // 2), rows // 2)
                grad = multiply_back(low[at], down[slot]) * slope[slot, at].astype(jnp.float32)
                acc[at] += multiply(grad.astype(jnp.bfloat16), up[slot])

            @pl.when(i + 2 < spans)
            def _():
                for copy in ffn_loads(layer, i + 2):
                    copy.start()

        if layer > 0:
            for i in range(2):
                for copy in ffn_loads(layer - 1, i):
                    copy.start()
        mine[2].wait()
        mine[3].wait()

        def first_norm(at):
            grad = norm_grad(acc[at], unit1[here, at].astype(jnp.float32), scale1[here, at, :1], gains[layer, 0])
            acc[at] = grad
            low[at] = grad.astype(jnp.bfloat16)

        each(rows // 64, 64, first_norm)
        mine[4].wait()
        for part in range(2):
            span = pl.ds(part * half, half)
            context[:, span] = multiply_back(low[...], wout[here, span]).astype(jnp.bfloat16)
        for copy in mine[5:8]:
            copy.wait()

        @pl.loop(0, width // LANES)
        def _(pair):
            attend_back(
                seqs, tok, rim, pair, q.at[here], k.at[here], v.at[here], prefix.at[layer], hide, lse.at[layer], context,
                made, dk, dv, prefix_grads.at[layer], 1.0 / math.sqrt(width // HEADS),
            )

        low_edge, high_edge, own_rows = pl.ds(0, rim), pl.ds(rim + rows, rim), pl.ds(rim, rows)
        for member, ref in enumerate((dk, dv)):
            lanes = pl.ds(member * width, width)
            edge[layer, 0, :, lanes] = ref[low_edge].astype(jnp.bfloat16)
            edge[layer, 1, :, lanes] = ref[high_edge].astype(jnp.bfloat16)

        def edge_copy(side, wide):
            return place.remote(
                edge.at[layer, side], edge_in.at[layer, side], edge_send.at[layer, side], edge_recv.at[layer, side], (place.row, wide)
            )

        mine[8].wait()
        for part in range(2):
            span = pl.ds(part * half, half)
            acc[:, span] += multiply_back(made[:, pl.ds(0, width)], wqkv[here, span, pl.ds(0, width)])
            if part == 0:
                @pl.when(place.part > 0)
                def _():
                    edge_copy(0, place.wide - 1).start()

                @pl.when(place.part < place.parts - 1)
                def _():
                    edge_copy(1, place.wide + 1).start()

        @pl.when(place.part < place.parts - 1)
        def _():
            edge_copy(0, place.wide).wait_recv()
            for member, ref in enumerate((dk, dv)):
                ref[pl.ds(rows, rim)] += edge_in[layer, 0, :, pl.ds(member * width, width)].astype(jnp.float32)

        @pl.when(place.part > 0)
        def _():
            edge_copy(1, place.wide).wait_recv()
            for member, ref in enumerate((dk, dv)):
                ref[pl.ds(rim, rim)] += edge_in[layer, 1, :, pl.ds(member * width, width)].astype(jnp.float32)

        for member, ref in enumerate((dk, dv)):
            def lower(at):
                made[at, pl.ds((1 + member) * width, width)] = ref[pl.ds(pl.multiple_of(at.start + rim, 64), 64)].astype(jnp.bfloat16)

            each(rows // 64, 64, lower)

        @pl.when(place.part > 0)
        def _():
            edge_copy(0, place.wide).wait_send()

        @pl.when(place.part < place.parts - 1)
        def _():
            edge_copy(1, place.wide).wait_send()

        others = pl.ds(width, 2 * width)
        for part in range(2):
            span = pl.ds(part * half, half)
            acc[:, span] += multiply_back(made[:, others], wqkv[here, span, others])

    low[...] = acc[...].astype(jnp.bfloat16)
    home_args = (lambda s: home.at[s], home_send, home_recv)
    for b in range(seqs):
        place.send_home_block(b, low.at[pl.ds(b * tok, tok)], *home_args, home_own)
    for s in range(seqs):
        place.got_home(s, low.at[pl.ds(0, tok)], *home_args, home_own)
        acc[pl.ds(s * tok, tok)] = home[s].astype(jnp.float32)
        pltpu.make_async_copy(acc.at[pl.ds(s * tok, tok)], grads.at[s], store_sem.at[s]).start()
    place.sent_home(low.at[pl.ds(0, tok)], *home_args)
    place.sent_home(out_rows(0), *out_args)
    for s in range(seqs):
        place.got_home(s, out_rows(0), *out_args, out_own)
        pltpu.make_async_copy(acc.at[pl.ds(s * tok, tok)], grads.at[s], store_sem.at[s]).wait()


def backward(y_low, cot, full, w_qkv, w_out, q, k, v, unit, scale, slope, lse, hide, gains, prefix, seqs):
    rows, width = y_low.shape
    layers, rim, tok = w_qkv.shape[0], PAIR_MAX, rows // seqs
    low, full_type = jnp.bfloat16, jnp.float32
    shape = jax.ShapeDtypeStruct
    dma = pltpu.SemaphoreType.DMA
    vmem = pltpu.VMEM
    return pl.pallas_call(
        functools.partial(backward_kernel, seqs, tok, rim),
        out_shape=(shape((seqs, tok, width), low), shape((seqs, tok, width), full_type), shape(prefix.shape, full_type)),
        in_specs=[pl.BlockSpec(memory_space=pl.ANY)] * 11 + [pl.BlockSpec(memory_space=pltpu.VMEM)] * 4,
        out_specs=(pl.BlockSpec(memory_space=pl.ANY),) * 2 + (pl.BlockSpec(memory_space=pltpu.VMEM),),
        scratch_shapes=[
            vmem((2,) + w_qkv.shape[1:], low), vmem((2,) + w_out.shape[1:], low), vmem((2, rows, width), low),
            vmem((2, rows + 2 * rim, width), low), vmem((2, rows + 2 * rim, width), low),
            vmem((2, rows, width), low), vmem((2, rows, width), low), vmem((2, rows, LANES), full_type), vmem((2, rows, LANES), full_type),
            vmem((2, SPAN, width), low), vmem((2, SPAN, width), low), vmem((2, rows, SPAN), low),
            vmem((rows, width), low), vmem((rows, width), full_type), vmem((rows, width), low), vmem((rows, width), low),
            vmem((rows, 3 * width), low), vmem((rows + 2 * rim, width), full_type), vmem((rows + 2 * rim, width), full_type),
            vmem((layers, 2, rim, 2 * width), low), vmem((layers, 2, rim, 2 * width), low), vmem((seqs, tok, width), low),
            dma((layers + 1, 9)), dma((2, 3)), dma, dma((seqs,)), dma, dma, dma((seqs,)), dma, dma((layers, 2)), dma((layers, 2)), dma((seqs,)),
        ],
        compiler_params=pltpu.CompilerParams(collective_id=1, has_side_effects=True, vmem_limit_bytes=67043328),
    )(y_low, cot, full, w_qkv, w_out, q, k, v, unit, scale, slope, lse, hide, gains, prefix)


def local(
    tokens,
    segments,
    w_qkv,
    b_qkv,
    w_out,
    b_out,
    norm_gain,
    norm_bias,
    w_up,
    b_up,
    w_down,
    b_down,
    prefix,
    cotangent,
):
    seqs, tok, width = tokens.shape
    layers, rim, rows = w_qkv.shape[0], PAIR_MAX, seqs * tok
    wides = lax.axis_size("wide")
    fast = wides == 8 and lax.axis_size("rows") == 4
    parts = wides // seqs
    wide = lax.axis_index("wide")
    ids = jnp.pad(segments, ((0, 0), (rim, rim)), constant_values=-1)
    ids = lax.dynamic_slice(ids, (lax.div(wide, parts), lax.rem(wide, parts) * rows), (1, rows + 2 * rim))[0]
    hide = jnp.stack(
        [
            jnp.where(ids[b * tok : b * tok + tok + 2 * rim, None] == ids[None, b * tok + rim : b * tok + rim + tok], 0.0, -1e30)
            for b in range(seqs)
        ]
    )
    full_in = w_up
    if not fast:
        full_in = jnp.stack([lax.all_gather(w, "wide", axis=1, tiled=True) for w in (w_up, w_down)], axis=1)
    gains, shifts = norm_gain[:, :, None], norm_bias[:, :, None]
    y_low, cot, full, q, k, v, unit, scale, slope, lse = forward(
        fast, tokens, cotangent, w_qkv, w_out, w_up, w_down, full_in, hide, b_qkv[:, None], b_out[:, None], gains, shifts,
        b_up.astype(jnp.float32).reshape(1, -1), b_down[:, None], prefix,
    )
    output, grads, prefix_grads = backward(
        y_low, cot, full if fast else full_in, w_qkv, w_out, q, k, v, unit, scale, slope, lse, hide, gains, prefix, seqs
    )
    return output, grads, lax.psum(prefix_grads, ("rows", "wide"))


def solution(mesh):
    return jax.shard_map(
        local,
        mesh=mesh,
        in_specs=(
            P("rows", "wide", None),
            P("rows", None),
            P(),
            P(),
            P(),
            P(),
            P(),
            P(),
            P(None, "wide", None),
            P(None, "wide"),
            P(None, "wide", None),
            P(),
            P(),
            P("rows", "wide", None),
        ),
        out_specs=(P("rows", "wide", None), P("rows", "wide", None), P()),
        check_vma=False,
    )
```

```python
import functools
import math

import jax
import jax.numpy as jnp
from jax import lax
from jax.experimental import pallas as pl
from jax.experimental.pallas import tpu as pltpu
from jax.sharding import PartitionSpec as P

HEADS = 16
PAIR_MAX = 128
MESH = pl.DeviceIdType.MESH
LANES = 128
SPAN = 1024
ROOT_HALF = math.sqrt(0.5)


def multiply(left, right):
    return jnp.dot(left, right, preferred_element_type=jnp.float32)


def multiply_back(left, right):
    return lax.dot_general(left, right, (((1,), (1,)), ((), ())), preferred_element_type=jnp.float32)


def multiply_first(left, right):
    return lax.dot_general(left, right, (((0,), (0,)), ((), ())), preferred_element_type=jnp.float32)


def two_heads(rows):
    half = rows.shape[1] // 2
    lane = lax.broadcasted_iota(jnp.int32, rows.shape, 1)
    nothing = jnp.zeros_like(rows)
    return jnp.concatenate([jnp.where(lane < half, rows, nothing), jnp.where(lane >= half, rows, nothing)], axis=0)


def own_heads(columns):
    half, count = columns.shape[0] // 2, columns.shape[1] // 2
    place = lax.broadcasted_iota(jnp.int32, (columns.shape[0], count), 0)
    return jnp.where(place < half, columns[:, :count], columns[:, count:]).T


def attend(blocks, rows, rim, pair, q_ref, k_ref, v_ref, prefix_ref, hide_ref, context_ref, lse_ref):
    lanes = pl.ds(pl.multiple_of(pair * 128, 128), 128)
    prefix_keys, prefix_values = prefix_ref[0, :, lanes], prefix_ref[1, :, lanes]
    for block in range(blocks):
        here = pl.ds(block * rows, rows)
        window = pl.ds(block * rows, rows + 2 * rim)
        queries = two_heads(q_ref[here, lanes])
        hide = hide_ref[block]
        fixed = multiply_back(prefix_keys, queries)
        near = multiply_back(k_ref[window, lanes], queries) + jnp.concatenate([hide, hide], axis=1)
        top = jnp.maximum(jnp.max(fixed, axis=0, keepdims=True), jnp.max(near, axis=0, keepdims=True))
        fixed, near = jnp.exp(fixed - top), jnp.exp(near - top)
        total = jnp.sum(fixed, axis=0, keepdims=True) + jnp.sum(near, axis=0, keepdims=True)
        share = 1.0 / total
        columns = multiply_first(prefix_values, fixed.astype(jnp.bfloat16)) + multiply_first(
            v_ref[window, lanes], near.astype(jnp.bfloat16)
        )
        context_ref[here, lanes] = own_heads(columns * share).astype(jnp.bfloat16)
        lse_ref[pair * blocks + block] = top + jnp.log(total)


def attend_back(blocks, rows, rim, pair, q_ref, k_ref, v_ref, prefix_ref, hide_ref, lse_ref, grad_ref, dq_ref, dk_ref, dv_ref, dp_ref, scale):
    lanes = pl.ds(pl.multiple_of(pair * 128, 128), 128)
    prefix_keys, prefix_values = prefix_ref[0, :, lanes], prefix_ref[1, :, lanes]
    for block in range(blocks):
        here = pl.ds(block * rows, rows)
        window = pl.ds(block * rows, rows + 2 * rim)
        queries = two_heads(q_ref[here, lanes])
        grads = two_heads(grad_ref[here, lanes])
        hide = hide_ref[block]
        keys, values = k_ref[window, lanes], v_ref[window, lanes]
        lse = lse_ref[pair * blocks + block]
        fixed = jnp.exp(multiply_back(prefix_keys, queries) - lse)
        near = jnp.exp(multiply_back(keys, queries) + jnp.concatenate([hide, hide], axis=1) - lse)
        grad_fixed = multiply_back(prefix_values, grads)
        grad_near = multiply_back(values, grads)
        dots = jnp.sum(fixed * grad_fixed, axis=0, keepdims=True) + jnp.sum(near * grad_near, axis=0, keepdims=True)
        grad_fixed = (fixed * (grad_fixed - dots)).astype(jnp.bfloat16)
        grad_near = (near * (grad_near - dots)).astype(jnp.bfloat16)
        fixed, near = fixed.astype(jnp.bfloat16), near.astype(jnp.bfloat16)
        columns = multiply_first(prefix_keys, grad_fixed) + multiply_first(keys, grad_near)
        dq_ref[here, lanes] = (own_heads(columns) * scale).astype(jnp.bfloat16)
        new_keys, new_values = multiply(grad_near, queries), multiply(near, grads)
        fixed_keys, fixed_values = multiply(grad_fixed, queries), multiply(fixed, grads)
        old = pl.ds(block * rows, 2 * rim)
        fresh = pl.ds(block * rows + 2 * rim, rows)
        if block == 0:
            dk_ref[window, lanes], dv_ref[window, lanes] = new_keys, new_values
            dp_ref[0, :, lanes], dp_ref[1, :, lanes] = fixed_keys, fixed_values
        else:
            dk_ref[old, lanes] += new_keys[: 2 * rim]
            dv_ref[old, lanes] += new_values[: 2 * rim]
            dk_ref[fresh, lanes], dv_ref[fresh, lanes] = new_keys[2 * rim :], new_values[2 * rim :]
            dp_ref[0, :, lanes] += fixed_keys
            dp_ref[1, :, lanes] += fixed_values


def gelu_pair(values):
    size = jnp.abs(values) * ROOT_HALF
    bell = jnp.exp(values * values * -0.5)
    t = 1.0 / (1.0 + 0.3275911 * size)
    series = ((((1.061405429 * t - 1.453152027) * t + 1.421413741) * t - 0.284496736) * t + 0.254829592) * t
    tail = 0.5 * series * bell
    below = jnp.where(values < 0, tail, 1.0 - tail)
    return values * below, below + values * bell * (1.0 / math.sqrt(2.0 * math.pi))


def normalize(values):
    center = values - jnp.mean(values, axis=-1, keepdims=True)
    scale = lax.rsqrt(jnp.mean(center * center, axis=-1, keepdims=True) + 1e-05)
    return center * scale, scale


def norm_grad(grad, unit, scale, gain):
    inner = grad * gain
    first = jnp.mean(inner, axis=-1, keepdims=True)
    second = jnp.mean(inner * unit, axis=-1, keepdims=True)
    return scale * (inner - first - unit * second)


def each(count, step, body):
    @pl.loop(0, count)
    def _(i):
        body(pl.ds(pl.multiple_of(i * step, step), step))


class Place:
    def __init__(self, seqs, tok):
        self.seqs, self.tok, self.rows = seqs, tok, seqs * tok
        self.wide_size = lax.axis_size("wide")
        self.parts = self.wide_size // seqs
        self.row, self.wide = lax.axis_index("rows"), lax.axis_index("wide")
        self.seq, self.part = lax.div(self.wide, self.parts), lax.rem(self.wide, self.parts)

    def others(self, body):
        @pl.loop(1, self.wide_size)
        def _(step):
            body(lax.rem(self.wide + step, self.wide_size))

    def barrier(self, more):
        sem = pltpu.get_barrier_semaphore()
        self.others(lambda other: pl.semaphore_signal(sem, inc=1, device_id=(self.row, other), device_id_type=MESH))
        for device in more:
            pl.semaphore_signal(sem, inc=1, device_id=device, device_id_type=MESH)
        pl.semaphore_wait(sem, self.wide_size - 1 + len(more))

    def remote(self, src, dst, send, recv, device):
        return pltpu.make_async_remote_copy(
            src_ref=src, dst_ref=dst, send_sem=send, recv_sem=recv, device_id=device, device_id_type=MESH
        )

    def send_out(self, parts, target, send, recv, own):
        block = lax.rem(self.wide, self.seqs)
        for s in range(self.seqs):
            goal = s * self.parts + lax.div(self.wide, self.seqs)

            @pl.when(goal != self.wide)
            def _():
                self.remote(parts(s), target(block), send, recv.at[block], (self.row, goal)).start()

            @pl.when(goal == self.wide)
            def _():
                pltpu.make_async_copy(parts(s), target(block), own).start()

    def sent_out(self, parts, target, send, recv, own):
        block = lax.rem(self.wide, self.seqs)
        for s in range(self.seqs):
            goal = s * self.parts + lax.div(self.wide, self.seqs)

            @pl.when(goal != self.wide)
            def _():
                self.remote(parts(s), target(block), send, recv.at[block], (self.row, goal)).wait_send()

    def got_out(self, parts, target, send, recv, own):
        for b in range(self.seqs):
            source = self.part * self.seqs + b

            @pl.when(source != self.wide)
            def _():
                self.remote(parts(0), target(b), send, recv.at[b], (self.row, self.wide)).wait_recv()

            @pl.when(source == self.wide)
            def _():
                pltpu.make_async_copy(parts(0), target(b), own).wait()

    def send_home_block(self, b, part, target, send, recv, own):
        goal = self.part * self.seqs + b

        @pl.when(goal != self.wide)
        def _():
            self.remote(part, target(self.seq), send, recv.at[self.seq], (self.row, goal)).start()

        @pl.when(goal == self.wide)
        def _():
            pltpu.make_async_copy(part, target(self.seq), own).start()

    def sent_home(self, part, target, send, recv):
        for b in range(self.seqs):
            goal = self.part * self.seqs + b

            @pl.when(goal != self.wide)
            def _():
                self.remote(part, target(self.seq), send, recv.at[self.seq], (self.row, goal)).wait_send()

    def got_home(self, s, part, target, send, recv, own):
        source = s * self.parts + lax.div(self.wide, self.seqs)

        @pl.when(source != self.wide)
        def _():
            self.remote(part, target(s), send, recv.at[s], (self.row, self.wide)).wait_recv()

        @pl.when(source == self.wide)
        def _():
            pltpu.make_async_copy(part, target(s), own).wait()


class Gather:
    def __init__(self, shards, full, sems):
        self.shards = shards
        self.full = full
        self.send_sem, self.zs, self.xs, self.ys, self.ds, self.cz, self.cx, self.cy, self.cd, self.cown, self.own = sems
        self.row = lax.axis_index("rows")
        self.wide = lax.axis_index("wide")
        self.z, self.core = lax.div(self.wide, 2), lax.rem(self.wide, 2)
        self.shard_rows = shards[0].shape[1]
        self.unit_rows = self.shard_rows // 4
        self.row_x = self.row + 1 - 2 * lax.rem(self.row, 2)
        self.row_y = lax.rem(self.row + 2, 4)
        self.row_d = 3 - self.row

    def unit(self, layer, member, z, core, quarter):
        start = (z * 2 + core) * self.shard_rows + quarter * self.unit_rows
        return self.full.at[layer, member, pl.ds(pl.multiple_of(start, self.unit_rows), self.unit_rows)]

    def shard(self, layer, member, z, core):
        start = (z * 2 + core) * self.shard_rows
        return self.full.at[layer, member, pl.ds(pl.multiple_of(start, self.shard_rows), self.shard_rows)]

    def copy(self, src, dst, recv, kind):
        if kind == "x":
            device = (self.row_x, self.wide)
        elif kind == "y":
            device = (self.row_y, self.wide)
        elif kind == "core":
            device = (self.row, self.z * 2 + 1 - self.core)
        else:
            device = (self.row, self.wide + 2 - 4 * kind)
        return pltpu.make_async_remote_copy(
            src_ref=src, dst_ref=dst, send_sem=self.send_sem, recv_sem=recv, device_id=device, device_id_type=MESH
        )

    def start_z(self, layer):
        for member in range(2):
            start = pl.multiple_of(self.row * self.unit_rows, self.unit_rows)
            mine = self.shards[member].at[layer, pl.ds(start, self.unit_rows)]
            here = self.unit(layer, member, self.z, self.core, self.row)

            @pl.when(self.z < 3)
            def _():
                self.copy(mine, here, self.zs.at[layer, member, 0, 0], 0).start()

            @pl.when(self.z > 0)
            def _():
                self.copy(mine, here, self.zs.at[layer, member, 0, 1], 1).start()

    def start_core(self, layer):
        for member in range(2):
            place = self.shard(layer, member, self.z, self.core)
            pltpu.make_async_copy(self.shards[member].at[layer], place, self.own.at[layer, member]).start()
            self.copy(self.shards[member].at[layer], place, self.cown.at[layer, member], "core").start()

    def slot(self, i):
        near = jnp.minimum(self.z, 3 - self.z)
        far_side = 1 - lax.div(self.z, 2)
        both = jnp.minimum(lax.div(i, jnp.maximum(2 * near, 1)), 1) + (1 - jnp.minimum(near, 1))
        both = 1 - jnp.minimum(both, 1)
        step = both * lax.div(i, 2) + (1 - both) * (i - near)
        side = both * lax.rem(i, 2) + (1 - both) * far_side
        return step, side, self.z + (1 + step) * (2 * side - 1)

    def on_z(self, layer, i):
        step, side, origin = self.slot(i)
        for member in range(2):
            unit = self.unit(layer, member, origin, self.core, self.row)
            self.copy(unit, unit, self.zs.at[layer, member, step, side], "x").wait_recv()
            target = self.z + 1 - 2 * side

            @pl.when((target >= 0) & (target < 4))
            def _():
                self.copy(unit, unit, self.zs.at[layer, member, step + 1, side], side).start()

            self.copy(unit, unit, self.xs.at[layer, member, step, side], "x").start()
            self.copy(unit, unit, self.ys.at[layer, member, step, side], "y").start()
            self.copy(unit, unit, self.cz.at[layer, member, step, side], "core").start()

    def on_xy(self, layer, i):
        step, side, origin = self.slot(i)
        for member in range(2):
            unit = self.unit(layer, member, origin, self.core, self.row_x)
            self.copy(unit, unit, self.xs.at[layer, member, step, side], "x").wait_recv()
            if member == 0:
                self.copy(unit, unit, self.ds.at[layer, member, step, side], "y").start()
            self.copy(unit, unit, self.cx.at[layer, member, step, side], "core").start()
            unit = self.unit(layer, member, origin, self.core, self.row_y)
            self.copy(unit, unit, self.ys.at[layer, member, step, side], "y").wait_recv()
            if member == 1:
                self.copy(unit, unit, self.ds.at[layer, member, step, side], "x").start()
            self.copy(unit, unit, self.cy.at[layer, member, step, side], "core").start()

    def on_d(self, layer, i):
        step, side, origin = self.slot(i)
        for member in range(2):
            unit = self.unit(layer, member, origin, self.core, self.row_d)
            self.copy(unit, unit, self.ds.at[layer, member, step, side], "x").wait_recv()
            self.copy(unit, unit, self.cd.at[layer, member, step, side], "core").start()

    def on_core(self, layer, i):
        step, side, origin = self.slot(i)
        for member in range(2):
            for sem, quarter in ((self.cz, self.row), (self.cx, self.row_x), (self.cy, self.row_y), (self.cd, self.row_d)):
                unit = self.unit(layer, member, origin, 1 - self.core, quarter)
                self.copy(unit, unit, sem.at[layer, member, step, side], "core").wait_recv()

    def on_own(self, layer):
        for member in range(2):
            place = self.shard(layer, member, self.z, self.core)
            pltpu.make_async_copy(self.shards[member].at[layer], place, self.own.at[layer, member]).wait()
            place = self.shard(layer, member, self.z, 1 - self.core)
            self.copy(place, place, self.cown.at[layer, member], "core").wait_recv()

    def drain(self, layers):
        def wait(units):
            span = self.full.at[0, 0, pl.ds(0, units * self.unit_rows)]
            self.copy(span, span, self.own.at[0, 0], "core").wait_send()

        @pl.loop(0, layers)
        def _(layer):
            wait(8)

            @pl.when(self.z < 3)
            def _():
                wait(2)

            @pl.when(self.z > 0)
            def _():
                wait(2)

            @pl.loop(0, 3)
            def _(i):
                step, side, origin = self.slot(i)
                target = self.z + 1 - 2 * side

                @pl.when((target >= 0) & (target < 4))
                def _():
                    wait(2)

                wait(14)


class PrefixSum:
    def __init__(self, place, parts, inbox, planes, total, sems):
        self.parts, self.inbox, self.planes, self.total = parts, inbox, planes, total
        self.send_sem, self.in_sem, self.plane_sem, self.total_sem = sems
        self.row = place.row
        self.z, self.core = lax.div(place.wide, 2), lax.rem(place.wide, 2)
        self.me = self.row * 2 + self.core
        self.size = inbox.shape[2]

    def peers(self, body):
        @pl.loop(1, 8)
        def _(step):
            body(lax.rem(self.me + step, 8))

    def others(self):
        return [(lax.rem(self.row + step, 4), self.z * 2 + core) for step in range(1, 4) for core in range(2)]

    def piece(self, ref, layer, index):
        start = lax.rem(index, 4) * self.size
        return ref.at[layer, lax.div(index, 4), pl.ds(pl.multiple_of(start, self.size), self.size)]

    def copy(self, src, dst, recv, row, wide):
        return pltpu.make_async_remote_copy(
            src_ref=src, dst_ref=dst, send_sem=self.send_sem, recv_sem=recv, device_id=(row, wide), device_id_type=MESH
        )

    def in_copy(self, layer, peer, origin):
        return self.copy(
            self.piece(self.parts, layer, peer), self.inbox.at[layer, origin], self.in_sem.at[layer, origin],
            lax.div(peer, 2), self.z * 2 + lax.rem(peer, 2),
        )

    def plane_copy(self, layer, z, origin):
        place = self.planes.at[layer, origin]
        return self.copy(place, place, self.plane_sem.at[layer, origin], self.row, z * 2 + self.core)

    def total_copy(self, layer, peer, origin):
        place = self.piece(self.total, layer, origin)
        return self.copy(place, place, self.total_sem.at[layer, origin], lax.div(peer, 2), self.z * 2 + lax.rem(peer, 2))

    def planes_others(self, body):
        @pl.loop(1, 4)
        def _(step):
            body(lax.rem(self.z + step, 4))

    def start(self, layer):
        self.peers(lambda peer: self.in_copy(layer, peer, self.me).start())

    def middle(self, layer):
        self.peers(lambda peer: self.in_copy(layer, self.me, peer).wait_recv())
        value = self.piece(self.parts, layer, self.me)[...]
        for step in range(1, 8):
            value += self.inbox[layer, lax.rem(self.me + step, 8)]
        self.planes[layer, self.z] = value
        self.planes_others(lambda z: self.plane_copy(layer, z, self.z).start())

    def last(self, layer):
        self.planes_others(lambda z: self.plane_copy(layer, self.z, z).wait_recv())
        value = self.planes[layer, 0]
        for z in range(1, 4):
            value += self.planes[layer, z]
        self.piece(self.total, layer, self.me)[...] = value
        self.peers(lambda peer: self.total_copy(layer, peer, self.me).start())

    def finish(self, layer):
        self.peers(lambda peer: self.total_copy(layer, self.me, peer).wait_recv())
        self.peers(lambda peer: self.in_copy(layer, peer, self.me).wait_send())
        self.planes_others(lambda z: self.plane_copy(layer, z, self.z).wait_send())
        self.peers(lambda peer: self.total_copy(layer, peer, self.me).wait_send())


def prefix_scratch(shape):
    layers, members, count, width = shape
    size = members * count // 8
    dma = pltpu.SemaphoreType.DMA
    return [
        pltpu.VMEM(shape, jnp.float32), pltpu.VMEM((layers, 8, size, width), jnp.float32),
        pltpu.VMEM((layers, 4, size, width), jnp.float32), dma, dma((layers, 8)), dma((layers, 4)), dma((layers, 8)),
    ]


def gather_sems(layers):
    return (
        [pltpu.SemaphoreType.DMA]
        + [pltpu.SemaphoreType.DMA((layers, 2, 3, 2))] * 8
        + [pltpu.SemaphoreType.DMA((layers, 2))] * 2
    )


def forward_kernel(
    fast, seqs, tok, rim,
    tokens, cotangent, w_qkv, w_out, w_up, w_down, full_in,
    hide, b_qkv, b_out, gains, shifts, b_up, b_down, prefix,
    y_low, cot_out, full_out, q_out, k_out, v_out, unit_out, scale_out, slope_out, lse_out,
    full, wqkv, wout, x, low, acc, q, k, v, halo, context, slope, unit1, unit2, scale1, scale2, lse, bias,
    load_sem, store_sem, slope_sem, full_sem, tok_send, tok_recv, tok_own, cot_send, cot_recv, cot_own,
    halo_send, halo_recv, bias_send, bias_recv, bias_own,
    *gather_sem,
):
    layers, width = w_qkv.shape[0], tokens.shape[2]
    place = Place(seqs, tok)
    rows = place.rows
    gather = Gather((w_up, w_down), full, gather_sem) if fast else None
    place.barrier(((gather.row_x, place.wide), (gather.row_y, place.wide)) if fast else ())
    own_bias = bias.at[place.wide]

    def load(layer):
        return (
            pltpu.make_async_copy(w_qkv.at[layer], wqkv, load_sem.at[0]),
            pltpu.make_async_copy(w_out.at[layer], wout, load_sem.at[1]),
        )

    def put_bias(other):
        return place.remote(b_up, own_bias, bias_send, bias_recv.at[place.wide], (place.row, other))

    def got_bias(other):
        return place.remote(b_up, bias.at[other], bias_send, bias_recv.at[other], (place.row, other))

    if fast:
        gather.start_z(0)
        gather.start_core(0)
    else:
        pltpu.make_async_copy(full_in, full, full_sem.at[0]).start()
    for copy in load(0):
        copy.start()
    place.others(lambda other: put_bias(other).start())
    pltpu.make_async_copy(b_up, own_bias, bias_own).start()

    tok_args = (lambda s: tokens.at[s], lambda b: low.at[pl.ds(pl.multiple_of(b * tok, tok), tok)], tok_send, tok_recv, tok_own)
    cot_args = (lambda s: cotangent.at[s], lambda b: cot_out.at[pl.ds(pl.multiple_of(b * tok, tok), tok)], cot_send, cot_recv, cot_own)
    events = []
    if fast:
        gather.on_z(0, 0)
        place.send_out(*tok_args)
        gather.on_z(0, 1)
        gather.on_xy(0, 0)
        gather.start_z(1)
        gather.start_core(1)
        gather.on_z(0, 2)
        gather.on_xy(0, 1)
        events = [
            (gather.on_d, 0, 0), (gather.on_xy, 0, 2), (gather.on_z, 1, 0), (gather.on_d, 0, 1), (gather.on_d, 0, 2),
            (gather.on_z, 1, 1), (gather.on_z, 1, 2), (gather.on_xy, 1, 0),
        ]
    else:
        place.send_out(*tok_args)

    def tick(count=1):
        for _ in range(min(count, len(events))):
            event, layer, i = events.pop(0)
            event(layer, i)

    blank = jnp.zeros((rim, width), jnp.bfloat16)

    @pl.when(place.part == 0)
    def _():
        k[pl.ds(0, rim)] = blank
        v[pl.ds(0, rim)] = blank

    @pl.when(place.part == place.parts - 1)
    def _():
        k[pl.ds(rim + rows, rim)] = blank
        v[pl.ds(rim + rows, rim)] = blank

    place.got_out(*tok_args)

    def halo_copy(layer, member, side, wide):
        ref = (k, v)[member]
        return place.remote(
            ref.at[pl.ds((rows, rim)[side], rim)], halo.at[layer, member, side],
            halo_send.at[member, side], halo_recv.at[layer, member, side], (place.row, wide),
        )

    def halos(body, to):
        for side in range(2):
            @pl.when(place.part < place.parts - 1 if (side == 0) == to else place.part > 0)
            def _():
                for member in range(2):
                    body(member, side, jnp.clip(place.wide + (1 - 2 * side), 0, place.wide_size - 1))

    def got_halo(layer, member, side, wide):
        halo_copy(layer, member, side, place.wide).wait_recv()
        (k, v)[member][pl.ds((0, rim + rows)[side], rim)] = halo[layer, member, side]

    def kept(layer):
        return [
            pltpu.make_async_copy(src, dst.at[layer], store_sem.at[i])
            for i, (src, dst) in enumerate(((q, q_out), (k, k_out), (v, v_out)))
        ]

    def kept_norm(layer, which):
        unit, scale = ((unit1, scale1), (unit2, scale2))[which]
        return [
            pltpu.make_async_copy(unit, unit_out.at[layer, which], store_sem.at[3 + which]),
            pltpu.make_async_copy(scale, scale_out.at[layer, which], store_sem.at[5 + which]),
        ]

    half = width // 2
    for layer in range(layers):
        if layer > 0:
            for copy in kept(layer - 1) + kept_norm(layer - 1, 0) + kept_norm(layer - 1, 1):
                copy.wait()
        load(layer)[0].wait()
        for part in (2, 3, 4, 5, 0, 1):
            lanes = pl.ds(part * half, half)
            made = multiply(low[...], wqkv[:, lanes]) + b_qkv[layer : layer + 1, lanes]
            kind, side = part // 2, pl.ds((part % 2) * half, half)
            if kind == 0:
                q[:, side] = made.astype(jnp.bfloat16) * (1.0 / math.sqrt(width // HEADS))
            else:
                (k, v)[kind - 1][pl.ds(rim, rows), side] = made.astype(jnp.bfloat16)
            if part == 5:
                tick()
                halos(lambda *at: halo_copy(layer, *at).start(), True)
        if layer + 1 < layers:
            load(layer + 1)[0].start()
        tick()
        halos(lambda *at: got_halo(layer, *at), False)
        halos(lambda *at: halo_copy(layer, *at).wait_send(), True)
        for copy in kept(layer):
            copy.start()

        for first in (0, 4):
            @pl.loop(first, first + 4)
            def _(pair):
                attend(seqs, tok, rim, pair, q, k, v, prefix.at[layer], hide, context, lse.at[layer])

            tick()
        load(layer)[1].wait()
        for part in range(2):
            lanes = pl.ds(part * half, half)
            acc[:, lanes] = multiply(context[...], wout[:, lanes])
        if layer + 1 < layers:
            load(layer + 1)[1].start()
        tick()

        def first_norm(at):
            before = low[at].astype(jnp.float32) if layer == 0 else x[at]
            unit, scale = normalize(before + acc[at] + b_out[layer : layer + 1])
            unit1[at] = unit.astype(jnp.bfloat16)
            scale1[at] = jnp.broadcast_to(scale, (scale.shape[0], LANES))
            normed = unit * gains[layer, :1] + shifts[layer, :1]
            low[at] = normed.astype(jnp.bfloat16)
            acc[at] = normed + b_down[layer : layer + 1]

        each(rows // 64, 64, first_norm)
        for copy in kept_norm(layer, 0):
            copy.start()
        tick()
        if layer == 0:
            pltpu.make_async_copy(b_up, own_bias, bias_own).wait()
            place.others(lambda other: got_bias(other).wait_recv())

            place.others(lambda other: put_bias(other).wait_send())
            if not fast:
                pltpu.make_async_copy(full_in, full, full_sem.at[0]).wait()

        hidden = b_up.shape[1] // layers

        @pl.loop(0, full.shape[2] // SPAN)
        def _(i):
            spot = i
            if fast:
                @pl.when(i == 0)
                def _():
                    gather.on_own(layer)

                @pl.when(i > 0)
                def _():
                    if layer == 1:
                        @pl.when(i > 1)
                        def _():
                            gather.on_xy(1, i - 1)

                        gather.on_d(1, i - 1)
                    gather.on_core(layer, i - 1)

                origin = gather.slot(jnp.maximum(i - 1, 0))[2]
                started = jnp.minimum(i, 1)
                spot = started * origin + (1 - started) * gather.z
            units = pl.ds(pl.multiple_of(spot * SPAN, SPAN), SPAN)
            slot = lax.rem(i, 2)
            step_bias = jnp.concatenate(
                [bias[spot * (SPAN // hidden) + n, :, pl.ds(layer * hidden, hidden)] for n in range(SPAN // hidden)], axis=1
            )

            @pl.when(i > 1)
            def _():
                pltpu.make_async_copy(slope.at[slot], slope_out.at[layer, spot], slope_sem.at[slot]).wait()

            for part in range(2):
                at = pl.ds(part * (rows // 2), rows // 2)
                act, rise = gelu_pair(multiply_back(low[at], full[layer, 0, units]) + step_bias)
                slope[slot, at] = rise.astype(jnp.bfloat16)
                acc[at] += multiply(act.astype(jnp.bfloat16), full[layer, 1, units])
            pltpu.make_async_copy(slope.at[slot], slope_out.at[layer, spot], slope_sem.at[slot]).start()
            if fast:
                pltpu.make_async_copy(full.at[layer, :, units], full_out.at[layer, :, units], full_sem.at[layer]).start()

        for slot in range(2):
            pltpu.make_async_copy(slope.at[slot], slope_out.at[layer, 0], slope_sem.at[slot]).wait()

        def second_norm(at):
            unit, scale = normalize(acc[at])
            unit2[at] = unit.astype(jnp.bfloat16)
            scale2[at] = jnp.broadcast_to(scale, (scale.shape[0], LANES))
            after = unit * gains[layer, 1:] + shifts[layer, 1:]
            low[at] = after.astype(jnp.bfloat16)
            if layer + 1 < layers:
                x[at] = after

        each(rows // 64, 64, second_norm)
        for copy in kept_norm(layer, 1):
            copy.start()
        if layer == 0:
            place.send_out(*cot_args)
            tick(2)
    last = [pltpu.make_async_copy(low, y_low, store_sem.at[7]), pltpu.make_async_copy(lse, lse_out, store_sem.at[8])]
    for copy in last:
        copy.start()
    place.sent_out(*tok_args)
    place.got_out(*cot_args)
    place.sent_out(*cot_args)
    for copy in last + kept(layers - 1) + kept_norm(layers - 1, 0) + kept_norm(layers - 1, 1):
        copy.wait()
    if fast:
        gather.drain(layers)
        for layer in range(layers):
            pltpu.make_async_copy(full.at[layer], full_out.at[layer], full_sem.at[layer]).wait()


def forward(fast, tokens, cotangent, w_qkv, w_out, w_up, w_down, full_in, hide, b_qkv, b_out, gains, shifts, b_up, b_down, prefix):
    seqs, tok, width = tokens.shape
    layers, rim, rows = w_qkv.shape[0], PAIR_MAX, seqs * tok
    wides = lax.axis_size("wide")
    units = w_up.shape[1] * wides
    low, full_type = jnp.bfloat16, jnp.float32
    spans = units // SPAN
    shape = jax.ShapeDtypeStruct
    dma = pltpu.SemaphoreType.DMA
    scores = (layers, width // LANES * seqs, 1, 2 * tok)
    return pl.pallas_call(
        functools.partial(forward_kernel, fast, seqs, tok, rim),
        out_shape=(
            shape((rows, width), low), shape((rows, width), low), shape((layers, 2, units, width), low),
            shape((layers, rows, width), low), shape((layers, rows + 2 * rim, width), low),
            shape((layers, rows + 2 * rim, width), low), shape((layers, 2, rows, width), low),
            shape((layers, 2, rows, LANES), full_type), shape((layers, spans, rows, SPAN), low), shape(scores, full_type),
        ),
        in_specs=[pl.BlockSpec(memory_space=pl.ANY)] * 7 + [pl.BlockSpec(memory_space=pltpu.VMEM)] * 8,
        out_specs=(pl.BlockSpec(memory_space=pl.ANY),) * 10,
        scratch_shapes=[
            pltpu.VMEM((layers, 2, units, width), low), pltpu.VMEM(w_qkv.shape[1:], low), pltpu.VMEM(w_out.shape[1:], low),
            pltpu.VMEM((rows, width), full_type), pltpu.VMEM((rows, width), low), pltpu.VMEM((rows, width), full_type),
            pltpu.VMEM((rows, width), low), pltpu.VMEM((rows + 2 * rim, width), low), pltpu.VMEM((rows + 2 * rim, width), low),
            pltpu.VMEM((layers, 2, 2, rim, width), low), pltpu.VMEM((rows, width), low), pltpu.VMEM((2, rows, SPAN), low),
            pltpu.VMEM((rows, width), low), pltpu.VMEM((rows, width), low),
            pltpu.VMEM((rows, LANES), full_type), pltpu.VMEM((rows, LANES), full_type),
            pltpu.VMEM(scores, full_type), pltpu.VMEM((wides,) + b_up.shape, full_type),
            dma((2,)), dma((9,)), dma((2,)), dma((layers,)), dma, dma((seqs,)), dma, dma, dma((seqs,)), dma,
            dma((2, 2)), dma((layers, 2, 2)), dma, dma((wides,)), dma,
        ] + (gather_sems(layers) if fast else []),
        compiler_params=pltpu.CompilerParams(collective_id=0, has_side_effects=True, vmem_limit_bytes=67043328),
    )(tokens, cotangent, w_qkv, w_out, w_up, w_down, full_in, hide, b_qkv, b_out, gains, shifts, b_up, b_down, prefix)


def backward_kernel(
    fast, seqs, tok, rim,
    y_low, cot_in, full, w_qkv, w_out, q_in, k_in, v_in, unit_in, scale_in, slope_in,
    lse, hide, gains, prefix,
    out, grads, prefix_grads,
    wqkv, wout, q, k, v, unit1, unit2, scale1, scale2, up, down, slope, cot, acc, low, context, made, dk, dv, edge, edge_in,
    load_sem, ffn_sem, out_send, out_recv, out_own, home_send, home_recv, home_own, edge_send, edge_recv,
    *sums,
):
    layers, width = w_qkv.shape[0], w_qkv.shape[1]
    place = Place(seqs, tok)
    rows = place.rows
    prefix_sum, prefix_parts = None, prefix_grads
    if fast:
        prefix_parts = sums[0]
        prefix_sum = PrefixSum(place, *sums[:3], prefix_grads, sums[3:])
    place.barrier(prefix_sum.others() if fast else ())
    spans = slope_in.shape[1]

    def out_rows(b):
        return y_low.at[pl.ds(b * tok, tok)]

    out_args = (lambda s: out.at[s], out_send, out_recv)
    for b in range(seqs):
        place.send_home_block(b, out_rows(b), *out_args, out_own)

    cot_copy = pltpu.make_async_copy(cot_in, cot, load_sem.at[layers, 0])
    cot_copy.start()

    def loads(layer):
        pairs = (
            (unit_in.at[layer, 1], unit2), (scale_in.at[layer, 1], scale2), (unit_in.at[layer, 0], unit1),
            (scale_in.at[layer, 0], scale1), (w_out.at[layer], wout), (q_in.at[layer], q), (k_in.at[layer], k),
            (v_in.at[layer], v),
        )
        copies = [pltpu.make_async_copy(src, dst.at[layer % 2], load_sem.at[layer, i]) for i, (src, dst) in enumerate(pairs)]
        return copies + [pltpu.make_async_copy(w_qkv.at[layer], wqkv, load_sem.at[layer, 8])]

    def ffn_loads(layer, i):
        slot = lax.rem(i, 2)
        units = pl.ds(pl.multiple_of(i * SPAN, SPAN), SPAN)
        return [
            pltpu.make_async_copy(full.at[layer, 1, units], down.at[slot], ffn_sem.at[slot, 0]),
            pltpu.make_async_copy(slope_in.at[layer, i], slope.at[slot], ffn_sem.at[slot, 1]),
            pltpu.make_async_copy(full.at[layer, 0, units], up.at[slot], ffn_sem.at[slot, 2]),
        ]

    order = list(reversed(range(layers)))
    for copy in loads(order[0])[:2]:
        copy.start()
    for i in range(2):
        for copy in ffn_loads(order[0], i):
            copy.start()
    for copy in loads(order[0])[2:]:
        copy.start()
    half = width // 2
    for layer in order:
        here = layer % 2
        mine = loads(layer)
        if layer == order[0]:
            cot_copy.wait()
        if layer > 0:
            for copy in loads(layer - 1)[:8]:
                copy.start()
        if layer < order[0]:
            mine[8].start()
        mine[0].wait()
        mine[1].wait()

        def second_norm(at):
            grad = cot[at].astype(jnp.float32) if layer == order[0] else acc[at]
            grad = norm_grad(grad, unit2[here, at].astype(jnp.float32), scale2[here, at, :1], gains[layer, 1:])
            acc[at] = grad
            low[at] = grad.astype(jnp.bfloat16)

        each(rows // 64, 64, second_norm)

        @pl.loop(0, spans)
        def _(i):
            slot = lax.rem(i, 2)
            for copy in ffn_loads(layer, i):
                copy.wait()
            for part in range(2):
                at = pl.ds(part * (rows // 2), rows // 2)
                grad = multiply_back(low[at], down[slot]) * slope[slot, at].astype(jnp.float32)
                acc[at] += multiply(grad.astype(jnp.bfloat16), up[slot])

            @pl.when(i + 2 < spans)
            def _():
                for copy in ffn_loads(layer, i + 2):
                    copy.start()

        if layer > 0:
            for i in range(2):
                for copy in ffn_loads(layer - 1, i):
                    copy.start()
        mine[2].wait()
        mine[3].wait()

        def first_norm(at):
            grad = norm_grad(acc[at], unit1[here, at].astype(jnp.float32), scale1[here, at, :1], gains[layer, :1])
            acc[at] = grad
            low[at] = grad.astype(jnp.bfloat16)

        each(rows // 64, 64, first_norm)
        if fast and layer + 1 < layers:
            prefix_sum.last(layer + 1)
        mine[4].wait()
        for part in range(2):
            span = pl.ds(part * half, half)
            context[:, span] = multiply_back(low[...], wout[here, span]).astype(jnp.bfloat16)
        for copy in mine[5:8]:
            copy.wait()

        @pl.loop(0, width // LANES)
        def _(pair):
            attend_back(
                seqs, tok, rim, pair, q.at[here], k.at[here], v.at[here], prefix.at[layer], hide, lse.at[layer], context,
                made, dk, dv, prefix_parts.at[layer], 1.0 / math.sqrt(width // HEADS),
            )

        if fast:
            prefix_sum.start(layer)

        low_edge, high_edge, own_rows = pl.ds(0, rim), pl.ds(rim + rows, rim), pl.ds(rim, rows)
        for member, ref in enumerate((dk, dv)):
            lanes = pl.ds(member * width, width)
            edge[layer, 0, :, lanes] = ref[low_edge].astype(jnp.bfloat16)
            edge[layer, 1, :, lanes] = ref[high_edge].astype(jnp.bfloat16)

        def edge_copy(side, wide):
            return place.remote(
                edge.at[layer, side], edge_in.at[layer, side], edge_send.at[layer, side], edge_recv.at[layer, side], (place.row, wide)
            )

        mine[8].wait()
        for part in range(2):
            span = pl.ds(part * half, half)
            acc[:, span] += multiply_back(made[:, pl.ds(0, width)], wqkv[span, pl.ds(0, width)])
            if part == 0:
                @pl.when(place.part > 0)
                def _():
                    edge_copy(0, place.wide - 1).start()

                @pl.when(place.part < place.parts - 1)
                def _():
                    edge_copy(1, place.wide + 1).start()

        @pl.when(place.part < place.parts - 1)
        def _():
            edge_copy(0, place.wide).wait_recv()
            for member, ref in enumerate((dk, dv)):
                ref[pl.ds(rows, rim)] += edge_in[layer, 0, :, pl.ds(member * width, width)].astype(jnp.float32)

        @pl.when(place.part > 0)
        def _():
            edge_copy(1, place.wide).wait_recv()
            for member, ref in enumerate((dk, dv)):
                ref[pl.ds(rim, rim)] += edge_in[layer, 1, :, pl.ds(member * width, width)].astype(jnp.float32)

        for member, ref in enumerate((dk, dv)):
            def lower(at):
                made[at, pl.ds((1 + member) * width, width)] = ref[pl.ds(pl.multiple_of(at.start + rim, 64), 64)].astype(jnp.bfloat16)

            each(rows // 64, 64, lower)

        @pl.when(place.part > 0)
        def _():
            edge_copy(0, place.wide).wait_send()

        @pl.when(place.part < place.parts - 1)
        def _():
            edge_copy(1, place.wide).wait_send()

        if fast:
            prefix_sum.middle(layer)
        others = pl.ds(width, 2 * width)
        for part in range(2):
            span = pl.ds(part * half, half)
            acc[:, span] += multiply_back(made[:, others], wqkv[span, others])

    low[...] = acc[...].astype(jnp.bfloat16)
    home_args = (lambda s: grads.at[s], home_send, home_recv)
    for b in range(seqs):
        place.send_home_block(b, low.at[pl.ds(b * tok, tok)], *home_args, home_own)
    if fast:
        prefix_sum.last(0)
    for s in range(seqs):
        place.got_home(s, low.at[pl.ds(0, tok)], *home_args, home_own)
        place.got_home(s, out_rows(0), *out_args, out_own)
    place.sent_home(low.at[pl.ds(0, tok)], *home_args)
    place.sent_home(out_rows(0), *out_args)
    if fast:
        for layer in order:
            prefix_sum.finish(layer)


def backward(fast, y_low, cot, full, w_qkv, w_out, q, k, v, unit, scale, slope, lse, hide, gains, prefix, seqs):
    rows, width = y_low.shape
    layers, rim, tok = w_qkv.shape[0], PAIR_MAX, rows // seqs
    low, full_type = jnp.bfloat16, jnp.float32
    shape = jax.ShapeDtypeStruct
    dma = pltpu.SemaphoreType.DMA
    vmem = pltpu.VMEM
    return pl.pallas_call(
        functools.partial(backward_kernel, fast, seqs, tok, rim),
        out_shape=(shape((seqs, tok, width), low), shape((seqs, tok, width), low), shape(prefix.shape, full_type)),
        in_specs=[pl.BlockSpec(memory_space=pl.ANY)] * 11 + [pl.BlockSpec(memory_space=pltpu.VMEM)] * 4,
        out_specs=(pl.BlockSpec(memory_space=pl.ANY),) * 2 + (pl.BlockSpec(memory_space=pltpu.VMEM),),
        scratch_shapes=[
            vmem(w_qkv.shape[1:], low), vmem((2,) + w_out.shape[1:], low), vmem((2, rows, width), low),
            vmem((2, rows + 2 * rim, width), low), vmem((2, rows + 2 * rim, width), low),
            vmem((2, rows, width), low), vmem((2, rows, width), low), vmem((2, rows, LANES), full_type), vmem((2, rows, LANES), full_type),
            vmem((2, SPAN, width), low), vmem((2, SPAN, width), low), vmem((2, rows, SPAN), low),
            vmem((rows, width), low), vmem((rows, width), full_type), vmem((rows, width), low), vmem((rows, width), low),
            vmem((rows, 3 * width), low), vmem((rows + 2 * rim, width), full_type), vmem((rows + 2 * rim, width), full_type),
            vmem((layers, 2, rim, 2 * width), low), vmem((layers, 2, rim, 2 * width), low),
            dma((layers + 1, 9)), dma((2, 3)), dma, dma((seqs,)), dma, dma, dma((seqs,)), dma, dma((layers, 2)), dma((layers, 2)),
        ] + (prefix_scratch(prefix.shape) if fast else []),
        compiler_params=pltpu.CompilerParams(collective_id=1, has_side_effects=True, vmem_limit_bytes=67043328),
    )(y_low, cot, full, w_qkv, w_out, q, k, v, unit, scale, slope, lse, hide, gains, prefix)


def local(
    tokens,
    segments,
    w_qkv,
    b_qkv,
    w_out,
    b_out,
    norm_gain,
    norm_bias,
    w_up,
    b_up,
    w_down,
    b_down,
    prefix,
    cotangent,
):
    seqs, tok, width = tokens.shape
    layers, rim, rows = w_qkv.shape[0], PAIR_MAX, seqs * tok
    wides = lax.axis_size("wide")
    fast = wides == 8 and lax.axis_size("rows") == 4
    parts = wides // seqs
    wide = lax.axis_index("wide")
    ids = jnp.pad(segments, ((0, 0), (rim, rim)), constant_values=-1)
    ids = lax.dynamic_slice(ids, (lax.div(wide, parts), lax.rem(wide, parts) * rows), (1, rows + 2 * rim))[0]
    hide = jnp.stack(
        [
            jnp.where(ids[b * tok : b * tok + tok + 2 * rim, None] == ids[None, b * tok + rim : b * tok + rim + tok], 0.0, -1e30)
            for b in range(seqs)
        ]
    )
    full_in = w_up
    if not fast:
        full_in = jnp.stack([lax.all_gather(w, "wide", axis=1, tiled=True) for w in (w_up, w_down)], axis=1)
    y_low, cot, full, q, k, v, unit, scale, slope, lse = forward(
        fast, tokens, cotangent, w_qkv, w_out, w_up, w_down, full_in, hide, b_qkv, b_out, norm_gain, norm_bias,
        b_up.astype(jnp.float32).reshape(1, -1), b_down, prefix,
    )
    output, grads, prefix_grads = backward(
        fast, y_low, cot, full if fast else full_in, w_qkv, w_out, q, k, v, unit, scale, slope, lse, hide, norm_gain, prefix, seqs
    )
    if not fast:
        prefix_grads = lax.psum(prefix_grads, ("rows", "wide"))
    return output, grads.astype(jnp.float32), prefix_grads


def solution(mesh):
    return jax.shard_map(
        local,
        mesh=mesh,
        in_specs=(
            P("rows", "wide", None),
            P("rows", None),
            P(),
            P(),
            P(),
            P(),
            P(),
            P(),
            P(None, "wide", None),
            P(None, "wide"),
            P(None, "wide", None),
            P(),
            P(),
            P("rows", "wide", None),
        ),
        out_specs=(P("rows", "wide", None), P("rows", "wide", None), P()),
        check_vma=False,
    )
```

```python
import functools
import math

import jax
import jax.numpy as jnp
from jax import lax
from jax.experimental import pallas as pl
from jax.experimental.pallas import tpu as pltpu
from jax.sharding import PartitionSpec as P

HEADS = 16
PAIR_MAX = 128
MESH = pl.DeviceIdType.MESH
LANES = 128
SPAN = 1024
ROOT_HALF = math.sqrt(0.5)


def multiply(left, right):
    return jnp.dot(left, right, preferred_element_type=jnp.float32)


def multiply_back(left, right):
    return lax.dot_general(left, right, (((1,), (1,)), ((), ())), preferred_element_type=jnp.float32)


def multiply_first(left, right):
    return lax.dot_general(left, right, (((0,), (0,)), ((), ())), preferred_element_type=jnp.float32)


def two_heads(rows):
    half = rows.shape[1] // 2
    lane = lax.broadcasted_iota(jnp.int32, rows.shape, 1)
    nothing = jnp.zeros_like(rows)
    return jnp.concatenate([jnp.where(lane < half, rows, nothing), jnp.where(lane >= half, rows, nothing)], axis=0)


def own_heads(columns):
    half, count = columns.shape[0] // 2, columns.shape[1] // 2
    place = lax.broadcasted_iota(jnp.int32, (columns.shape[0], count), 0)
    return jnp.where(place < half, columns[:, :count], columns[:, count:]).T


def attend(blocks, rows, rim, pair, q_ref, k_ref, v_ref, prefix_ref, hide_ref, context_ref, lse_ref):
    lanes = pl.ds(pl.multiple_of(pair * 128, 128), 128)
    prefix_keys, prefix_values = prefix_ref[0, :, lanes], prefix_ref[1, :, lanes]
    for block in range(blocks):
        here = pl.ds(block * rows, rows)
        window = pl.ds(block * rows, rows + 2 * rim)
        queries = two_heads(q_ref[here, lanes])
        hide = hide_ref[block]
        fixed = multiply_back(prefix_keys, queries)
        near = multiply_back(k_ref[window, lanes], queries) + jnp.concatenate([hide, hide], axis=1)
        top = jnp.maximum(jnp.max(fixed, axis=0, keepdims=True), jnp.max(near, axis=0, keepdims=True))
        fixed, near = jnp.exp(fixed - top), jnp.exp(near - top)
        total = jnp.sum(fixed, axis=0, keepdims=True) + jnp.sum(near, axis=0, keepdims=True)
        share = 1.0 / total
        columns = multiply_first(prefix_values, fixed.astype(jnp.bfloat16)) + multiply_first(
            v_ref[window, lanes], near.astype(jnp.bfloat16)
        )
        context_ref[here, lanes] = own_heads(columns * share).astype(jnp.bfloat16)
        lse_ref[pair * blocks + block] = top + jnp.log(total)


def attend_back(blocks, rows, rim, pair, q_ref, k_ref, v_ref, prefix_ref, hide_ref, lse_ref, grad_ref, dq_ref, dk_ref, dv_ref, dp_ref, scale):
    lanes = pl.ds(pl.multiple_of(pair * 128, 128), 128)
    prefix_keys, prefix_values = prefix_ref[0, :, lanes], prefix_ref[1, :, lanes]
    for block in range(blocks):
        here = pl.ds(block * rows, rows)
        window = pl.ds(block * rows, rows + 2 * rim)
        queries = two_heads(q_ref[here, lanes])
        grads = two_heads(grad_ref[here, lanes])
        hide = hide_ref[block]
        keys, values = k_ref[window, lanes], v_ref[window, lanes]
        lse = lse_ref[pair * blocks + block]
        fixed = jnp.exp(multiply_back(prefix_keys, queries) - lse)
        near = jnp.exp(multiply_back(keys, queries) + jnp.concatenate([hide, hide], axis=1) - lse)
        grad_fixed = multiply_back(prefix_values, grads)
        grad_near = multiply_back(values, grads)
        dots = jnp.sum(fixed * grad_fixed, axis=0, keepdims=True) + jnp.sum(near * grad_near, axis=0, keepdims=True)
        grad_fixed = (fixed * (grad_fixed - dots)).astype(jnp.bfloat16)
        grad_near = (near * (grad_near - dots)).astype(jnp.bfloat16)
        fixed, near = fixed.astype(jnp.bfloat16), near.astype(jnp.bfloat16)
        columns = multiply_first(prefix_keys, grad_fixed) + multiply_first(keys, grad_near)
        dq_ref[here, lanes] = (own_heads(columns) * scale).astype(jnp.bfloat16)
        new_keys, new_values = multiply(grad_near, queries), multiply(near, grads)
        fixed_keys, fixed_values = multiply(grad_fixed, queries), multiply(fixed, grads)
        old = pl.ds(block * rows, 2 * rim)
        fresh = pl.ds(block * rows + 2 * rim, rows)
        if block == 0:
            dk_ref[window, lanes], dv_ref[window, lanes] = new_keys, new_values
            dp_ref[0, :, lanes], dp_ref[1, :, lanes] = fixed_keys, fixed_values
        else:
            dk_ref[old, lanes] += new_keys[: 2 * rim]
            dv_ref[old, lanes] += new_values[: 2 * rim]
            dk_ref[fresh, lanes], dv_ref[fresh, lanes] = new_keys[2 * rim :], new_values[2 * rim :]
            dp_ref[0, :, lanes] += fixed_keys
            dp_ref[1, :, lanes] += fixed_values


def gelu_pair(values):
    size = jnp.abs(values) * ROOT_HALF
    bell = jnp.exp(values * values * -0.5)
    t = 1.0 / (1.0 + 0.3275911 * size)
    series = ((((1.061405429 * t - 1.453152027) * t + 1.421413741) * t - 0.284496736) * t + 0.254829592) * t
    tail = 0.5 * series * bell
    below = jnp.where(values < 0, tail, 1.0 - tail)
    return values * below, below + values * bell * (1.0 / math.sqrt(2.0 * math.pi))


def normalize(values):
    center = values - jnp.mean(values, axis=-1, keepdims=True)
    scale = lax.rsqrt(jnp.mean(center * center, axis=-1, keepdims=True) + 1e-05)
    return center * scale, scale


def norm_grad(grad, unit, scale, gain):
    inner = grad * gain
    first = jnp.mean(inner, axis=-1, keepdims=True)
    second = jnp.mean(inner * unit, axis=-1, keepdims=True)
    return scale * (inner - first - unit * second)


def each(count, step, body):
    @pl.loop(0, count)
    def _(i):
        body(pl.ds(pl.multiple_of(i * step, step), step))


class Place:
    def __init__(self, seqs, tok):
        self.seqs, self.tok, self.rows = seqs, tok, seqs * tok
        self.wide_size = lax.axis_size("wide")
        self.parts = self.wide_size // seqs
        self.row, self.wide = lax.axis_index("rows"), lax.axis_index("wide")
        self.seq, self.part = lax.div(self.wide, self.parts), lax.rem(self.wide, self.parts)

    def others(self, body):
        @pl.loop(1, self.wide_size)
        def _(step):
            body(lax.rem(self.wide + step, self.wide_size))

    def barrier(self, more):
        sem = pltpu.get_barrier_semaphore()
        self.others(lambda other: pl.semaphore_signal(sem, inc=1, device_id=(self.row, other), device_id_type=MESH))
        for device in more:
            pl.semaphore_signal(sem, inc=1, device_id=device, device_id_type=MESH)
        pl.semaphore_wait(sem, self.wide_size - 1 + len(more))

    def remote(self, src, dst, send, recv, device):
        return pltpu.make_async_remote_copy(
            src_ref=src, dst_ref=dst, send_sem=send, recv_sem=recv, device_id=device, device_id_type=MESH
        )

    def send_out(self, parts, target, send, recv, own):
        block = lax.rem(self.wide, self.seqs)
        for s in range(self.seqs):
            goal = s * self.parts + lax.div(self.wide, self.seqs)

            @pl.when(goal != self.wide)
            def _():
                self.remote(parts(s), target(block), send, recv.at[block], (self.row, goal)).start()

            @pl.when(goal == self.wide)
            def _():
                pltpu.make_async_copy(parts(s), target(block), own).start()

    def sent_out(self, parts, target, send, recv, own):
        block = lax.rem(self.wide, self.seqs)
        for s in range(self.seqs):
            goal = s * self.parts + lax.div(self.wide, self.seqs)

            @pl.when(goal != self.wide)
            def _():
                self.remote(parts(s), target(block), send, recv.at[block], (self.row, goal)).wait_send()

    def got_out(self, parts, target, send, recv, own):
        for b in range(self.seqs):
            source = self.part * self.seqs + b

            @pl.when(source != self.wide)
            def _():
                self.remote(parts(0), target(b), send, recv.at[b], (self.row, self.wide)).wait_recv()

            @pl.when(source == self.wide)
            def _():
                pltpu.make_async_copy(parts(0), target(b), own).wait()

    def send_home_block(self, b, part, target, send, recv, own):
        goal = self.part * self.seqs + b

        @pl.when(goal != self.wide)
        def _():
            self.remote(part, target(self.seq), send, recv.at[self.seq], (self.row, goal)).start()

        @pl.when(goal == self.wide)
        def _():
            pltpu.make_async_copy(part, target(self.seq), own).start()

    def sent_home(self, part, target, send, recv):
        for b in range(self.seqs):
            goal = self.part * self.seqs + b

            @pl.when(goal != self.wide)
            def _():
                self.remote(part, target(self.seq), send, recv.at[self.seq], (self.row, goal)).wait_send()

    def got_home(self, s, part, target, send, recv, own):
        source = s * self.parts + lax.div(self.wide, self.seqs)

        @pl.when(source != self.wide)
        def _():
            self.remote(part, target(s), send, recv.at[s], (self.row, self.wide)).wait_recv()

        @pl.when(source == self.wide)
        def _():
            pltpu.make_async_copy(part, target(s), own).wait()


class Gather:
    def __init__(self, shards, full, sems):
        self.shards = shards
        self.full = full
        self.send_sem, self.zs, self.xs, self.ys, self.ds, self.cz, self.cx, self.cy, self.cd, self.cown, self.own = sems
        self.row = lax.axis_index("rows")
        self.wide = lax.axis_index("wide")
        self.z, self.core = lax.div(self.wide, 2), lax.rem(self.wide, 2)
        self.shard_rows = shards[0].shape[1]
        self.unit_rows = self.shard_rows // 4
        self.row_x = self.row + 1 - 2 * lax.rem(self.row, 2)
        self.row_y = lax.rem(self.row + 2, 4)
        self.row_d = 3 - self.row

    def unit(self, layer, member, z, core, quarter):
        start = (z * 2 + core) * self.shard_rows + quarter * self.unit_rows
        return self.full.at[layer, member, pl.ds(pl.multiple_of(start, self.unit_rows), self.unit_rows)]

    def shard(self, layer, member, z, core):
        start = (z * 2 + core) * self.shard_rows
        return self.full.at[layer, member, pl.ds(pl.multiple_of(start, self.shard_rows), self.shard_rows)]

    def copy(self, src, dst, recv, kind):
        if kind == "x":
            device = (self.row_x, self.wide)
        elif kind == "y":
            device = (self.row_y, self.wide)
        elif kind == "core":
            device = (self.row, self.z * 2 + 1 - self.core)
        else:
            device = (self.row, self.wide + 2 - 4 * kind)
        return pltpu.make_async_remote_copy(
            src_ref=src, dst_ref=dst, send_sem=self.send_sem, recv_sem=recv, device_id=device, device_id_type=MESH
        )

    def start_z(self, layer):
        for member in range(2):
            start = pl.multiple_of(self.row * self.unit_rows, self.unit_rows)
            mine = self.shards[member].at[layer, pl.ds(start, self.unit_rows)]
            here = self.unit(layer, member, self.z, self.core, self.row)

            @pl.when(self.z < 3)
            def _():
                self.copy(mine, here, self.zs.at[layer, member, 0, 0], 0).start()

            @pl.when(self.z > 0)
            def _():
                self.copy(mine, here, self.zs.at[layer, member, 0, 1], 1).start()

    def start_core(self, layer):
        for member in range(2):
            place = self.shard(layer, member, self.z, self.core)
            pltpu.make_async_copy(self.shards[member].at[layer], place, self.own.at[layer, member]).start()
            self.copy(self.shards[member].at[layer], place, self.cown.at[layer, member], "core").start()

    def slot(self, i):
        near = jnp.minimum(self.z, 3 - self.z)
        far_side = 1 - lax.div(self.z, 2)
        both = jnp.minimum(lax.div(i, jnp.maximum(2 * near, 1)), 1) + (1 - jnp.minimum(near, 1))
        both = 1 - jnp.minimum(both, 1)
        step = both * lax.div(i, 2) + (1 - both) * (i - near)
        side = both * lax.rem(i, 2) + (1 - both) * far_side
        return step, side, self.z + (1 + step) * (2 * side - 1)

    def on_z(self, layer, i):
        step, side, origin = self.slot(i)
        for member in range(2):
            unit = self.unit(layer, member, origin, self.core, self.row)
            self.copy(unit, unit, self.zs.at[layer, member, step, side], "x").wait_recv()
            target = self.z + 1 - 2 * side

            @pl.when((target >= 0) & (target < 4))
            def _():
                self.copy(unit, unit, self.zs.at[layer, member, step + 1, side], side).start()

            self.copy(unit, unit, self.xs.at[layer, member, step, side], "x").start()
            self.copy(unit, unit, self.ys.at[layer, member, step, side], "y").start()
            self.copy(unit, unit, self.cz.at[layer, member, step, side], "core").start()

    def on_first(self, layer, _):
        self.on_z(layer, 0)

        @pl.when((self.z > 0) & (self.z < 3))
        def _():
            self.on_z(layer, 1)

    def on_second(self, layer, _):
        self.on_z(layer, 1 + jnp.minimum(self.z, 1) * jnp.minimum(3 - self.z, 1))

    def on_third(self, layer, _):
        @pl.when((self.z == 0) | (self.z == 3))
        def _():
            self.on_z(layer, 2)

    def on_xy(self, layer, i):
        step, side, origin = self.slot(i)
        for member in range(2):
            unit = self.unit(layer, member, origin, self.core, self.row_x)
            self.copy(unit, unit, self.xs.at[layer, member, step, side], "x").wait_recv()
            if member == 0:
                self.copy(unit, unit, self.ds.at[layer, member, step, side], "y").start()
            self.copy(unit, unit, self.cx.at[layer, member, step, side], "core").start()
            unit = self.unit(layer, member, origin, self.core, self.row_y)
            self.copy(unit, unit, self.ys.at[layer, member, step, side], "y").wait_recv()
            if member == 1:
                self.copy(unit, unit, self.ds.at[layer, member, step, side], "x").start()
            self.copy(unit, unit, self.cy.at[layer, member, step, side], "core").start()

    def on_d(self, layer, i):
        step, side, origin = self.slot(i)
        for member in range(2):
            unit = self.unit(layer, member, origin, self.core, self.row_d)
            self.copy(unit, unit, self.ds.at[layer, member, step, side], "x").wait_recv()
            self.copy(unit, unit, self.cd.at[layer, member, step, side], "core").start()

    def on_core(self, layer, i):
        step, side, origin = self.slot(i)
        for member in range(2):
            for sem, quarter in ((self.cz, self.row), (self.cx, self.row_x), (self.cy, self.row_y), (self.cd, self.row_d)):
                unit = self.unit(layer, member, origin, 1 - self.core, quarter)
                self.copy(unit, unit, sem.at[layer, member, step, side], "core").wait_recv()

    def on_own(self, layer):
        for member in range(2):
            place = self.shard(layer, member, self.z, self.core)
            pltpu.make_async_copy(self.shards[member].at[layer], place, self.own.at[layer, member]).wait()
            place = self.shard(layer, member, self.z, 1 - self.core)
            self.copy(place, place, self.cown.at[layer, member], "core").wait_recv()

    def drain(self, layers):
        def wait(units):
            span = self.full.at[0, 0, pl.ds(0, units * self.unit_rows)]
            self.copy(span, span, self.own.at[0, 0], "core").wait_send()

        @pl.loop(0, layers)
        def _(layer):
            wait(8)

            @pl.when(self.z < 3)
            def _():
                wait(2)

            @pl.when(self.z > 0)
            def _():
                wait(2)

            @pl.loop(0, 3)
            def _(i):
                step, side, origin = self.slot(i)
                target = self.z + 1 - 2 * side

                @pl.when((target >= 0) & (target < 4))
                def _():
                    wait(2)

                wait(14)


class PrefixSum:
    def __init__(self, place, parts, inbox, planes, total, sems):
        self.parts, self.inbox, self.planes, self.total = parts, inbox, planes, total
        self.send_sem, self.in_sem, self.plane_sem, self.total_sem = sems
        self.row = place.row
        self.z, self.core = lax.div(place.wide, 2), lax.rem(place.wide, 2)
        self.me = self.row * 2 + self.core
        self.size = inbox.shape[2]

    def peers(self, body):
        @pl.loop(1, 8)
        def _(step):
            body(lax.rem(self.me + step, 8))

    def others(self):
        return [(lax.rem(self.row + step, 4), self.z * 2 + core) for step in range(1, 4) for core in range(2)]

    def piece(self, ref, layer, index):
        start = lax.rem(index, 4) * self.size
        return ref.at[layer, lax.div(index, 4), pl.ds(pl.multiple_of(start, self.size), self.size)]

    def copy(self, src, dst, recv, row, wide):
        return pltpu.make_async_remote_copy(
            src_ref=src, dst_ref=dst, send_sem=self.send_sem, recv_sem=recv, device_id=(row, wide), device_id_type=MESH
        )

    def in_copy(self, layer, peer, origin):
        return self.copy(
            self.piece(self.parts, layer, peer), self.inbox.at[layer, origin], self.in_sem.at[layer, origin],
            lax.div(peer, 2), self.z * 2 + lax.rem(peer, 2),
        )

    def plane_copy(self, layer, z, origin):
        place = self.planes.at[layer, origin]
        return self.copy(place, place, self.plane_sem.at[layer, origin], self.row, z * 2 + self.core)

    def total_copy(self, layer, peer, origin):
        place = self.piece(self.total, layer, origin)
        return self.copy(place, place, self.total_sem.at[layer, origin], lax.div(peer, 2), self.z * 2 + lax.rem(peer, 2))

    def planes_others(self, body):
        @pl.loop(1, 4)
        def _(step):
            body(lax.rem(self.z + step, 4))

    def start(self, layer):
        self.peers(lambda peer: self.in_copy(layer, peer, self.me).start())

    def middle(self, layer):
        self.peers(lambda peer: self.in_copy(layer, self.me, peer).wait_recv())
        value = self.piece(self.parts, layer, self.me)[...]
        for step in range(1, 8):
            value += self.inbox[layer, lax.rem(self.me + step, 8)]
        self.planes[layer, self.z] = value
        self.planes_others(lambda z: self.plane_copy(layer, z, self.z).start())

    def last(self, layer):
        self.planes_others(lambda z: self.plane_copy(layer, self.z, z).wait_recv())
        value = self.planes[layer, 0]
        for z in range(1, 4):
            value += self.planes[layer, z]
        self.piece(self.total, layer, self.me)[...] = value
        self.peers(lambda peer: self.total_copy(layer, peer, self.me).start())

    def finish(self, layer):
        self.peers(lambda peer: self.total_copy(layer, self.me, peer).wait_recv())
        self.peers(lambda peer: self.in_copy(layer, peer, self.me).wait_send())
        self.planes_others(lambda z: self.plane_copy(layer, z, self.z).wait_send())
        self.peers(lambda peer: self.total_copy(layer, peer, self.me).wait_send())


def prefix_scratch(shape):
    layers, members, count, width = shape
    size = members * count // 8
    dma = pltpu.SemaphoreType.DMA
    return [
        pltpu.VMEM(shape, jnp.float32), pltpu.VMEM((layers, 8, size, width), jnp.float32),
        pltpu.VMEM((layers, 4, size, width), jnp.float32), dma, dma((layers, 8)), dma((layers, 4)), dma((layers, 8)),
    ]


def gather_sems(layers):
    return (
        [pltpu.SemaphoreType.DMA]
        + [pltpu.SemaphoreType.DMA((layers, 2, 3, 2))] * 8
        + [pltpu.SemaphoreType.DMA((layers, 2))] * 2
    )


def forward_kernel(
    fast, seqs, tok, rim,
    tokens, cotangent, w_qkv, w_out, w_up, w_down, full_in,
    hide, b_qkv, b_out, gains, shifts, b_up, b_down, prefix,
    y_low, cot_out, full_out, q_out, k_out, v_out, unit_out, scale_out, slope_out, lse_out,
    full, wqkv, wout, x, low, acc, q, k, v, halo, context, slope, unit1, unit2, scale1, scale2, lse, bias,
    load_sem, store_sem, slope_sem, full_sem, tok_send, tok_recv, tok_own, cot_send, cot_recv, cot_own,
    halo_send, halo_recv, bias_send, bias_recv, bias_own,
    *gather_sem,
):
    layers, width = w_qkv.shape[0], tokens.shape[2]
    place = Place(seqs, tok)
    rows = place.rows
    gather = Gather((w_up, w_down), full, gather_sem) if fast else None
    place.barrier(((gather.row_x, place.wide), (gather.row_y, place.wide)) if fast else ())
    own_bias = bias.at[place.wide]

    def load(layer):
        return (
            pltpu.make_async_copy(w_qkv.at[layer], wqkv, load_sem.at[0]),
            pltpu.make_async_copy(w_out.at[layer], wout, load_sem.at[1]),
        )

    def put_bias(other):
        return place.remote(b_up, own_bias, bias_send, bias_recv.at[place.wide], (place.row, other))

    def got_bias(other):
        return place.remote(b_up, bias.at[other], bias_send, bias_recv.at[other], (place.row, other))

    if fast:
        gather.start_z(0)
        gather.start_core(0)
    else:
        pltpu.make_async_copy(full_in, full, full_sem.at[0]).start()
    for copy in load(0):
        copy.start()
    place.others(lambda other: put_bias(other).start())
    pltpu.make_async_copy(b_up, own_bias, bias_own).start()

    tok_args = (lambda s: tokens.at[s], lambda b: low.at[pl.ds(pl.multiple_of(b * tok, tok), tok)], tok_send, tok_recv, tok_own)
    cot_args = (lambda s: cotangent.at[s], lambda b: cot_out.at[pl.ds(pl.multiple_of(b * tok, tok), tok)], cot_send, cot_recv, cot_own)
    events = {}
    if fast:
        gather.on_first(0, 0)
        place.send_out(*tok_args)
        gather.on_second(0, 0)
        gather.on_xy(0, 0)
        events = {
            (0, "queries"): [(gather.on_xy, 0, 1)],
            (0, "pair", 1): [(gather.on_third, 0, 0)],
            (0, "pair", 4): [(gather.on_first, 1, 0), (gather.on_d, 0, 0)],
            (0, "projected"): [(gather.on_d, 0, 1)],
            (0, "normed"): [(gather.on_xy, 0, 2)],
            (0, "step", 1): [(gather.on_core, 0, 0)],
            (0, "step", 2): [(gather.on_second, 1, 0), (gather.on_core, 0, 1), (gather.on_d, 0, 2)],
            (0, "step", 3): [(gather.on_core, 0, 2)],
            (0, "done"): [(gather.on_xy, 1, 0), (gather.on_third, 1, 0)],
            (1, "pair", 4): [(gather.on_xy, 1, 1)],
            (1, "projected"): [(gather.on_d, 1, 0)],
            (1, "normed"): [(gather.on_d, 1, 1)],
            (1, "step", 1): [(gather.on_xy, 1, 2), (gather.on_core, 1, 0)],
            (1, "step", 2): [(gather.on_d, 1, 2), (gather.on_core, 1, 1)],
            (1, "step", 3): [(gather.on_core, 1, 2)],
        }
    else:
        place.send_out(*tok_args)

    def tick(*when):
        for event, layer, i in events.get(when, ()):
            event(layer, i)

    def loop_tick(layer, kind, index, count):
        for n in range(count):
            if (layer, kind, n) in events:
                @pl.when(index == n)
                def _():
                    tick(layer, kind, n)

    blank = jnp.zeros((rim, width), jnp.bfloat16)

    @pl.when(place.part == 0)
    def _():
        k[pl.ds(0, rim)] = blank
        v[pl.ds(0, rim)] = blank

    @pl.when(place.part == place.parts - 1)
    def _():
        k[pl.ds(rim + rows, rim)] = blank
        v[pl.ds(rim + rows, rim)] = blank

    place.got_out(*tok_args)
    if fast:
        gather.start_z(1)
        gather.start_core(1)

    def halo_copy(layer, member, side, wide):
        ref = (k, v)[member]
        return place.remote(
            ref.at[pl.ds((rows, rim)[side], rim)], halo.at[layer, member, side],
            halo_send.at[member, side], halo_recv.at[layer, member, side], (place.row, wide),
        )

    def halos(body, to):
        for side in range(2):
            @pl.when(place.part < place.parts - 1 if (side == 0) == to else place.part > 0)
            def _():
                for member in range(2):
                    body(member, side, jnp.clip(place.wide + (1 - 2 * side), 0, place.wide_size - 1))

    def got_halo(layer, member, side, wide):
        halo_copy(layer, member, side, place.wide).wait_recv()
        (k, v)[member][pl.ds((0, rim + rows)[side], rim)] = halo[layer, member, side]

    def kept(layer):
        return [
            pltpu.make_async_copy(src, dst.at[layer], store_sem.at[i])
            for i, (src, dst) in enumerate(((q, q_out), (k, k_out), (v, v_out)))
        ]

    def kept_norm(layer, which):
        unit, scale = ((unit1, scale1), (unit2, scale2))[which]
        return [
            pltpu.make_async_copy(unit, unit_out.at[layer, which], store_sem.at[3 + which]),
            pltpu.make_async_copy(scale, scale_out.at[layer, which], store_sem.at[5 + which]),
        ]

    half = width // 2
    for layer in range(layers):
        if layer > 0:
            for copy in kept(layer - 1) + kept_norm(layer - 1, 0) + kept_norm(layer - 1, 1):
                copy.wait()
        load(layer)[0].wait()
        for part in (2, 3, 4, 5, 0, 1):
            lanes = pl.ds(part * half, half)
            made = multiply(low[...], wqkv[:, lanes]) + b_qkv[layer : layer + 1, lanes]
            kind, side = part // 2, pl.ds((part % 2) * half, half)
            if kind == 0:
                q[:, side] = made.astype(jnp.bfloat16) * (1.0 / math.sqrt(width // HEADS))
            else:
                (k, v)[kind - 1][pl.ds(rim, rows), side] = made.astype(jnp.bfloat16)
            if part == 5:
                halos(lambda *at: halo_copy(layer, *at).start(), True)
        if layer + 1 < layers:
            load(layer + 1)[0].start()
        tick(layer, "queries")
        halos(lambda *at: got_halo(layer, *at), False)
        halos(lambda *at: halo_copy(layer, *at).wait_send(), True)
        for copy in kept(layer):
            copy.start()

        @pl.loop(0, width // LANES)
        def _(pair):
            attend(seqs, tok, rim, pair, q, k, v, prefix.at[layer], hide, context, lse.at[layer])
            loop_tick(layer, "pair", pair, width // LANES)

        load(layer)[1].wait()
        for part in range(2):
            lanes = pl.ds(part * half, half)
            acc[:, lanes] = multiply(context[...], wout[:, lanes])
        if layer + 1 < layers:
            load(layer + 1)[1].start()
        tick(layer, "projected")

        def first_norm(at):
            before = low[at].astype(jnp.float32) if layer == 0 else x[at]
            unit, scale = normalize(before + acc[at] + b_out[layer : layer + 1])
            unit1[at] = unit.astype(jnp.bfloat16)
            scale1[at] = jnp.broadcast_to(scale, (scale.shape[0], LANES))
            normed = unit * gains[layer, :1] + shifts[layer, :1]
            low[at] = normed.astype(jnp.bfloat16)
            acc[at] = normed + b_down[layer : layer + 1]

        each(rows // 64, 64, first_norm)
        for copy in kept_norm(layer, 0):
            copy.start()
        tick(layer, "normed")
        if layer == 0:
            pltpu.make_async_copy(b_up, own_bias, bias_own).wait()
            place.others(lambda other: got_bias(other).wait_recv())

            place.others(lambda other: put_bias(other).wait_send())
            if not fast:
                pltpu.make_async_copy(full_in, full, full_sem.at[0]).wait()

        hidden = b_up.shape[1] // layers

        @pl.loop(0, full.shape[2] // SPAN)
        def _(i):
            spot = i
            if fast:
                @pl.when(i == 0)
                def _():
                    gather.on_own(layer)

                loop_tick(layer, "step", i, full.shape[2] // SPAN)
                origin = gather.slot(jnp.maximum(i - 1, 0))[2]
                started = jnp.minimum(i, 1)
                spot = started * origin + (1 - started) * gather.z
            units = pl.ds(pl.multiple_of(spot * SPAN, SPAN), SPAN)
            slot = lax.rem(i, 2)
            step_bias = jnp.concatenate(
                [bias[spot * (SPAN // hidden) + n, :, pl.ds(layer * hidden, hidden)] for n in range(SPAN // hidden)], axis=1
            )

            @pl.when(i > 1)
            def _():
                pltpu.make_async_copy(slope.at[slot], slope_out.at[layer, spot], slope_sem.at[slot]).wait()

            for part in range(2):
                at = pl.ds(part * (rows // 2), rows // 2)
                act, rise = gelu_pair(multiply_back(low[at], full[layer, 0, units]) + step_bias)
                slope[slot, at] = rise.astype(jnp.bfloat16)
                acc[at] += multiply(act.astype(jnp.bfloat16), full[layer, 1, units])
            pltpu.make_async_copy(slope.at[slot], slope_out.at[layer, spot], slope_sem.at[slot]).start()
            if fast:
                pltpu.make_async_copy(full.at[layer, :, units], full_out.at[layer, :, units], full_sem.at[layer]).start()

        for slot in range(2):
            pltpu.make_async_copy(slope.at[slot], slope_out.at[layer, 0], slope_sem.at[slot]).wait()

        def second_norm(at):
            unit, scale = normalize(acc[at])
            unit2[at] = unit.astype(jnp.bfloat16)
            scale2[at] = jnp.broadcast_to(scale, (scale.shape[0], LANES))
            after = unit * gains[layer, 1:] + shifts[layer, 1:]
            low[at] = after.astype(jnp.bfloat16)
            if layer + 1 < layers:
                x[at] = after

        each(rows // 64, 64, second_norm)
        for copy in kept_norm(layer, 1):
            copy.start()
        if layer == 0:
            place.send_out(*cot_args)
            tick(0, "done")
    last = [pltpu.make_async_copy(low, y_low, store_sem.at[7]), pltpu.make_async_copy(lse, lse_out, store_sem.at[8])]
    for copy in last:
        copy.start()
    place.sent_out(*tok_args)
    place.got_out(*cot_args)
    place.sent_out(*cot_args)
    for copy in last + kept(layers - 1) + kept_norm(layers - 1, 0) + kept_norm(layers - 1, 1):
        copy.wait()
    if fast:
        gather.drain(layers)
        for layer in range(layers):
            pltpu.make_async_copy(full.at[layer], full_out.at[layer], full_sem.at[layer]).wait()


def forward(fast, tokens, cotangent, w_qkv, w_out, w_up, w_down, full_in, hide, b_qkv, b_out, gains, shifts, b_up, b_down, prefix):
    seqs, tok, width = tokens.shape
    layers, rim, rows = w_qkv.shape[0], PAIR_MAX, seqs * tok
    wides = lax.axis_size("wide")
    units = w_up.shape[1] * wides
    low, full_type = jnp.bfloat16, jnp.float32
    spans = units // SPAN
    shape = jax.ShapeDtypeStruct
    dma = pltpu.SemaphoreType.DMA
    scores = (layers, width // LANES * seqs, 1, 2 * tok)
    return pl.pallas_call(
        functools.partial(forward_kernel, fast, seqs, tok, rim),
        out_shape=(
            shape((rows, width), low), shape((rows, width), low), shape((layers, 2, units, width), low),
            shape((layers, rows, width), low), shape((layers, rows + 2 * rim, width), low),
            shape((layers, rows + 2 * rim, width), low), shape((layers, 2, rows, width), low),
            shape((layers, 2, rows, LANES), full_type), shape((layers, spans, rows, SPAN), low), shape(scores, full_type),
        ),
        in_specs=[pl.BlockSpec(memory_space=pl.ANY)] * 7 + [pl.BlockSpec(memory_space=pltpu.VMEM)] * 8,
        out_specs=(pl.BlockSpec(memory_space=pl.ANY),) * 10,
        scratch_shapes=[
            pltpu.VMEM((layers, 2, units, width), low), pltpu.VMEM(w_qkv.shape[1:], low), pltpu.VMEM(w_out.shape[1:], low),
            pltpu.VMEM((rows, width), full_type), pltpu.VMEM((rows, width), low), pltpu.VMEM((rows, width), full_type),
            pltpu.VMEM((rows, width), low), pltpu.VMEM((rows + 2 * rim, width), low), pltpu.VMEM((rows + 2 * rim, width), low),
            pltpu.VMEM((layers, 2, 2, rim, width), low), pltpu.VMEM((rows, width), low), pltpu.VMEM((2, rows, SPAN), low),
            pltpu.VMEM((rows, width), low), pltpu.VMEM((rows, width), low),
            pltpu.VMEM((rows, LANES), full_type), pltpu.VMEM((rows, LANES), full_type),
            pltpu.VMEM(scores, full_type), pltpu.VMEM((wides,) + b_up.shape, full_type),
            dma((2,)), dma((9,)), dma((2,)), dma((layers,)), dma, dma((seqs,)), dma, dma, dma((seqs,)), dma,
            dma((2, 2)), dma((layers, 2, 2)), dma, dma((wides,)), dma,
        ] + (gather_sems(layers) if fast else []),
        compiler_params=pltpu.CompilerParams(collective_id=0, has_side_effects=True, vmem_limit_bytes=67043328),
    )(tokens, cotangent, w_qkv, w_out, w_up, w_down, full_in, hide, b_qkv, b_out, gains, shifts, b_up, b_down, prefix)


def backward_kernel(
    fast, seqs, tok, rim,
    y_low, cot_in, full, w_qkv, w_out, q_in, k_in, v_in, unit_in, scale_in, slope_in,
    lse, hide, gains, prefix,
    out, grads, prefix_grads,
    wqkv, wout, q, k, v, unit1, unit2, scale1, scale2, up, down, slope, cot, acc, low, context, made, dk, dv, edge, edge_in,
    load_sem, ffn_sem, out_send, out_recv, out_own, home_send, home_recv, home_own, edge_send, edge_recv,
    *sums,
):
    layers, width = w_qkv.shape[0], w_qkv.shape[1]
    place = Place(seqs, tok)
    rows = place.rows
    prefix_sum, prefix_parts = None, prefix_grads
    if fast:
        prefix_parts = sums[0]
        prefix_sum = PrefixSum(place, *sums[:3], prefix_grads, sums[3:])
    place.barrier(prefix_sum.others() if fast else ())
    spans = slope_in.shape[1]

    def out_rows(b):
        return y_low.at[pl.ds(b * tok, tok)]

    out_args = (lambda s: out.at[s], out_send, out_recv)
    for b in range(seqs):
        place.send_home_block(b, out_rows(b), *out_args, out_own)

    cot_copy = pltpu.make_async_copy(cot_in, cot, load_sem.at[layers, 0])
    cot_copy.start()

    def loads(layer):
        pairs = (
            (unit_in.at[layer, 1], unit2), (scale_in.at[layer, 1], scale2), (unit_in.at[layer, 0], unit1),
            (scale_in.at[layer, 0], scale1), (w_out.at[layer], wout), (q_in.at[layer], q), (k_in.at[layer], k),
            (v_in.at[layer], v),
        )
        copies = [pltpu.make_async_copy(src, dst.at[layer % 2], load_sem.at[layer, i]) for i, (src, dst) in enumerate(pairs)]
        return copies + [pltpu.make_async_copy(w_qkv.at[layer], wqkv, load_sem.at[layer, 8])]

    def ffn_loads(layer, i):
        slot = lax.rem(i, 2)
        units = pl.ds(pl.multiple_of(i * SPAN, SPAN), SPAN)
        return [
            pltpu.make_async_copy(full.at[layer, 1, units], down.at[slot], ffn_sem.at[slot, 0]),
            pltpu.make_async_copy(slope_in.at[layer, i], slope.at[slot], ffn_sem.at[slot, 1]),
            pltpu.make_async_copy(full.at[layer, 0, units], up.at[slot], ffn_sem.at[slot, 2]),
        ]

    order = list(reversed(range(layers)))
    for copy in loads(order[0])[:2]:
        copy.start()
    for i in range(2):
        for copy in ffn_loads(order[0], i):
            copy.start()
    for copy in loads(order[0])[2:]:
        copy.start()
    half = width // 2
    for layer in order:
        here = layer % 2
        mine = loads(layer)
        if layer == order[0]:
            cot_copy.wait()
        if layer > 0:
            for copy in loads(layer - 1)[:8]:
                copy.start()
        if layer < order[0]:
            mine[8].start()
        mine[0].wait()
        mine[1].wait()

        def second_norm(at):
            grad = cot[at].astype(jnp.float32) if layer == order[0] else acc[at]
            grad = norm_grad(grad, unit2[here, at].astype(jnp.float32), scale2[here, at, :1], gains[layer, 1:])
            acc[at] = grad
            low[at] = grad.astype(jnp.bfloat16)

        each(rows // 64, 64, second_norm)

        @pl.loop(0, spans)
        def _(i):
            slot = lax.rem(i, 2)
            for copy in ffn_loads(layer, i):
                copy.wait()
            for part in range(2):
                at = pl.ds(part * (rows // 2), rows // 2)
                grad = multiply_back(low[at], down[slot]) * slope[slot, at].astype(jnp.float32)
                acc[at] += multiply(grad.astype(jnp.bfloat16), up[slot])

            @pl.when(i + 2 < spans)
            def _():
                for copy in ffn_loads(layer, i + 2):
                    copy.start()

        if layer > 0:
            for i in range(2):
                for copy in ffn_loads(layer - 1, i):
                    copy.start()
        mine[2].wait()
        mine[3].wait()

        def first_norm(at):
            grad = norm_grad(acc[at], unit1[here, at].astype(jnp.float32), scale1[here, at, :1], gains[layer, :1])
            acc[at] = grad
            low[at] = grad.astype(jnp.bfloat16)

        each(rows // 64, 64, first_norm)
        if fast and layer + 1 < layers:
            prefix_sum.last(layer + 1)
        mine[4].wait()
        for part in range(2):
            span = pl.ds(part * half, half)
            context[:, span] = multiply_back(low[...], wout[here, span]).astype(jnp.bfloat16)
        for copy in mine[5:8]:
            copy.wait()

        @pl.loop(0, width // LANES)
        def _(pair):
            attend_back(
                seqs, tok, rim, pair, q.at[here], k.at[here], v.at[here], prefix.at[layer], hide, lse.at[layer], context,
                made, dk, dv, prefix_parts.at[layer], 1.0 / math.sqrt(width // HEADS),
            )

        if fast:
            prefix_sum.start(layer)

        low_edge, high_edge, own_rows = pl.ds(0, rim), pl.ds(rim + rows, rim), pl.ds(rim, rows)
        for member, ref in enumerate((dk, dv)):
            lanes = pl.ds(member * width, width)
            edge[layer, 0, :, lanes] = ref[low_edge].astype(jnp.bfloat16)
            edge[layer, 1, :, lanes] = ref[high_edge].astype(jnp.bfloat16)

        def edge_copy(side, wide):
            return place.remote(
                edge.at[layer, side], edge_in.at[layer, side], edge_send.at[layer, side], edge_recv.at[layer, side], (place.row, wide)
            )

        mine[8].wait()
        for part in range(2):
            span = pl.ds(part * half, half)
            acc[:, span] += multiply_back(made[:, pl.ds(0, width)], wqkv[span, pl.ds(0, width)])
            if part == 0:
                @pl.when(place.part > 0)
                def _():
                    edge_copy(0, place.wide - 1).start()

                @pl.when(place.part < place.parts - 1)
                def _():
                    edge_copy(1, place.wide + 1).start()

        @pl.when(place.part < place.parts - 1)
        def _():
            edge_copy(0, place.wide).wait_recv()
            for member, ref in enumerate((dk, dv)):
                ref[pl.ds(rows, rim)] += edge_in[layer, 0, :, pl.ds(member * width, width)].astype(jnp.float32)

        @pl.when(place.part > 0)
        def _():
            edge_copy(1, place.wide).wait_recv()
            for member, ref in enumerate((dk, dv)):
                ref[pl.ds(rim, rim)] += edge_in[layer, 1, :, pl.ds(member * width, width)].astype(jnp.float32)

        for member, ref in enumerate((dk, dv)):
            def lower(at):
                made[at, pl.ds((1 + member) * width, width)] = ref[pl.ds(pl.multiple_of(at.start + rim, 64), 64)].astype(jnp.bfloat16)

            each(rows // 64, 64, lower)

        @pl.when(place.part > 0)
        def _():
            edge_copy(0, place.wide).wait_send()

        @pl.when(place.part < place.parts - 1)
        def _():
            edge_copy(1, place.wide).wait_send()

        if fast:
            prefix_sum.middle(layer)
        others = pl.ds(width, 2 * width)
        for part in range(2):
            span = pl.ds(part * half, half)
            acc[:, span] += multiply_back(made[:, others], wqkv[span, others])

    low[...] = acc[...].astype(jnp.bfloat16)
    home_args = (lambda s: grads.at[s], home_send, home_recv)
    for b in range(seqs):
        place.send_home_block(b, low.at[pl.ds(b * tok, tok)], *home_args, home_own)
    if fast:
        prefix_sum.last(0)
    for s in range(seqs):
        place.got_home(s, low.at[pl.ds(0, tok)], *home_args, home_own)
        place.got_home(s, out_rows(0), *out_args, out_own)
    place.sent_home(low.at[pl.ds(0, tok)], *home_args)
    place.sent_home(out_rows(0), *out_args)
    if fast:
        for layer in order:
            prefix_sum.finish(layer)


def backward(fast, y_low, cot, full, w_qkv, w_out, q, k, v, unit, scale, slope, lse, hide, gains, prefix, seqs):
    rows, width = y_low.shape
    layers, rim, tok = w_qkv.shape[0], PAIR_MAX, rows // seqs
    low, full_type = jnp.bfloat16, jnp.float32
    shape = jax.ShapeDtypeStruct
    dma = pltpu.SemaphoreType.DMA
    vmem = pltpu.VMEM
    return pl.pallas_call(
        functools.partial(backward_kernel, fast, seqs, tok, rim),
        out_shape=(shape((seqs, tok, width), low), shape((seqs, tok, width), low), shape(prefix.shape, full_type)),
        in_specs=[pl.BlockSpec(memory_space=pl.ANY)] * 11 + [pl.BlockSpec(memory_space=pltpu.VMEM)] * 4,
        out_specs=(pl.BlockSpec(memory_space=pl.ANY),) * 2 + (pl.BlockSpec(memory_space=pltpu.VMEM),),
        scratch_shapes=[
            vmem(w_qkv.shape[1:], low), vmem((2,) + w_out.shape[1:], low), vmem((2, rows, width), low),
            vmem((2, rows + 2 * rim, width), low), vmem((2, rows + 2 * rim, width), low),
            vmem((2, rows, width), low), vmem((2, rows, width), low), vmem((2, rows, LANES), full_type), vmem((2, rows, LANES), full_type),
            vmem((2, SPAN, width), low), vmem((2, SPAN, width), low), vmem((2, rows, SPAN), low),
            vmem((rows, width), low), vmem((rows, width), full_type), vmem((rows, width), low), vmem((rows, width), low),
            vmem((rows, 3 * width), low), vmem((rows + 2 * rim, width), full_type), vmem((rows + 2 * rim, width), full_type),
            vmem((layers, 2, rim, 2 * width), low), vmem((layers, 2, rim, 2 * width), low),
            dma((layers + 1, 9)), dma((2, 3)), dma, dma((seqs,)), dma, dma, dma((seqs,)), dma, dma((layers, 2)), dma((layers, 2)),
        ] + (prefix_scratch(prefix.shape) if fast else []),
        compiler_params=pltpu.CompilerParams(collective_id=1, has_side_effects=True, vmem_limit_bytes=67043328),
    )(y_low, cot, full, w_qkv, w_out, q, k, v, unit, scale, slope, lse, hide, gains, prefix)


def local(
    tokens,
    segments,
    w_qkv,
    b_qkv,
    w_out,
    b_out,
    norm_gain,
    norm_bias,
    w_up,
    b_up,
    w_down,
    b_down,
    prefix,
    cotangent,
):
    seqs, tok, width = tokens.shape
    layers, rim, rows = w_qkv.shape[0], PAIR_MAX, seqs * tok
    wides = lax.axis_size("wide")
    fast = wides == 8 and lax.axis_size("rows") == 4
    parts = wides // seqs
    wide = lax.axis_index("wide")
    ids = jnp.pad(segments, ((0, 0), (rim, rim)), constant_values=-1)
    ids = lax.dynamic_slice(ids, (lax.div(wide, parts), lax.rem(wide, parts) * rows), (1, rows + 2 * rim))[0]
    hide = jnp.stack(
        [
            jnp.where(ids[b * tok : b * tok + tok + 2 * rim, None] == ids[None, b * tok + rim : b * tok + rim + tok], 0.0, -1e30)
            for b in range(seqs)
        ]
    )
    full_in = w_up
    if not fast:
        full_in = jnp.stack([lax.all_gather(w, "wide", axis=1, tiled=True) for w in (w_up, w_down)], axis=1)
    y_low, cot, full, q, k, v, unit, scale, slope, lse = forward(
        fast, tokens, cotangent, w_qkv, w_out, w_up, w_down, full_in, hide, b_qkv, b_out, norm_gain, norm_bias,
        b_up.astype(jnp.float32).reshape(1, -1), b_down, prefix,
    )
    output, grads, prefix_grads = backward(
        fast, y_low, cot, full if fast else full_in, w_qkv, w_out, q, k, v, unit, scale, slope, lse, hide, norm_gain, prefix, seqs
    )
    if not fast:
        prefix_grads = lax.psum(prefix_grads, ("rows", "wide"))
    return output, grads.astype(jnp.float32), prefix_grads


def solution(mesh):
    return jax.shard_map(
        local,
        mesh=mesh,
        in_specs=(
            P("rows", "wide", None),
            P("rows", None),
            P(),
            P(),
            P(),
            P(),
            P(),
            P(),
            P(None, "wide", None),
            P(None, "wide"),
            P(None, "wide", None),
            P(),
            P(),
            P("rows", "wide", None),
        ),
        out_specs=(P("rows", "wide", None), P("rows", "wide", None), P()),
        check_vma=False,
    )
```

```python
import functools
import math

import jax
import jax.numpy as jnp
from jax import lax
from jax.experimental import pallas as pl
from jax.experimental.pallas import tpu as pltpu
from jax.sharding import PartitionSpec as P

HEADS = 16
PAIR_MAX = 128
MESH = pl.DeviceIdType.MESH
LANES = 128
SPAN = 1024
ROOT_HALF = math.sqrt(0.5)


def multiply(left, right):
    return jnp.dot(left, right, preferred_element_type=jnp.float32)


def multiply_back(left, right):
    return lax.dot_general(left, right, (((1,), (1,)), ((), ())), preferred_element_type=jnp.float32)


def multiply_first(left, right):
    return lax.dot_general(left, right, (((0,), (0,)), ((), ())), preferred_element_type=jnp.float32)


def two_heads(rows):
    half = rows.shape[1] // 2
    lane = lax.broadcasted_iota(jnp.int32, rows.shape, 1)
    nothing = jnp.zeros_like(rows)
    return jnp.concatenate([jnp.where(lane < half, rows, nothing), jnp.where(lane >= half, rows, nothing)], axis=0)


def own_heads(columns):
    half, count = columns.shape[0] // 2, columns.shape[1] // 2
    place = lax.broadcasted_iota(jnp.int32, (columns.shape[0], count), 0)
    return jnp.where(place < half, columns[:, :count], columns[:, count:]).T


def attend(blocks, rows, rim, pair, q_ref, k_ref, v_ref, prefix_ref, hide_ref, context_ref, lse_ref):
    lanes = pl.ds(pl.multiple_of(pair * 128, 128), 128)
    for block in range(blocks):
        here = pl.ds(block * rows, rows)
        window = pl.ds(block * rows, rows + 2 * rim)
        queries = two_heads(q_ref[here, lanes])
        hide = hide_ref[block]
        keys = jnp.concatenate([prefix_ref[0, :, lanes], k_ref[window, lanes]], axis=0)
        values = jnp.concatenate([prefix_ref[1, :, lanes], v_ref[window, lanes]], axis=0)
        scores = multiply_back(keys, queries) + jnp.concatenate([hide, hide], axis=1)
        top = jnp.max(scores, axis=0, keepdims=True)
        scores = jnp.exp(scores - top)
        total = jnp.sum(scores, axis=0, keepdims=True)
        share = 1.0 / total
        columns = multiply_first(values, scores.astype(jnp.bfloat16))
        context_ref[here, lanes] = own_heads(columns * share).astype(jnp.bfloat16)
        lse_ref[pair * blocks + block] = top + jnp.log(total)


def attend_back(
    blocks, rows, rim, pair, q_ref, k_ref, v_ref, prefix_ref, hide_ref, lse_ref, context_ref, grad_ref, dq_ref, dk_ref, dv_ref, dp_ref, scale
):
    lanes = pl.ds(pl.multiple_of(pair * 128, 128), 128)
    for block in range(blocks):
        here = pl.ds(block * rows, rows)
        grad = grad_ref[here, lanes]
        queries, grads = two_heads(q_ref[here, lanes]), two_heads(grad)
        shared = (grad.astype(jnp.float32) * context_ref[here, lanes].astype(jnp.float32)).T
        half = shared.shape[0] // 2
        dots = jnp.concatenate(
            [jnp.sum(shared[:half], axis=0, keepdims=True), jnp.sum(shared[half:], axis=0, keepdims=True)], axis=1
        )
        lse = lse_ref[pair * blocks + block]
        window = pl.ds(block * rows, rows + 2 * rim)
        keys = jnp.concatenate([prefix_ref[0, :, lanes], k_ref[window, lanes]], axis=0)
        values = jnp.concatenate([prefix_ref[1, :, lanes], v_ref[window, lanes]], axis=0)
        hide = hide_ref[block]
        probs = jnp.exp(multiply_back(keys, queries) + (jnp.concatenate([hide, hide], axis=1) - lse))
        grad_scores = (probs * (multiply_back(values, grads) - dots)).astype(jnp.bfloat16)
        new_values = multiply(probs.astype(jnp.bfloat16), grads)
        new_keys = multiply(grad_scores, queries)
        columns = multiply_first(keys, grad_scores)
        count = prefix_ref.shape[1]
        old, fresh = pl.ds(block * rows, 2 * rim), pl.ds(block * rows + 2 * rim, rows)
        if block == 0:
            dk_ref[window, lanes], dv_ref[window, lanes] = new_keys[count:], new_values[count:]
            dp_ref[0, :, lanes], dp_ref[1, :, lanes] = new_keys[:count], new_values[:count]
        else:
            dk_ref[old, lanes] += new_keys[count : count + 2 * rim]
            dv_ref[old, lanes] += new_values[count : count + 2 * rim]
            dk_ref[fresh, lanes], dv_ref[fresh, lanes] = new_keys[count + 2 * rim :], new_values[count + 2 * rim :]
            dp_ref[0, :, lanes] += new_keys[:count]
            dp_ref[1, :, lanes] += new_values[:count]
        dq_ref[here, lanes] = (own_heads(columns) * scale).astype(jnp.bfloat16)


def gelu_pair(values):
    size = jnp.abs(values) * ROOT_HALF
    bell = jnp.exp(values * values * -0.5)
    t = 1.0 / (1.0 + 0.3275911 * size)
    series = ((((1.061405429 * t - 1.453152027) * t + 1.421413741) * t - 0.284496736) * t + 0.254829592) * t
    tail = 0.5 * series * bell
    below = jnp.where(values < 0, tail, 1.0 - tail)
    return values * below, below + values * bell * (1.0 / math.sqrt(2.0 * math.pi))


def normalize(values):
    center = values - jnp.mean(values, axis=-1, keepdims=True)
    scale = lax.rsqrt(jnp.mean(center * center, axis=-1, keepdims=True) + 1e-05)
    return center * scale, scale


def norm_grad(grad, unit, scale, gain):
    inner = grad * gain
    first = jnp.mean(inner, axis=-1, keepdims=True)
    second = jnp.mean(inner * unit, axis=-1, keepdims=True)
    return scale * (inner - first - unit * second)


def each(count, step, body):
    @pl.loop(0, count)
    def _(i):
        body(pl.ds(pl.multiple_of(i * step, step), step))


class Place:
    def __init__(self, seqs, tok):
        self.seqs, self.tok, self.rows = seqs, tok, seqs * tok
        self.wide_size = lax.axis_size("wide")
        self.parts = self.wide_size // seqs
        self.row, self.wide = lax.axis_index("rows"), lax.axis_index("wide")
        self.seq, self.part = lax.div(self.wide, self.parts), lax.rem(self.wide, self.parts)

    def others(self, body):
        @pl.loop(1, self.wide_size)
        def _(step):
            body(lax.rem(self.wide + step, self.wide_size))

    def barrier(self, more):
        sem = pltpu.get_barrier_semaphore()
        self.others(lambda other: pl.semaphore_signal(sem, inc=1, device_id=(self.row, other), device_id_type=MESH))
        for device in more:
            pl.semaphore_signal(sem, inc=1, device_id=device, device_id_type=MESH)
        pl.semaphore_wait(sem, self.wide_size - 1 + len(more))

    def remote(self, src, dst, send, recv, device):
        return pltpu.make_async_remote_copy(
            src_ref=src, dst_ref=dst, send_sem=send, recv_sem=recv, device_id=device, device_id_type=MESH
        )

    def send_out(self, parts, target, send, recv, own):
        block = lax.rem(self.wide, self.seqs)
        for s in range(self.seqs):
            goal = s * self.parts + lax.div(self.wide, self.seqs)

            @pl.when(goal != self.wide)
            def _():
                self.remote(parts(s), target(block), send, recv.at[block], (self.row, goal)).start()

            @pl.when(goal == self.wide)
            def _():
                pltpu.make_async_copy(parts(s), target(block), own).start()

    def sent_out(self, parts, target, send, recv, own):
        block = lax.rem(self.wide, self.seqs)
        for s in range(self.seqs):
            goal = s * self.parts + lax.div(self.wide, self.seqs)

            @pl.when(goal != self.wide)
            def _():
                self.remote(parts(s), target(block), send, recv.at[block], (self.row, goal)).wait_send()

    def got_out(self, parts, target, send, recv, own):
        for b in range(self.seqs):
            source = self.part * self.seqs + b

            @pl.when(source != self.wide)
            def _():
                self.remote(parts(0), target(b), send, recv.at[b], (self.row, self.wide)).wait_recv()

            @pl.when(source == self.wide)
            def _():
                pltpu.make_async_copy(parts(0), target(b), own).wait()

    def send_home_block(self, b, part, target, send, recv, own):
        goal = self.part * self.seqs + b

        @pl.when(goal != self.wide)
        def _():
            self.remote(part, target(self.seq), send, recv.at[self.seq], (self.row, goal)).start()

        @pl.when(goal == self.wide)
        def _():
            pltpu.make_async_copy(part, target(self.seq), own).start()

    def sent_home(self, part, target, send, recv):
        for b in range(self.seqs):
            goal = self.part * self.seqs + b

            @pl.when(goal != self.wide)
            def _():
                self.remote(part, target(self.seq), send, recv.at[self.seq], (self.row, goal)).wait_send()

    def got_home(self, s, part, target, send, recv, own):
        source = s * self.parts + lax.div(self.wide, self.seqs)

        @pl.when(source != self.wide)
        def _():
            self.remote(part, target(s), send, recv.at[s], (self.row, self.wide)).wait_recv()

        @pl.when(source == self.wide)
        def _():
            pltpu.make_async_copy(part, target(s), own).wait()


class Gather:
    def __init__(self, shards, full, sems):
        self.shards = shards
        self.full = full
        self.send_sem, self.zs, self.xs, self.ys, self.ds, self.cz, self.cx, self.cy, self.cd, self.cown, self.own = sems
        self.row = lax.axis_index("rows")
        self.wide = lax.axis_index("wide")
        self.z, self.core = lax.div(self.wide, 2), lax.rem(self.wide, 2)
        self.shard_rows = shards[0].shape[1]
        self.unit_rows = self.shard_rows // 4
        self.row_x = self.row + 1 - 2 * lax.rem(self.row, 2)
        self.row_y = lax.rem(self.row + 2, 4)
        self.row_d = 3 - self.row

    def unit(self, layer, member, z, core, quarter):
        start = (z * 2 + core) * self.shard_rows + quarter * self.unit_rows
        return self.full.at[layer, member, pl.ds(pl.multiple_of(start, self.unit_rows), self.unit_rows)]

    def shard(self, layer, member, z, core):
        start = (z * 2 + core) * self.shard_rows
        return self.full.at[layer, member, pl.ds(pl.multiple_of(start, self.shard_rows), self.shard_rows)]

    def copy(self, src, dst, recv, kind):
        if kind == "x":
            device = (self.row_x, self.wide)
        elif kind == "y":
            device = (self.row_y, self.wide)
        elif kind == "core":
            device = (self.row, self.z * 2 + 1 - self.core)
        else:
            device = (self.row, self.wide + 2 - 4 * kind)
        return pltpu.make_async_remote_copy(
            src_ref=src, dst_ref=dst, send_sem=self.send_sem, recv_sem=recv, device_id=device, device_id_type=MESH
        )

    def start_z(self, layer):
        for member in range(2):
            start = pl.multiple_of(self.row * self.unit_rows, self.unit_rows)
            mine = self.shards[member].at[layer, pl.ds(start, self.unit_rows)]
            here = self.unit(layer, member, self.z, self.core, self.row)

            @pl.when(self.z < 3)
            def _():
                self.copy(mine, here, self.zs.at[layer, member, 0, 0], 0).start()

            @pl.when(self.z > 0)
            def _():
                self.copy(mine, here, self.zs.at[layer, member, 0, 1], 1).start()

    def start_core(self, layer):
        for member in range(2):
            place = self.shard(layer, member, self.z, self.core)
            pltpu.make_async_copy(self.shards[member].at[layer], place, self.own.at[layer, member]).start()
            self.copy(self.shards[member].at[layer], place, self.cown.at[layer, member], "core").start()

    def slot(self, i):
        near = jnp.minimum(self.z, 3 - self.z)
        far_side = 1 - lax.div(self.z, 2)
        both = jnp.minimum(lax.div(i, jnp.maximum(2 * near, 1)), 1) + (1 - jnp.minimum(near, 1))
        both = 1 - jnp.minimum(both, 1)
        step = both * lax.div(i, 2) + (1 - both) * (i - near)
        side = both * lax.rem(i, 2) + (1 - both) * far_side
        return step, side, self.z + (1 + step) * (2 * side - 1)

    def on_z(self, layer, i):
        step, side, origin = self.slot(i)
        for member in range(2):
            unit = self.unit(layer, member, origin, self.core, self.row)
            self.copy(unit, unit, self.zs.at[layer, member, step, side], "x").wait_recv()
            target = self.z + 1 - 2 * side

            @pl.when((target >= 0) & (target < 4))
            def _():
                self.copy(unit, unit, self.zs.at[layer, member, step + 1, side], side).start()

            self.copy(unit, unit, self.xs.at[layer, member, step, side], "x").start()
            self.copy(unit, unit, self.ys.at[layer, member, step, side], "y").start()
            self.copy(unit, unit, self.cz.at[layer, member, step, side], "core").start()

    def on_first(self, layer, _):
        self.on_z(layer, 0)

        @pl.when((self.z > 0) & (self.z < 3))
        def _():
            self.on_z(layer, 1)

    def on_second(self, layer, _):
        self.on_z(layer, 1 + jnp.minimum(self.z, 1) * jnp.minimum(3 - self.z, 1))

    def on_third(self, layer, _):
        @pl.when((self.z == 0) | (self.z == 3))
        def _():
            self.on_z(layer, 2)

    def on_xy(self, layer, i):
        step, side, origin = self.slot(i)
        for member in range(2):
            unit = self.unit(layer, member, origin, self.core, self.row_x)
            self.copy(unit, unit, self.xs.at[layer, member, step, side], "x").wait_recv()
            if member == 0:
                self.copy(unit, unit, self.ds.at[layer, member, step, side], "y").start()
            self.copy(unit, unit, self.cx.at[layer, member, step, side], "core").start()
            unit = self.unit(layer, member, origin, self.core, self.row_y)
            self.copy(unit, unit, self.ys.at[layer, member, step, side], "y").wait_recv()
            if member == 1:
                self.copy(unit, unit, self.ds.at[layer, member, step, side], "x").start()
            self.copy(unit, unit, self.cy.at[layer, member, step, side], "core").start()

    def on_d(self, layer, i):
        step, side, origin = self.slot(i)
        for member in range(2):
            unit = self.unit(layer, member, origin, self.core, self.row_d)
            self.copy(unit, unit, self.ds.at[layer, member, step, side], "x").wait_recv()
            self.copy(unit, unit, self.cd.at[layer, member, step, side], "core").start()

    def on_core(self, layer, i):
        step, side, origin = self.slot(i)
        for member in range(2):
            for sem, quarter in ((self.cz, self.row), (self.cx, self.row_x), (self.cy, self.row_y), (self.cd, self.row_d)):
                unit = self.unit(layer, member, origin, 1 - self.core, quarter)
                self.copy(unit, unit, sem.at[layer, member, step, side], "core").wait_recv()

    def on_own(self, layer):
        for member in range(2):
            place = self.shard(layer, member, self.z, self.core)
            pltpu.make_async_copy(self.shards[member].at[layer], place, self.own.at[layer, member]).wait()
            place = self.shard(layer, member, self.z, 1 - self.core)
            self.copy(place, place, self.cown.at[layer, member], "core").wait_recv()

    def drain(self, layers):
        def wait(units):
            span = self.full.at[0, 0, pl.ds(0, units * self.unit_rows)]
            self.copy(span, span, self.own.at[0, 0], "core").wait_send()

        @pl.loop(0, layers)
        def _(layer):
            wait(8)

            @pl.when(self.z < 3)
            def _():
                wait(2)

            @pl.when(self.z > 0)
            def _():
                wait(2)

            @pl.loop(0, 3)
            def _(i):
                step, side, origin = self.slot(i)
                target = self.z + 1 - 2 * side

                @pl.when((target >= 0) & (target < 4))
                def _():
                    wait(2)

                wait(14)


class PrefixSum:
    def __init__(self, place, parts, inbox, planes, total, sems):
        self.parts, self.inbox, self.planes, self.total = parts, inbox, planes, total
        self.send_sem, self.in_sem, self.plane_sem, self.total_sem = sems
        self.row = place.row
        self.z, self.core = lax.div(place.wide, 2), lax.rem(place.wide, 2)
        self.me = self.row * 2 + self.core
        self.size = inbox.shape[2]

    def peers(self, body):
        @pl.loop(1, 8)
        def _(step):
            body(lax.rem(self.me + step, 8))

    def others(self):
        return [(lax.rem(self.row + step, 4), self.z * 2 + core) for step in range(1, 4) for core in range(2)]

    def piece(self, ref, layer, index):
        start = lax.rem(index, 4) * self.size
        return ref.at[layer, lax.div(index, 4), pl.ds(pl.multiple_of(start, self.size), self.size)]

    def copy(self, src, dst, recv, row, wide):
        return pltpu.make_async_remote_copy(
            src_ref=src, dst_ref=dst, send_sem=self.send_sem, recv_sem=recv, device_id=(row, wide), device_id_type=MESH
        )

    def in_copy(self, layer, peer, origin):
        return self.copy(
            self.piece(self.parts, layer, peer), self.inbox.at[layer, origin], self.in_sem.at[layer, origin],
            lax.div(peer, 2), self.z * 2 + lax.rem(peer, 2),
        )

    def plane_copy(self, layer, z, origin):
        place = self.planes.at[layer, origin]
        return self.copy(place, place, self.plane_sem.at[layer, origin], self.row, z * 2 + self.core)

    def total_copy(self, layer, peer, origin):
        place = self.piece(self.total, layer, origin)
        return self.copy(place, place, self.total_sem.at[layer, origin], lax.div(peer, 2), self.z * 2 + lax.rem(peer, 2))

    def planes_others(self, body):
        @pl.loop(1, 4)
        def _(step):
            body(lax.rem(self.z + step, 4))

    def start(self, layer):
        self.peers(lambda peer: self.in_copy(layer, peer, self.me).start())

    def middle(self, layer):
        self.peers(lambda peer: self.in_copy(layer, self.me, peer).wait_recv())
        value = self.piece(self.parts, layer, self.me)[...]
        for step in range(1, 8):
            value += self.inbox[layer, lax.rem(self.me + step, 8)]
        self.planes[layer, self.z] = value
        self.planes_others(lambda z: self.plane_copy(layer, z, self.z).start())

    def last(self, layer):
        self.planes_others(lambda z: self.plane_copy(layer, self.z, z).wait_recv())
        value = self.planes[layer, 0]
        for z in range(1, 4):
            value += self.planes[layer, z]
        self.piece(self.total, layer, self.me)[...] = value
        self.peers(lambda peer: self.total_copy(layer, peer, self.me).start())

    def finish(self, layer):
        self.peers(lambda peer: self.total_copy(layer, self.me, peer).wait_recv())
        self.peers(lambda peer: self.in_copy(layer, peer, self.me).wait_send())
        self.planes_others(lambda z: self.plane_copy(layer, z, self.z).wait_send())
        self.peers(lambda peer: self.total_copy(layer, peer, self.me).wait_send())


def prefix_scratch(shape):
    layers, members, count, width = shape
    size = members * count // 8
    dma = pltpu.SemaphoreType.DMA
    return [
        pltpu.VMEM(shape, jnp.float32), pltpu.VMEM((layers, 8, size, width), jnp.float32),
        pltpu.VMEM((layers, 4, size, width), jnp.float32), dma, dma((layers, 8)), dma((layers, 4)), dma((layers, 8)),
    ]


def gather_sems(layers):
    return (
        [pltpu.SemaphoreType.DMA]
        + [pltpu.SemaphoreType.DMA((layers, 2, 3, 2))] * 8
        + [pltpu.SemaphoreType.DMA((layers, 2))] * 2
    )


def forward_kernel(
    fast, seqs, tok, rim,
    tokens, cotangent, w_qkv, w_out, w_up, w_down, full_in,
    hide, b_qkv, b_out, gains, shifts, b_up, b_down, prefix,
    y_low, cot_out, full_out, q_out, k_out, v_out, unit_out, scale_out, slope_out, lse_out, context_out,
    full, wqkv, wout, x, low, acc, q, k, v, halo, context, slope, unit1, unit2, scale1, scale2, lse, bias,
    load_sem, store_sem, slope_sem, full_sem, tok_send, tok_recv, tok_own, cot_send, cot_recv, cot_own,
    halo_send, halo_recv, bias_send, bias_recv, bias_own,
    *gather_sem,
):
    layers, width = w_qkv.shape[0], tokens.shape[2]
    place = Place(seqs, tok)
    rows = place.rows
    gather = Gather((w_up, w_down), full, gather_sem) if fast else None
    place.barrier(((gather.row_x, place.wide), (gather.row_y, place.wide)) if fast else ())
    own_bias = bias.at[place.wide]

    def load(layer):
        return (
            pltpu.make_async_copy(w_qkv.at[layer], wqkv, load_sem.at[0]),
            pltpu.make_async_copy(w_out.at[layer], wout, load_sem.at[1]),
        )

    def put_bias(other):
        return place.remote(b_up, own_bias, bias_send, bias_recv.at[place.wide], (place.row, other))

    def got_bias(other):
        return place.remote(b_up, bias.at[other], bias_send, bias_recv.at[other], (place.row, other))

    if fast:
        gather.start_z(0)
        gather.start_core(0)
    else:
        pltpu.make_async_copy(full_in, full, full_sem.at[0]).start()
    for copy in load(0):
        copy.start()
    place.others(lambda other: put_bias(other).start())
    pltpu.make_async_copy(b_up, own_bias, bias_own).start()

    tok_args = (lambda s: tokens.at[s], lambda b: low.at[pl.ds(pl.multiple_of(b * tok, tok), tok)], tok_send, tok_recv, tok_own)
    cot_args = (lambda s: cotangent.at[s], lambda b: cot_out.at[pl.ds(pl.multiple_of(b * tok, tok), tok)], cot_send, cot_recv, cot_own)
    events = {}
    if fast:
        gather.on_first(0, 0)
        place.send_out(*tok_args)
        gather.on_second(0, 0)
        gather.on_xy(0, 0)
        events = {
            (0, "queries"): [(gather.on_third, 0, 0)],
            (0, "pair", 1): [(gather.on_xy, 0, 1)],
            (0, "pair", 4): [(gather.on_first, 1, 0), (gather.on_d, 0, 0)],
            (0, "pair", 7): [(gather.on_xy, 0, 2)],
            (0, "projected"): [(gather.on_d, 0, 1)],
            (0, "normed"): [(gather.on_second, 1, 0)],
            (0, "step", 1): [(gather.on_core, 0, 0)],
            (0, "step", 2): [(gather.on_xy, 1, 0), (gather.on_core, 0, 1), (gather.on_d, 0, 2)],
            (0, "step", 3): [(gather.on_core, 0, 2), (gather.on_third, 1, 0)],
            (1, "pair", 2): [(gather.on_xy, 1, 1)],
            (1, "projected"): [(gather.on_d, 1, 0)],
            (1, "normed"): [(gather.on_d, 1, 1), (gather.on_xy, 1, 2)],
            (1, "step", 1): [(gather.on_core, 1, 0)],
            (1, "step", 2): [(gather.on_d, 1, 2), (gather.on_core, 1, 1)],
            (1, "step", 3): [(gather.on_core, 1, 2)],
        }
    else:
        place.send_out(*tok_args)

    def tick(*when):
        for event, layer, i in events.get(when, ()):
            event(layer, i)

    def loop_tick(layer, kind, index, count):
        for n in range(count):
            if (layer, kind, n) in events:
                @pl.when(index == n)
                def _():
                    tick(layer, kind, n)

    blank = jnp.zeros((rim, width), jnp.bfloat16)

    @pl.when(place.part == 0)
    def _():
        k[pl.ds(0, rim)] = blank
        v[pl.ds(0, rim)] = blank

    @pl.when(place.part == place.parts - 1)
    def _():
        k[pl.ds(rim + rows, rim)] = blank
        v[pl.ds(rim + rows, rim)] = blank

    place.got_out(*tok_args)
    if fast:
        gather.start_z(1)
        gather.start_core(1)

    def halo_copy(layer, member, side, wide):
        ref = (k, v)[member]
        return place.remote(
            ref.at[pl.ds((rows, rim)[side], rim)], halo.at[layer, member, side],
            halo_send.at[member, side], halo_recv.at[layer, member, side], (place.row, wide),
        )

    def halos(body, to):
        for side in range(2):
            @pl.when(place.part < place.parts - 1 if (side == 0) == to else place.part > 0)
            def _():
                for member in range(2):
                    body(member, side, jnp.clip(place.wide + (1 - 2 * side), 0, place.wide_size - 1))

    def got_halo(layer, member, side, wide):
        halo_copy(layer, member, side, place.wide).wait_recv()
        (k, v)[member][pl.ds((0, rim + rows)[side], rim)] = halo[layer, member, side]

    def kept(layer):
        return [
            pltpu.make_async_copy(src, dst.at[layer], store_sem.at[i])
            for i, (src, dst) in enumerate(((q, q_out), (k, k_out), (v, v_out)))
        ]

    def kept_context(layer):
        return [pltpu.make_async_copy(context, context_out.at[layer], store_sem.at[9])]

    def kept_norm(layer, which):
        unit, scale = ((unit1, scale1), (unit2, scale2))[which]
        return [
            pltpu.make_async_copy(unit, unit_out.at[layer, which], store_sem.at[3 + which]),
            pltpu.make_async_copy(scale, scale_out.at[layer, which], store_sem.at[5 + which]),
        ]

    half = width // 2
    for layer in range(layers):
        if layer > 0:
            for copy in kept(layer - 1) + kept_context(layer - 1) + kept_norm(layer - 1, 0) + kept_norm(layer - 1, 1):
                copy.wait()
        load(layer)[0].wait()
        for part in (2, 3, 4, 5, 0, 1):
            lanes = pl.ds(part * half, half)
            made = multiply(low[...], wqkv[:, lanes]) + b_qkv[layer : layer + 1, lanes]
            kind, side = part // 2, pl.ds((part % 2) * half, half)
            if kind == 0:
                q[:, side] = made.astype(jnp.bfloat16) * (1.0 / math.sqrt(width // HEADS))
            else:
                (k, v)[kind - 1][pl.ds(rim, rows), side] = made.astype(jnp.bfloat16)
            if part == 5:
                halos(lambda *at: halo_copy(layer, *at).start(), True)
        if layer + 1 < layers:
            load(layer + 1)[0].start()
        tick(layer, "queries")
        halos(lambda *at: got_halo(layer, *at), False)
        halos(lambda *at: halo_copy(layer, *at).wait_send(), True)
        for copy in kept(layer):
            copy.start()

        @pl.loop(0, width // LANES)
        def _(pair):
            attend(seqs, tok, rim, pair, q, k, v, prefix.at[layer], hide, context, lse.at[layer])
            loop_tick(layer, "pair", pair, width // LANES)

        for copy in kept_context(layer):
            copy.start()
        load(layer)[1].wait()
        for part in range(2):
            lanes = pl.ds(part * half, half)
            acc[:, lanes] = multiply(context[...], wout[:, lanes])
        if layer + 1 < layers:
            load(layer + 1)[1].start()
        tick(layer, "projected")

        def first_norm(at):
            before = low[at].astype(jnp.float32) if layer == 0 else x[at]
            unit, scale = normalize(before + acc[at] + b_out[layer : layer + 1])
            unit1[at] = unit.astype(jnp.bfloat16)
            scale1[at] = jnp.broadcast_to(scale, (scale.shape[0], LANES))
            normed = unit * gains[layer, :1] + shifts[layer, :1]
            low[at] = normed.astype(jnp.bfloat16)
            acc[at] = normed + b_down[layer : layer + 1]

        each(rows // 64, 64, first_norm)
        for copy in kept_norm(layer, 0):
            copy.start()
        tick(layer, "normed")
        if layer == 0:
            pltpu.make_async_copy(b_up, own_bias, bias_own).wait()
            place.others(lambda other: got_bias(other).wait_recv())

            place.others(lambda other: put_bias(other).wait_send())
            if not fast:
                pltpu.make_async_copy(full_in, full, full_sem.at[0]).wait()

        hidden = b_up.shape[1] // layers

        @pl.loop(0, full.shape[2] // SPAN)
        def _(i):
            spot = i
            if fast:
                @pl.when(i == 0)
                def _():
                    gather.on_own(layer)

                loop_tick(layer, "step", i, full.shape[2] // SPAN)
                origin = gather.slot(jnp.maximum(i - 1, 0))[2]
                started = jnp.minimum(i, 1)
                spot = started * origin + (1 - started) * gather.z
            units = pl.ds(pl.multiple_of(spot * SPAN, SPAN), SPAN)
            slot = lax.rem(i, 2)
            step_bias = jnp.concatenate(
                [bias[spot * (SPAN // hidden) + n, :, pl.ds(layer * hidden, hidden)] for n in range(SPAN // hidden)], axis=1
            )

            @pl.when(i > 1)
            def _():
                pltpu.make_async_copy(slope.at[slot], slope_out.at[layer, spot], slope_sem.at[slot]).wait()

            for part in range(2):
                at = pl.ds(part * (rows // 2), rows // 2)
                act, rise = gelu_pair(multiply_back(low[at], full[layer, 0, units]) + step_bias)
                slope[slot, at] = rise.astype(jnp.bfloat16)
                acc[at] += multiply(act.astype(jnp.bfloat16), full[layer, 1, units])
            pltpu.make_async_copy(slope.at[slot], slope_out.at[layer, spot], slope_sem.at[slot]).start()
            if fast:
                pltpu.make_async_copy(full.at[layer, :, units], full_out.at[layer, :, units], full_sem.at[layer]).start()

        for slot in range(2):
            pltpu.make_async_copy(slope.at[slot], slope_out.at[layer, 0], slope_sem.at[slot]).wait()

        def second_norm(at):
            unit, scale = normalize(acc[at])
            unit2[at] = unit.astype(jnp.bfloat16)
            scale2[at] = jnp.broadcast_to(scale, (scale.shape[0], LANES))
            after = unit * gains[layer, 1:] + shifts[layer, 1:]
            low[at] = after.astype(jnp.bfloat16)
            if layer + 1 < layers:
                x[at] = after

        each(rows // 64, 64, second_norm)
        for copy in kept_norm(layer, 1):
            copy.start()
        if layer == 0:
            place.send_out(*cot_args)
            tick(0, "done")
    last = [pltpu.make_async_copy(low, y_low, store_sem.at[7]), pltpu.make_async_copy(lse, lse_out, store_sem.at[8])]
    for copy in last:
        copy.start()
    place.sent_out(*tok_args)
    place.got_out(*cot_args)
    place.sent_out(*cot_args)
    for copy in last + kept(layers - 1) + kept_context(layers - 1) + kept_norm(layers - 1, 0) + kept_norm(layers - 1, 1):
        copy.wait()
    if fast:
        gather.drain(layers)
        for layer in range(layers):
            pltpu.make_async_copy(full.at[layer], full_out.at[layer], full_sem.at[layer]).wait()


def forward(fast, tokens, cotangent, w_qkv, w_out, w_up, w_down, full_in, hide, b_qkv, b_out, gains, shifts, b_up, b_down, prefix):
    seqs, tok, width = tokens.shape
    layers, rim, rows = w_qkv.shape[0], PAIR_MAX, seqs * tok
    wides = lax.axis_size("wide")
    units = w_up.shape[1] * wides
    low, full_type = jnp.bfloat16, jnp.float32
    spans = units // SPAN
    shape = jax.ShapeDtypeStruct
    dma = pltpu.SemaphoreType.DMA
    scores = (layers, width // LANES * seqs, 1, 2 * tok)
    return pl.pallas_call(
        functools.partial(forward_kernel, fast, seqs, tok, rim),
        out_shape=(
            shape((rows, width), low), shape((rows, width), low), shape((layers, 2, units, width), low),
            shape((layers, rows, width), low), shape((layers, rows + 2 * rim, width), low),
            shape((layers, rows + 2 * rim, width), low), shape((layers, 2, rows, width), low),
            shape((layers, 2, rows, LANES), full_type), shape((layers, spans, rows, SPAN), low), shape(scores, full_type),
            shape((layers, rows, width), low),
        ),
        in_specs=[pl.BlockSpec(memory_space=pl.ANY)] * 7 + [pl.BlockSpec(memory_space=pltpu.VMEM)] * 8,
        out_specs=(pl.BlockSpec(memory_space=pl.ANY),) * 11,
        scratch_shapes=[
            pltpu.VMEM((layers, 2, units, width), low), pltpu.VMEM(w_qkv.shape[1:], low), pltpu.VMEM(w_out.shape[1:], low),
            pltpu.VMEM((rows, width), full_type), pltpu.VMEM((rows, width), low), pltpu.VMEM((rows, width), full_type),
            pltpu.VMEM((rows, width), low), pltpu.VMEM((rows + 2 * rim, width), low), pltpu.VMEM((rows + 2 * rim, width), low),
            pltpu.VMEM((layers, 2, 2, rim, width), low), pltpu.VMEM((rows, width), low), pltpu.VMEM((2, rows, SPAN), low),
            pltpu.VMEM((rows, width), low), pltpu.VMEM((rows, width), low),
            pltpu.VMEM((rows, LANES), full_type), pltpu.VMEM((rows, LANES), full_type),
            pltpu.VMEM(scores, full_type), pltpu.VMEM((wides,) + b_up.shape, full_type),
            dma((2,)), dma((10,)), dma((2,)), dma((layers,)), dma, dma((seqs,)), dma, dma, dma((seqs,)), dma,
            dma((2, 2)), dma((layers, 2, 2)), dma, dma((wides,)), dma,
        ] + (gather_sems(layers) if fast else []),
        compiler_params=pltpu.CompilerParams(collective_id=0, has_side_effects=True, vmem_limit_bytes=67043328),
    )(tokens, cotangent, w_qkv, w_out, w_up, w_down, full_in, hide, b_qkv, b_out, gains, shifts, b_up, b_down, prefix)


def backward_kernel(
    fast, seqs, tok, rim,
    y_low, cot_in, full, w_qkv, w_out, q_in, k_in, v_in, unit_in, scale_in, slope_in, context_in,
    lse, hide, gains, prefix,
    out, grads, prefix_grads,
    wqkv, wout, q, k, v, unit1, unit2, scale1, scale2, up, down, slope, cot, acc, low, context, made, dk, dv, edge, edge_in, saved,
    load_sem, ffn_sem, out_send, out_recv, out_own, home_send, home_recv, home_own, edge_send, edge_recv,
    *sums,
):
    layers, width = w_qkv.shape[0], w_qkv.shape[1]
    place = Place(seqs, tok)
    rows = place.rows
    prefix_sum, prefix_parts = None, prefix_grads
    if fast:
        prefix_parts = sums[0]
        prefix_sum = PrefixSum(place, *sums[:3], prefix_grads, sums[3:])
    place.barrier(prefix_sum.others() if fast else ())
    spans = slope_in.shape[1]

    def out_rows(b):
        return y_low.at[pl.ds(b * tok, tok)]

    out_args = (lambda s: out.at[s], out_send, out_recv)
    for b in range(seqs):
        place.send_home_block(b, out_rows(b), *out_args, out_own)

    cot_copy = pltpu.make_async_copy(cot_in, cot, load_sem.at[layers, 0])
    cot_copy.start()

    def loads(layer):
        pairs = (
            (unit_in.at[layer, 1], unit2), (scale_in.at[layer, 1], scale2), (unit_in.at[layer, 0], unit1),
            (scale_in.at[layer, 0], scale1), (w_out.at[layer], wout), (q_in.at[layer], q), (k_in.at[layer], k),
            (v_in.at[layer], v),
        )
        copies = [pltpu.make_async_copy(src, dst.at[layer % 2], load_sem.at[layer, i]) for i, (src, dst) in enumerate(pairs)]
        return copies + [
            pltpu.make_async_copy(w_qkv.at[layer], wqkv, load_sem.at[layer, 8]),
            pltpu.make_async_copy(context_in.at[layer], saved, load_sem.at[layer, 9]),
        ]

    def ffn_loads(layer, i):
        slot = lax.rem(i, 2)
        units = pl.ds(pl.multiple_of(i * SPAN, SPAN), SPAN)
        return [
            pltpu.make_async_copy(full.at[layer, 1, units], down.at[slot], ffn_sem.at[slot, 0]),
            pltpu.make_async_copy(slope_in.at[layer, i], slope.at[slot], ffn_sem.at[slot, 1]),
            pltpu.make_async_copy(full.at[layer, 0, units], up.at[slot], ffn_sem.at[slot, 2]),
        ]

    order = list(reversed(range(layers)))
    for copy in loads(order[0])[:2]:
        copy.start()
    for i in range(2):
        for copy in ffn_loads(order[0], i):
            copy.start()
    for copy in loads(order[0])[2:]:
        copy.start()
    half = width // 2
    for layer in order:
        here = layer % 2
        mine = loads(layer)
        if layer == order[0]:
            cot_copy.wait()
        if layer > 0:
            for copy in loads(layer - 1)[:8]:
                copy.start()
        if layer < order[0]:
            mine[8].start()
            mine[9].start()
        mine[0].wait()
        mine[1].wait()

        def second_norm(at):
            grad = cot[at].astype(jnp.float32) if layer == order[0] else acc[at]
            grad = norm_grad(grad, unit2[here, at].astype(jnp.float32), scale2[here, at, :1], gains[layer, 1:])
            acc[at] = grad
            low[at] = grad.astype(jnp.bfloat16)

        each(rows // 64, 64, second_norm)
        if fast and layer + 1 < layers:
            prefix_sum.middle(layer + 1)

        @pl.loop(0, spans)
        def _(i):
            slot = lax.rem(i, 2)
            for copy in ffn_loads(layer, i):
                copy.wait()
            for part in range(2):
                at = pl.ds(part * (rows // 2), rows // 2)
                grad = multiply_back(low[at], down[slot]) * slope[slot, at].astype(jnp.float32)
                acc[at] += multiply(grad.astype(jnp.bfloat16), up[slot])

            @pl.when(i + 2 < spans)
            def _():
                for copy in ffn_loads(layer, i + 2):
                    copy.start()

        if layer > 0:
            for i in range(2):
                for copy in ffn_loads(layer - 1, i):
                    copy.start()
        mine[2].wait()
        mine[3].wait()

        def first_norm(at):
            grad = norm_grad(acc[at], unit1[here, at].astype(jnp.float32), scale1[here, at, :1], gains[layer, :1])
            acc[at] = grad
            low[at] = grad.astype(jnp.bfloat16)

        each(rows // 64, 64, first_norm)
        if fast and layer + 1 < layers:
            prefix_sum.last(layer + 1)
        mine[4].wait()
        for part in range(2):
            span = pl.ds(part * half, half)
            context[:, span] = multiply_back(low[...], wout[here, span]).astype(jnp.bfloat16)
        for copy in mine[5:8] + mine[9:]:
            copy.wait()

        @pl.loop(0, width // LANES)
        def _(pair):
            attend_back(
                seqs, tok, rim, pair, q.at[here], k.at[here], v.at[here], prefix.at[layer], hide, lse.at[layer], saved, context,
                made, dk, dv, prefix_parts.at[layer], 1.0 / math.sqrt(width // HEADS),
            )

        if fast:
            prefix_sum.start(layer)

        low_edge, high_edge, own_rows = pl.ds(0, rim), pl.ds(rim + rows, rim), pl.ds(rim, rows)
        for member, ref in enumerate((dk, dv)):
            lanes = pl.ds(member * width, width)
            edge[layer, 0, :, lanes] = ref[low_edge].astype(jnp.bfloat16)
            edge[layer, 1, :, lanes] = ref[high_edge].astype(jnp.bfloat16)

        def edge_copy(side, wide):
            return place.remote(
                edge.at[layer, side], edge_in.at[layer, side], edge_send.at[layer, side], edge_recv.at[layer, side], (place.row, wide)
            )

        mine[8].wait()
        for part in range(2):
            span = pl.ds(part * half, half)
            acc[:, span] += multiply_back(made[:, pl.ds(0, width)], wqkv[span, pl.ds(0, width)])
            if part == 0:
                @pl.when(place.part > 0)
                def _():
                    edge_copy(0, place.wide - 1).start()

                @pl.when(place.part < place.parts - 1)
                def _():
                    edge_copy(1, place.wide + 1).start()

        @pl.when(place.part < place.parts - 1)
        def _():
            edge_copy(0, place.wide).wait_recv()
            for member, ref in enumerate((dk, dv)):
                ref[pl.ds(rows, rim)] += edge_in[layer, 0, :, pl.ds(member * width, width)].astype(jnp.float32)

        @pl.when(place.part > 0)
        def _():
            edge_copy(1, place.wide).wait_recv()
            for member, ref in enumerate((dk, dv)):
                ref[pl.ds(rim, rim)] += edge_in[layer, 1, :, pl.ds(member * width, width)].astype(jnp.float32)

        for member, ref in enumerate((dk, dv)):
            def lower(at):
                made[at, pl.ds((1 + member) * width, width)] = ref[pl.ds(pl.multiple_of(at.start + rim, 64), 64)].astype(jnp.bfloat16)

            each(rows // 64, 64, lower)

        @pl.when(place.part > 0)
        def _():
            edge_copy(0, place.wide).wait_send()

        @pl.when(place.part < place.parts - 1)
        def _():
            edge_copy(1, place.wide).wait_send()

        others = pl.ds(width, 2 * width)
        if layer > 0:
            for part in range(2):
                span = pl.ds(part * half, half)
                acc[:, span] += multiply_back(made[:, others], wqkv[span, others])

    home_args = (lambda s: grads.at[s], home_send, home_recv)
    for part in range(2):
        at = pl.ds(part * (rows // 2), rows // 2)
        low[at] = (acc[at] + multiply_back(made[at, others], wqkv[:, others])).astype(jnp.bfloat16)
        for b in range(part * (seqs // 2), (part + 1) * (seqs // 2)):
            place.send_home_block(b, low.at[pl.ds(b * tok, tok)], *home_args, home_own)
        if fast and part == 0:
            prefix_sum.middle(0)
    if fast:
        prefix_sum.last(0)
    for s in range(seqs):
        place.got_home(s, low.at[pl.ds(0, tok)], *home_args, home_own)
        place.got_home(s, out_rows(0), *out_args, out_own)
    place.sent_home(low.at[pl.ds(0, tok)], *home_args)
    place.sent_home(out_rows(0), *out_args)
    if fast:
        for layer in order:
            prefix_sum.finish(layer)


def backward(fast, y_low, cot, full, w_qkv, w_out, q, k, v, unit, scale, slope, context, lse, hide, gains, prefix, seqs):
    rows, width = y_low.shape
    layers, rim, tok = w_qkv.shape[0], PAIR_MAX, rows // seqs
    low, full_type = jnp.bfloat16, jnp.float32
    shape = jax.ShapeDtypeStruct
    dma = pltpu.SemaphoreType.DMA
    vmem = pltpu.VMEM
    return pl.pallas_call(
        functools.partial(backward_kernel, fast, seqs, tok, rim),
        out_shape=(shape((seqs, tok, width), low), shape((seqs, tok, width), low), shape(prefix.shape, full_type)),
        in_specs=[pl.BlockSpec(memory_space=pl.ANY)] * 12 + [pl.BlockSpec(memory_space=pltpu.VMEM)] * 4,
        out_specs=(pl.BlockSpec(memory_space=pl.ANY),) * 2 + (pl.BlockSpec(memory_space=pltpu.VMEM),),
        scratch_shapes=[
            vmem(w_qkv.shape[1:], low), vmem((2,) + w_out.shape[1:], low), vmem((2, rows, width), low),
            vmem((2, rows + 2 * rim, width), low), vmem((2, rows + 2 * rim, width), low),
            vmem((2, rows, width), low), vmem((2, rows, width), low), vmem((2, rows, LANES), full_type), vmem((2, rows, LANES), full_type),
            vmem((2, SPAN, width), low), vmem((2, SPAN, width), low), vmem((2, rows, SPAN), low),
            vmem((rows, width), low), vmem((rows, width), full_type), vmem((rows, width), low), vmem((rows, width), low),
            vmem((rows, 3 * width), low), vmem((rows + 2 * rim, width), full_type), vmem((rows + 2 * rim, width), full_type),
            vmem((layers, 2, rim, 2 * width), low), vmem((layers, 2, rim, 2 * width), low), vmem((rows, width), low),
            dma((layers + 1, 10)), dma((2, 3)), dma, dma((seqs,)), dma, dma, dma((seqs,)), dma, dma((layers, 2)), dma((layers, 2)),
        ] + (prefix_scratch(prefix.shape) if fast else []),
        compiler_params=pltpu.CompilerParams(collective_id=1, has_side_effects=True, vmem_limit_bytes=67043328),
    )(y_low, cot, full, w_qkv, w_out, q, k, v, unit, scale, slope, context, lse, hide, gains, prefix)


def local(
    tokens,
    segments,
    w_qkv,
    b_qkv,
    w_out,
    b_out,
    norm_gain,
    norm_bias,
    w_up,
    b_up,
    w_down,
    b_down,
    prefix,
    cotangent,
):
    seqs, tok, width = tokens.shape
    layers, rim, rows = w_qkv.shape[0], PAIR_MAX, seqs * tok
    wides = lax.axis_size("wide")
    fast = wides == 8 and lax.axis_size("rows") == 4
    parts = wides // seqs
    wide = lax.axis_index("wide")
    ids = jnp.pad(segments, ((0, 0), (rim, rim)), constant_values=-1)
    ids = lax.dynamic_slice(ids, (lax.div(wide, parts), lax.rem(wide, parts) * rows), (1, rows + 2 * rim))[0]
    hide = jnp.stack(
        [
            jnp.where(ids[b * tok : b * tok + tok + 2 * rim, None] == ids[None, b * tok + rim : b * tok + rim + tok], 0.0, -1e30)
            for b in range(seqs)
        ]
    )
    hide = jnp.pad(hide, ((0, 0), (prefix.shape[2], 0), (0, 0)))
    full_in = w_up
    if not fast:
        full_in = jnp.stack([lax.all_gather(w, "wide", axis=1, tiled=True) for w in (w_up, w_down)], axis=1)
    y_low, cot, full, q, k, v, unit, scale, slope, lse, context = forward(
        fast, tokens, cotangent, w_qkv, w_out, w_up, w_down, full_in, hide, b_qkv, b_out, norm_gain, norm_bias,
        b_up.astype(jnp.float32).reshape(1, -1), b_down, prefix,
    )
    output, grads, prefix_grads = backward(
        fast, y_low, cot, full if fast else full_in, w_qkv, w_out, q, k, v, unit, scale, slope, context, lse, hide, norm_gain, prefix, seqs
    )
    if not fast:
        prefix_grads = lax.psum(prefix_grads, ("rows", "wide"))
    return output, grads.astype(jnp.float32), prefix_grads


def solution(mesh):
    return jax.shard_map(
        local,
        mesh=mesh,
        in_specs=(
            P("rows", "wide", None),
            P("rows", None),
            P(),
            P(),
            P(),
            P(),
            P(),
            P(),
            P(None, "wide", None),
            P(None, "wide"),
            P(None, "wide", None),
            P(),
            P(),
            P("rows", "wide", None),
        ),
        out_specs=(P("rows", "wide", None), P("rows", "wide", None), P()),
        check_vma=False,
    )
```

```python
import functools
import math

import jax
import jax.numpy as jnp
from jax import lax
from jax.experimental import pallas as pl
from jax.experimental.pallas import tpu as pltpu
from jax.sharding import PartitionSpec as P

HEADS = 16
PAIR_MAX = 128
MESH = pl.DeviceIdType.MESH
LANES = 128
SPAN = 1024
ROOT_HALF = math.sqrt(0.5)


def multiply(left, right):
    return jnp.dot(left, right, preferred_element_type=jnp.float32)


def multiply_back(left, right):
    return lax.dot_general(left, right, (((1,), (1,)), ((), ())), preferred_element_type=jnp.float32)


def multiply_first(left, right):
    return lax.dot_general(left, right, (((0,), (0,)), ((), ())), preferred_element_type=jnp.float32)


def two_heads(rows):
    half = rows.shape[1] // 2
    lane = lax.broadcasted_iota(jnp.int32, rows.shape, 1)
    nothing = jnp.zeros_like(rows)
    return jnp.concatenate([jnp.where(lane < half, rows, nothing), jnp.where(lane >= half, rows, nothing)], axis=0)


def own_heads(columns):
    half, count = columns.shape[0] // 2, columns.shape[1] // 2
    place = lax.broadcasted_iota(jnp.int32, (columns.shape[0], count), 0)
    return jnp.where(place < half, columns[:, :count], columns[:, count:]).T


def attend(blocks, rows, rim, pair, q_ref, k_ref, v_ref, prefix_ref, hide_ref, context_ref, lse_ref):
    lanes = pl.ds(pl.multiple_of(pair * 128, 128), 128)
    for block in range(blocks):
        here = pl.ds(block * rows, rows)
        window = pl.ds(block * rows, rows + 2 * rim)
        queries = two_heads(q_ref[here, lanes])
        hide = hide_ref[block]
        keys = jnp.concatenate([prefix_ref[0, :, lanes], k_ref[window, lanes]], axis=0)
        values = jnp.concatenate([prefix_ref[1, :, lanes], v_ref[window, lanes]], axis=0)
        scores = multiply_back(keys, queries) + jnp.concatenate([hide, hide], axis=1)
        top = jnp.max(scores, axis=0, keepdims=True)
        scores = jnp.exp(scores - top)
        total = jnp.sum(scores, axis=0, keepdims=True)
        share = 1.0 / total
        columns = multiply_first(values, scores.astype(jnp.bfloat16))
        context_ref[here, lanes] = own_heads(columns * share).astype(jnp.bfloat16)
        lse_ref[pair * blocks + block] = top + jnp.log(total)


def attend_back(
    blocks, rows, rim, pair, q_ref, k_ref, v_ref, prefix_ref, hide_ref, lse_ref, context_ref, grad_ref, dq_ref, dk_ref, dv_ref, dp_ref, scale
):
    lanes = pl.ds(pl.multiple_of(pair * 128, 128), 128)
    for block in range(blocks):
        here = pl.ds(block * rows, rows)
        grad = grad_ref[here, lanes]
        queries, grads = two_heads(q_ref[here, lanes]), two_heads(grad)
        shared = (grad.astype(jnp.float32) * context_ref[here, lanes].astype(jnp.float32)).T
        half = shared.shape[0] // 2
        dots = jnp.concatenate(
            [jnp.sum(shared[:half], axis=0, keepdims=True), jnp.sum(shared[half:], axis=0, keepdims=True)], axis=1
        )
        lse = lse_ref[pair * blocks + block]
        window = pl.ds(block * rows, rows + 2 * rim)
        keys = jnp.concatenate([prefix_ref[0, :, lanes], k_ref[window, lanes]], axis=0)
        values = jnp.concatenate([prefix_ref[1, :, lanes], v_ref[window, lanes]], axis=0)
        hide = hide_ref[block]
        probs = jnp.exp(multiply_back(keys, queries) + (jnp.concatenate([hide, hide], axis=1) - lse))
        grad_scores = (probs * (multiply_back(values, grads) - dots)).astype(jnp.bfloat16)
        new_values = multiply(probs.astype(jnp.bfloat16), grads)
        new_keys = multiply(grad_scores, queries)
        columns = multiply_first(keys, grad_scores)
        count = prefix_ref.shape[1]
        old, fresh = pl.ds(block * rows, 2 * rim), pl.ds(block * rows + 2 * rim, rows)
        if block == 0:
            dk_ref[window, lanes], dv_ref[window, lanes] = new_keys[count:], new_values[count:]
            dp_ref[0, :, lanes], dp_ref[1, :, lanes] = new_keys[:count], new_values[:count]
        else:
            dk_ref[old, lanes] += new_keys[count : count + 2 * rim]
            dv_ref[old, lanes] += new_values[count : count + 2 * rim]
            dk_ref[fresh, lanes], dv_ref[fresh, lanes] = new_keys[count + 2 * rim :], new_values[count + 2 * rim :]
            dp_ref[0, :, lanes] += new_keys[:count]
            dp_ref[1, :, lanes] += new_values[:count]
        dq_ref[here, lanes] = (own_heads(columns) * scale).astype(jnp.bfloat16)


def gelu_pair(values):
    size = jnp.abs(values) * ROOT_HALF
    bell = jnp.exp(values * values * -0.5)
    t = 1.0 / (1.0 + 0.3275911 * size)
    series = ((((1.061405429 * t - 1.453152027) * t + 1.421413741) * t - 0.284496736) * t + 0.254829592) * t
    tail = 0.5 * series * bell
    below = jnp.where(values < 0, tail, 1.0 - tail)
    return values * below, below + values * bell * (1.0 / math.sqrt(2.0 * math.pi))


def normalize(values):
    center = values - jnp.mean(values, axis=-1, keepdims=True)
    scale = lax.rsqrt(jnp.mean(center * center, axis=-1, keepdims=True) + 1e-05)
    return center * scale, scale


def norm_grad(grad, unit, scale, gain):
    inner = grad * gain
    first = jnp.mean(inner, axis=-1, keepdims=True)
    second = jnp.mean(inner * unit, axis=-1, keepdims=True)
    return scale * (inner - first - unit * second)


def each(count, step, body):
    @pl.loop(0, count)
    def _(i):
        body(pl.ds(pl.multiple_of(i * step, step), step))


class Place:
    def __init__(self, seqs, tok):
        self.seqs, self.tok, self.rows = seqs, tok, seqs * tok
        self.wide_size = lax.axis_size("wide")
        self.parts = self.wide_size // seqs
        self.row, self.wide = lax.axis_index("rows"), lax.axis_index("wide")
        self.seq, self.part = lax.div(self.wide, self.parts), lax.rem(self.wide, self.parts)

    def others(self, body):
        @pl.loop(1, self.wide_size)
        def _(step):
            body(lax.rem(self.wide + step, self.wide_size))

    def barrier(self, more):
        sem = pltpu.get_barrier_semaphore()
        self.others(lambda other: pl.semaphore_signal(sem, inc=1, device_id=(self.row, other), device_id_type=MESH))
        for device in more:
            pl.semaphore_signal(sem, inc=1, device_id=device, device_id_type=MESH)
        pl.semaphore_wait(sem, self.wide_size - 1 + len(more))

    def remote(self, src, dst, send, recv, device):
        return pltpu.make_async_remote_copy(
            src_ref=src, dst_ref=dst, send_sem=send, recv_sem=recv, device_id=device, device_id_type=MESH
        )

    def send_out(self, parts, target, send, recv, own):
        block = lax.rem(self.wide, self.seqs)
        for s in range(self.seqs):
            goal = s * self.parts + lax.div(self.wide, self.seqs)

            @pl.when(goal != self.wide)
            def _():
                self.remote(parts(s), target(block), send, recv.at[block], (self.row, goal)).start()

            @pl.when(goal == self.wide)
            def _():
                pltpu.make_async_copy(parts(s), target(block), own).start()

    def sent_out(self, parts, target, send, recv, own):
        block = lax.rem(self.wide, self.seqs)
        for s in range(self.seqs):
            goal = s * self.parts + lax.div(self.wide, self.seqs)

            @pl.when(goal != self.wide)
            def _():
                self.remote(parts(s), target(block), send, recv.at[block], (self.row, goal)).wait_send()

    def got_out(self, parts, target, send, recv, own):
        for b in range(self.seqs):
            source = self.part * self.seqs + b

            @pl.when(source != self.wide)
            def _():
                self.remote(parts(0), target(b), send, recv.at[b], (self.row, self.wide)).wait_recv()

            @pl.when(source == self.wide)
            def _():
                pltpu.make_async_copy(parts(0), target(b), own).wait()

    def send_home_block(self, b, part, target, send, recv, own):
        goal = self.part * self.seqs + b

        @pl.when(goal != self.wide)
        def _():
            self.remote(part, target(self.seq), send, recv.at[self.seq], (self.row, goal)).start()

        @pl.when(goal == self.wide)
        def _():
            pltpu.make_async_copy(part, target(self.seq), own).start()

    def sent_home(self, part, target, send, recv):
        for b in range(self.seqs):
            goal = self.part * self.seqs + b

            @pl.when(goal != self.wide)
            def _():
                self.remote(part, target(self.seq), send, recv.at[self.seq], (self.row, goal)).wait_send()

    def got_home(self, s, part, target, send, recv, own):
        source = s * self.parts + lax.div(self.wide, self.seqs)

        @pl.when(source != self.wide)
        def _():
            self.remote(part, target(s), send, recv.at[s], (self.row, self.wide)).wait_recv()

        @pl.when(source == self.wide)
        def _():
            pltpu.make_async_copy(part, target(s), own).wait()


def fill_hide(place, rim, segments, hide):
    count = hide.shape[1] - place.tok - 2 * rim
    base = place.part * place.rows

    def ids(start):
        start = pl.multiple_of(start, LANES)
        rows = segments[:, pl.ds(start, LANES)].astype(jnp.float32)
        here = lax.broadcasted_iota(jnp.int32, rows.shape, 0) == place.seq
        return jnp.sum(jnp.where(here, rows, 0.0), axis=0, keepdims=True)

    for b in range(place.seqs):
        hide[b, pl.ds(0, count)] = jnp.zeros((count, place.tok), jnp.float32)
        own = ids(base + b * place.tok)
        for chunk in range((place.tok + 2 * rim) // LANES):
            start = base + b * place.tok - rim + chunk * LANES
            safe = jnp.clip(start, 0, segments.shape[1] - LANES)
            keys = jnp.where(start == safe, ids(safe), -1.0)
            keys = jnp.broadcast_to(keys, (LANES, LANES)).T
            hide[b, pl.ds(count + chunk * LANES, LANES)] = jnp.where(keys == own, 0.0, -1e30)


class Gather:
    def __init__(self, shards, full, sems):
        self.shards = shards
        self.full = full
        self.send_sem, self.zs, self.xs, self.ys, self.ds, self.cz, self.cx, self.cy, self.cd, self.cown, self.own = sems
        self.row = lax.axis_index("rows")
        self.wide = lax.axis_index("wide")
        self.z, self.core = lax.div(self.wide, 2), lax.rem(self.wide, 2)
        self.shard_rows = shards[0].shape[1]
        self.unit_rows = self.shard_rows // 4
        self.row_x = self.row + 1 - 2 * lax.rem(self.row, 2)
        self.row_y = lax.rem(self.row + 2, 4)
        self.row_d = 3 - self.row

    def unit(self, layer, member, z, core, quarter):
        start = (z * 2 + core) * self.shard_rows + quarter * self.unit_rows
        return self.full.at[layer, member, pl.ds(pl.multiple_of(start, self.unit_rows), self.unit_rows)]

    def shard(self, layer, member, z, core):
        start = (z * 2 + core) * self.shard_rows
        return self.full.at[layer, member, pl.ds(pl.multiple_of(start, self.shard_rows), self.shard_rows)]

    def copy(self, src, dst, recv, kind):
        if kind == "x":
            device = (self.row_x, self.wide)
        elif kind == "y":
            device = (self.row_y, self.wide)
        elif kind == "core":
            device = (self.row, self.z * 2 + 1 - self.core)
        else:
            device = (self.row, self.wide + 2 - 4 * kind)
        return pltpu.make_async_remote_copy(
            src_ref=src, dst_ref=dst, send_sem=self.send_sem, recv_sem=recv, device_id=device, device_id_type=MESH
        )

    def start_z(self, layer):
        for member in range(2):
            start = pl.multiple_of(self.row * self.unit_rows, self.unit_rows)
            mine = self.shards[member].at[layer, pl.ds(start, self.unit_rows)]
            here = self.unit(layer, member, self.z, self.core, self.row)

            @pl.when(self.z < 3)
            def _():
                self.copy(mine, here, self.zs.at[layer, member, 0, 0], 0).start()

            @pl.when(self.z > 0)
            def _():
                self.copy(mine, here, self.zs.at[layer, member, 0, 1], 1).start()

    def start_core(self, layer):
        for member in range(2):
            place = self.shard(layer, member, self.z, self.core)
            pltpu.make_async_copy(self.shards[member].at[layer], place, self.own.at[layer, member]).start()
            self.copy(self.shards[member].at[layer], place, self.cown.at[layer, member], "core").start()

    def slot(self, i):
        near = jnp.minimum(self.z, 3 - self.z)
        far_side = 1 - lax.div(self.z, 2)
        both = jnp.minimum(lax.div(i, jnp.maximum(2 * near, 1)), 1) + (1 - jnp.minimum(near, 1))
        both = 1 - jnp.minimum(both, 1)
        step = both * lax.div(i, 2) + (1 - both) * (i - near)
        side = both * lax.rem(i, 2) + (1 - both) * far_side
        return step, side, self.z + (1 + step) * (2 * side - 1)

    def on_z(self, layer, i):
        step, side, origin = self.slot(i)
        for member in range(2):
            unit = self.unit(layer, member, origin, self.core, self.row)
            self.copy(unit, unit, self.zs.at[layer, member, step, side], "x").wait_recv()
            target = self.z + 1 - 2 * side

            @pl.when((target >= 0) & (target < 4))
            def _():
                self.copy(unit, unit, self.zs.at[layer, member, step + 1, side], side).start()

            self.copy(unit, unit, self.xs.at[layer, member, step, side], "x").start()
            self.copy(unit, unit, self.ys.at[layer, member, step, side], "y").start()
            self.copy(unit, unit, self.cz.at[layer, member, step, side], "core").start()

    def on_first(self, layer, _):
        self.on_z(layer, 0)

        @pl.when((self.z > 0) & (self.z < 3))
        def _():
            self.on_z(layer, 1)

    def on_second(self, layer, _):
        self.on_z(layer, 1 + jnp.minimum(self.z, 1) * jnp.minimum(3 - self.z, 1))

    def on_third(self, layer, _):
        @pl.when((self.z == 0) | (self.z == 3))
        def _():
            self.on_z(layer, 2)

    def on_xy(self, layer, i):
        step, side, origin = self.slot(i)
        for member in range(2):
            unit = self.unit(layer, member, origin, self.core, self.row_x)
            self.copy(unit, unit, self.xs.at[layer, member, step, side], "x").wait_recv()
            if member == 0:
                self.copy(unit, unit, self.ds.at[layer, member, step, side], "y").start()
            self.copy(unit, unit, self.cx.at[layer, member, step, side], "core").start()
            unit = self.unit(layer, member, origin, self.core, self.row_y)
            self.copy(unit, unit, self.ys.at[layer, member, step, side], "y").wait_recv()
            if member == 1:
                self.copy(unit, unit, self.ds.at[layer, member, step, side], "x").start()
            self.copy(unit, unit, self.cy.at[layer, member, step, side], "core").start()

    def on_d(self, layer, i):
        step, side, origin = self.slot(i)
        for member in range(2):
            unit = self.unit(layer, member, origin, self.core, self.row_d)
            self.copy(unit, unit, self.ds.at[layer, member, step, side], "x").wait_recv()
            self.copy(unit, unit, self.cd.at[layer, member, step, side], "core").start()

    def on_core(self, layer, i):
        step, side, origin = self.slot(i)
        for member in range(2):
            for sem, quarter in ((self.cz, self.row), (self.cx, self.row_x), (self.cy, self.row_y), (self.cd, self.row_d)):
                unit = self.unit(layer, member, origin, 1 - self.core, quarter)
                self.copy(unit, unit, sem.at[layer, member, step, side], "core").wait_recv()

    def on_own(self, layer):
        for member in range(2):
            place = self.shard(layer, member, self.z, self.core)
            pltpu.make_async_copy(self.shards[member].at[layer], place, self.own.at[layer, member]).wait()
            place = self.shard(layer, member, self.z, 1 - self.core)
            self.copy(place, place, self.cown.at[layer, member], "core").wait_recv()

    def drain(self, layers):
        def wait(units):
            span = self.full.at[0, 0, pl.ds(0, units * self.unit_rows)]
            self.copy(span, span, self.own.at[0, 0], "core").wait_send()

        @pl.loop(0, layers)
        def _(layer):
            wait(8)

            @pl.when(self.z < 3)
            def _():
                wait(2)

            @pl.when(self.z > 0)
            def _():
                wait(2)

            @pl.loop(0, 3)
            def _(i):
                step, side, origin = self.slot(i)
                target = self.z + 1 - 2 * side

                @pl.when((target >= 0) & (target < 4))
                def _():
                    wait(2)

                wait(14)


class PrefixSum:
    def __init__(self, place, parts, inbox, planes, total, sems):
        self.parts, self.inbox, self.planes, self.total = parts, inbox, planes, total
        self.send_sem, self.in_sem, self.plane_sem, self.total_sem = sems
        self.row = place.row
        self.z, self.core = lax.div(place.wide, 2), lax.rem(place.wide, 2)
        self.me = self.row * 2 + self.core
        self.size = inbox.shape[2]

    def peers(self, body):
        @pl.loop(1, 8)
        def _(step):
            body(lax.rem(self.me + step, 8))

    def others(self):
        return [(lax.rem(self.row + step, 4), self.z * 2 + core) for step in range(1, 4) for core in range(2)]

    def piece(self, ref, layer, index):
        start = lax.rem(index, 4) * self.size
        return ref.at[layer, lax.div(index, 4), pl.ds(pl.multiple_of(start, self.size), self.size)]

    def copy(self, src, dst, recv, row, wide):
        return pltpu.make_async_remote_copy(
            src_ref=src, dst_ref=dst, send_sem=self.send_sem, recv_sem=recv, device_id=(row, wide), device_id_type=MESH
        )

    def in_copy(self, layer, peer, origin):
        return self.copy(
            self.piece(self.parts, layer, peer), self.inbox.at[layer, origin], self.in_sem.at[layer, origin],
            lax.div(peer, 2), self.z * 2 + lax.rem(peer, 2),
        )

    def plane_copy(self, layer, z, origin):
        place = self.planes.at[layer, origin]
        return self.copy(place, place, self.plane_sem.at[layer, origin], self.row, z * 2 + self.core)

    def total_copy(self, layer, peer, origin):
        place = self.piece(self.total, layer, origin)
        return self.copy(place, place, self.total_sem.at[layer, origin], lax.div(peer, 2), self.z * 2 + lax.rem(peer, 2))

    def planes_others(self, body):
        @pl.loop(1, 4)
        def _(step):
            body(lax.rem(self.z + step, 4))

    def start(self, layer):
        self.peers(lambda peer: self.in_copy(layer, peer, self.me).start())

    def middle(self, layer):
        self.peers(lambda peer: self.in_copy(layer, self.me, peer).wait_recv())
        value = self.piece(self.parts, layer, self.me)[...]
        for step in range(1, 8):
            value += self.inbox[layer, lax.rem(self.me + step, 8)]
        self.planes[layer, self.z] = value
        self.planes_others(lambda z: self.plane_copy(layer, z, self.z).start())

    def last(self, layer):
        self.planes_others(lambda z: self.plane_copy(layer, self.z, z).wait_recv())
        value = self.planes[layer, 0]
        for z in range(1, 4):
            value += self.planes[layer, z]
        self.piece(self.total, layer, self.me)[...] = value
        self.peers(lambda peer: self.total_copy(layer, peer, self.me).start())

    def finish(self, layer):
        self.peers(lambda peer: self.total_copy(layer, self.me, peer).wait_recv())
        self.peers(lambda peer: self.in_copy(layer, peer, self.me).wait_send())
        self.planes_others(lambda z: self.plane_copy(layer, z, self.z).wait_send())
        self.peers(lambda peer: self.total_copy(layer, peer, self.me).wait_send())


def prefix_scratch(shape):
    layers, members, count, width = shape
    size = members * count // 8
    dma = pltpu.SemaphoreType.DMA
    return [
        pltpu.VMEM(shape, jnp.float32), pltpu.VMEM((layers, 8, size, width), jnp.float32),
        pltpu.VMEM((layers, 4, size, width), jnp.float32), dma, dma((layers, 8)), dma((layers, 4)), dma((layers, 8)),
    ]


def gather_sems(layers):
    return (
        [pltpu.SemaphoreType.DMA]
        + [pltpu.SemaphoreType.DMA((layers, 2, 3, 2))] * 8
        + [pltpu.SemaphoreType.DMA((layers, 2))] * 2
    )


def forward_kernel(
    fast, seqs, tok, rim,
    tokens, cotangent, w_qkv, w_out, w_up, w_down, full_in,
    segments, b_qkv, b_out, gains, shifts, b_up, b_down, prefix,
    y_low, cot_out, full_out, q_out, k_out, v_out, unit_out, scale_out, slope_out, lse_out, context_out,
    full, wqkv, wout, x, low, acc, q, k, v, halo, context, slope, unit1, unit2, scale1, scale2, lse, bias, hide,
    load_sem, store_sem, slope_sem, full_sem, tok_send, tok_recv, tok_own, cot_send, cot_recv, cot_own,
    halo_send, halo_recv, bias_send, bias_recv, bias_own,
    *gather_sem,
):
    layers, width = w_qkv.shape[0], tokens.shape[2]
    place = Place(seqs, tok)
    rows = place.rows
    gather = Gather((w_up, w_down), full, gather_sem) if fast else None
    place.barrier(((gather.row_x, place.wide), (gather.row_y, place.wide)) if fast else ())
    own_bias = bias.at[place.wide]

    def load(layer):
        return (
            pltpu.make_async_copy(w_qkv.at[layer], wqkv, load_sem.at[0]),
            pltpu.make_async_copy(w_out.at[layer], wout, load_sem.at[1]),
        )

    def put_bias(other):
        return place.remote(b_up, own_bias, bias_send, bias_recv.at[place.wide], (place.row, other))

    def got_bias(other):
        return place.remote(b_up, bias.at[other], bias_send, bias_recv.at[other], (place.row, other))

    if fast:
        gather.start_z(0)
        gather.start_core(0)
    else:
        pltpu.make_async_copy(full_in, full, full_sem.at[0]).start()
    for copy in load(0):
        copy.start()
    place.others(lambda other: put_bias(other).start())
    pltpu.make_async_copy(b_up, own_bias, bias_own).start()

    tok_args = (lambda s: tokens.at[s], lambda b: low.at[pl.ds(pl.multiple_of(b * tok, tok), tok)], tok_send, tok_recv, tok_own)
    cot_args = (lambda s: cotangent.at[s], lambda b: cot_out.at[pl.ds(pl.multiple_of(b * tok, tok), tok)], cot_send, cot_recv, cot_own)
    events = {}
    if fast:
        gather.on_first(0, 0)
        place.send_out(*tok_args)
        gather.on_second(0, 0)
        gather.on_xy(0, 0)
        events = {
            (0, "queries"): [(gather.on_third, 0, 0)],
            (0, "pair", 1): [(gather.on_xy, 0, 1)],
            (0, "pair", 4): [(gather.on_first, 1, 0), (gather.on_d, 0, 0)],
            (0, "pair", 7): [(gather.on_xy, 0, 2)],
            (0, "projected"): [(gather.on_d, 0, 1)],
            (0, "normed"): [(gather.on_second, 1, 0)],
            (0, "step", 1): [(gather.on_core, 0, 0)],
            (0, "step", 2): [(gather.on_xy, 1, 0), (gather.on_core, 0, 1), (gather.on_d, 0, 2)],
            (0, "step", 3): [(gather.on_core, 0, 2), (gather.on_third, 1, 0)],
            (1, "queries"): [(gather.on_xy, 1, 1)],
            (1, "pair", 7): [(gather.on_xy, 1, 2)],
            (1, "projected"): [(gather.on_d, 1, 0)],
            (1, "normed"): [(gather.on_d, 1, 1)],
            (1, "step", 1): [(gather.on_core, 1, 0)],
            (1, "step", 2): [(gather.on_d, 1, 2), (gather.on_core, 1, 1)],
            (1, "step", 3): [(gather.on_core, 1, 2)],
        }
    else:
        place.send_out(*tok_args)

    def tick(*when):
        for event, layer, i in events.get(when, ()):
            event(layer, i)

    def loop_tick(layer, kind, index, count):
        for n in range(count):
            if (layer, kind, n) in events:
                @pl.when(index == n)
                def _():
                    tick(layer, kind, n)

    blank = jnp.zeros((rim, width), jnp.bfloat16)

    @pl.when(place.part == 0)
    def _():
        k[pl.ds(0, rim)] = blank
        v[pl.ds(0, rim)] = blank

    @pl.when(place.part == place.parts - 1)
    def _():
        k[pl.ds(rim + rows, rim)] = blank
        v[pl.ds(rim + rows, rim)] = blank

    fill_hide(place, rim, segments, hide)
    place.got_out(*tok_args)
    if fast:
        gather.start_z(1)
        gather.start_core(1)

    def halo_copy(layer, member, side, wide):
        ref = (k, v)[member]
        return place.remote(
            ref.at[pl.ds((rows, rim)[side], rim)], halo.at[layer, member, side],
            halo_send.at[member, side], halo_recv.at[layer, member, side], (place.row, wide),
        )

    def halos(body, to):
        for side in range(2):
            @pl.when(place.part < place.parts - 1 if (side == 0) == to else place.part > 0)
            def _():
                for member in range(2):
                    body(member, side, jnp.clip(place.wide + (1 - 2 * side), 0, place.wide_size - 1))

    def got_halo(layer, member, side, wide):
        halo_copy(layer, member, side, place.wide).wait_recv()
        (k, v)[member][pl.ds((0, rim + rows)[side], rim)] = halo[layer, member, side]

    def kept(layer):
        return [
            pltpu.make_async_copy(src, dst.at[layer], store_sem.at[i])
            for i, (src, dst) in enumerate(((q, q_out), (k, k_out), (v, v_out)))
        ]

    def kept_context(layer):
        return [pltpu.make_async_copy(context, context_out.at[layer], store_sem.at[9])]

    def kept_norm(layer, which):
        unit, scale = ((unit1, scale1), (unit2, scale2))[which]
        return [
            pltpu.make_async_copy(unit, unit_out.at[layer, which], store_sem.at[3 + which]),
            pltpu.make_async_copy(scale, scale_out.at[layer, which], store_sem.at[5 + which]),
        ]

    half = width // 2
    for layer in range(layers):
        if layer > 0:
            for copy in kept(layer - 1) + kept_context(layer - 1) + kept_norm(layer - 1, 0) + kept_norm(layer - 1, 1):
                copy.wait()
        load(layer)[0].wait()
        for part in (2, 3, 4, 5, 0, 1):
            lanes = pl.ds(part * half, half)
            made = multiply(low[...], wqkv[:, lanes]) + b_qkv[layer : layer + 1, lanes]
            kind, side = part // 2, pl.ds((part % 2) * half, half)
            if kind == 0:
                q[:, side] = made.astype(jnp.bfloat16) * (1.0 / math.sqrt(width // HEADS))
            else:
                (k, v)[kind - 1][pl.ds(rim, rows), side] = made.astype(jnp.bfloat16)
            if part == 5:
                halos(lambda *at: halo_copy(layer, *at).start(), True)
        if layer + 1 < layers:
            load(layer + 1)[0].start()
        tick(layer, "queries")
        halos(lambda *at: got_halo(layer, *at), False)
        halos(lambda *at: halo_copy(layer, *at).wait_send(), True)
        for copy in kept(layer):
            copy.start()

        @pl.loop(0, width // LANES)
        def _(pair):
            attend(seqs, tok, rim, pair, q, k, v, prefix.at[layer], hide, context, lse.at[layer])
            loop_tick(layer, "pair", pair, width // LANES)

        for copy in kept_context(layer):
            copy.start()
        load(layer)[1].wait()
        for part in range(2):
            lanes = pl.ds(part * half, half)
            acc[:, lanes] = multiply(context[...], wout[:, lanes])
        if layer + 1 < layers:
            load(layer + 1)[1].start()
        tick(layer, "projected")

        def first_norm(at):
            before = low[at].astype(jnp.float32) if layer == 0 else x[at]
            unit, scale = normalize(before + acc[at] + b_out[layer : layer + 1])
            unit1[at] = unit.astype(jnp.bfloat16)
            scale1[at] = jnp.broadcast_to(scale, (scale.shape[0], LANES))
            normed = unit * gains[layer, :1] + shifts[layer, :1]
            low[at] = normed.astype(jnp.bfloat16)
            acc[at] = normed + b_down[layer : layer + 1]

        each(rows // 64, 64, first_norm)
        for copy in kept_norm(layer, 0):
            copy.start()
        tick(layer, "normed")
        if layer == 0:
            pltpu.make_async_copy(b_up, own_bias, bias_own).wait()
            place.others(lambda other: got_bias(other).wait_recv())

            place.others(lambda other: put_bias(other).wait_send())
            if not fast:
                pltpu.make_async_copy(full_in, full, full_sem.at[0]).wait()

        hidden = b_up.shape[1] // layers

        @pl.loop(0, full.shape[2] // SPAN)
        def _(i):
            spot = i
            if fast:
                @pl.when(i == 0)
                def _():
                    gather.on_own(layer)

                loop_tick(layer, "step", i, full.shape[2] // SPAN)
                origin = gather.slot(jnp.maximum(i - 1, 0))[2]
                started = jnp.minimum(i, 1)
                spot = started * origin + (1 - started) * gather.z
            units = pl.ds(pl.multiple_of(spot * SPAN, SPAN), SPAN)
            slot = lax.rem(i, 2)
            step_bias = jnp.concatenate(
                [bias[spot * (SPAN // hidden) + n, :, pl.ds(layer * hidden, hidden)] for n in range(SPAN // hidden)], axis=1
            )

            @pl.when(i > 1)
            def _():
                pltpu.make_async_copy(slope.at[slot], slope_out.at[layer, spot], slope_sem.at[slot]).wait()

            for part in range(2):
                at = pl.ds(part * (rows // 2), rows // 2)
                act, rise = gelu_pair(multiply_back(low[at], full[layer, 0, units]) + step_bias)
                slope[slot, at] = rise.astype(jnp.bfloat16)
                acc[at] += multiply(act.astype(jnp.bfloat16), full[layer, 1, units])
            pltpu.make_async_copy(slope.at[slot], slope_out.at[layer, spot], slope_sem.at[slot]).start()
            if fast:
                pltpu.make_async_copy(full.at[layer, :, units], full_out.at[layer, :, units], full_sem.at[layer]).start()

        for slot in range(2):
            pltpu.make_async_copy(slope.at[slot], slope_out.at[layer, 0], slope_sem.at[slot]).wait()

        def second_norm(at):
            unit, scale = normalize(acc[at])
            unit2[at] = unit.astype(jnp.bfloat16)
            scale2[at] = jnp.broadcast_to(scale, (scale.shape[0], LANES))
            after = unit * gains[layer, 1:] + shifts[layer, 1:]
            low[at] = after.astype(jnp.bfloat16)
            if layer + 1 < layers:
                x[at] = after

        each(rows // 64, 64, second_norm)
        for copy in kept_norm(layer, 1):
            copy.start()
        if layer == 0:
            place.send_out(*cot_args)
            tick(0, "done")
    last = [pltpu.make_async_copy(low, y_low, store_sem.at[7]), pltpu.make_async_copy(lse, lse_out, store_sem.at[8])]
    for copy in last:
        copy.start()
    place.sent_out(*tok_args)
    place.got_out(*cot_args)
    place.sent_out(*cot_args)
    for copy in last + kept(layers - 1) + kept_context(layers - 1) + kept_norm(layers - 1, 0) + kept_norm(layers - 1, 1):
        copy.wait()
    if fast:
        gather.drain(layers)
        for layer in range(layers):
            pltpu.make_async_copy(full.at[layer], full_out.at[layer], full_sem.at[layer]).wait()


def forward(fast, tokens, cotangent, w_qkv, w_out, w_up, w_down, full_in, segments, b_qkv, b_out, gains, shifts, b_up, b_down, prefix):
    seqs, tok, width = tokens.shape
    layers, rim, rows = w_qkv.shape[0], PAIR_MAX, seqs * tok
    wides = lax.axis_size("wide")
    units = w_up.shape[1] * wides
    low, full_type = jnp.bfloat16, jnp.float32
    spans = units // SPAN
    shape = jax.ShapeDtypeStruct
    dma = pltpu.SemaphoreType.DMA
    scores = (layers, width // LANES * seqs, 1, 2 * tok)
    return pl.pallas_call(
        functools.partial(forward_kernel, fast, seqs, tok, rim),
        out_shape=(
            shape((rows, width), low), shape((rows, width), low), shape((layers, 2, units, width), low),
            shape((layers, rows, width), low), shape((layers, rows + 2 * rim, width), low),
            shape((layers, rows + 2 * rim, width), low), shape((layers, 2, rows, width), low),
            shape((layers, 2, rows, LANES), full_type), shape((layers, spans, rows, SPAN), low), shape(scores, full_type),
            shape((layers, rows, width), low),
        ),
        in_specs=[pl.BlockSpec(memory_space=pl.ANY)] * 7 + [pl.BlockSpec(memory_space=pltpu.VMEM)] * 8,
        out_specs=(pl.BlockSpec(memory_space=pl.ANY),) * 11,
        scratch_shapes=[
            pltpu.VMEM((layers, 2, units, width), low), pltpu.VMEM(w_qkv.shape[1:], low), pltpu.VMEM(w_out.shape[1:], low),
            pltpu.VMEM((rows, width), full_type), pltpu.VMEM((rows, width), low), pltpu.VMEM((rows, width), full_type),
            pltpu.VMEM((rows, width), low), pltpu.VMEM((rows + 2 * rim, width), low), pltpu.VMEM((rows + 2 * rim, width), low),
            pltpu.VMEM((layers, 2, 2, rim, width), low), pltpu.VMEM((rows, width), low), pltpu.VMEM((2, rows, SPAN), low),
            pltpu.VMEM((rows, width), low), pltpu.VMEM((rows, width), low),
            pltpu.VMEM((rows, LANES), full_type), pltpu.VMEM((rows, LANES), full_type),
            pltpu.VMEM(scores, full_type), pltpu.VMEM((wides,) + b_up.shape, full_type),
            pltpu.VMEM((seqs, prefix.shape[2] + tok + 2 * rim, tok), full_type),
            dma((2,)), dma((10,)), dma((2,)), dma((layers,)), dma, dma((seqs,)), dma, dma, dma((seqs,)), dma,
            dma((2, 2)), dma((layers, 2, 2)), dma, dma((wides,)), dma,
        ] + (gather_sems(layers) if fast else []),
        compiler_params=pltpu.CompilerParams(collective_id=0, has_side_effects=True, vmem_limit_bytes=67043328),
    )(tokens, cotangent, w_qkv, w_out, w_up, w_down, full_in, segments, b_qkv, b_out, gains, shifts, b_up, b_down, prefix)


def backward_kernel(
    fast, seqs, tok, rim,
    y_low, cot_in, full, w_qkv, w_out, q_in, k_in, v_in, unit_in, scale_in, slope_in, context_in,
    lse, segments, gains, prefix,
    out, grads, prefix_grads,
    wqkv, wout, q, k, v, unit1, unit2, scale1, scale2, up, down, slope, cot, acc, low, context, made, dk, dv, edge, edge_in, saved, hide,
    load_sem, ffn_sem, out_send, out_recv, out_own, home_send, home_recv, home_own, edge_send, edge_recv,
    *sums,
):
    layers, width = w_qkv.shape[0], w_qkv.shape[1]
    place = Place(seqs, tok)
    rows = place.rows
    prefix_sum, prefix_parts = None, prefix_grads
    if fast:
        prefix_parts = sums[0]
        prefix_sum = PrefixSum(place, *sums[:3], prefix_grads, sums[3:])
    place.barrier(prefix_sum.others() if fast else ())
    spans = slope_in.shape[1]

    def out_rows(b):
        return y_low.at[pl.ds(b * tok, tok)]

    out_args = (lambda s: out.at[s], out_send, out_recv)
    for b in range(seqs):
        place.send_home_block(b, out_rows(b), *out_args, out_own)

    cot_copy = pltpu.make_async_copy(cot_in, cot, load_sem.at[layers, 0])
    cot_copy.start()

    def loads(layer):
        pairs = (
            (unit_in.at[layer, 1], unit2), (scale_in.at[layer, 1], scale2), (unit_in.at[layer, 0], unit1),
            (scale_in.at[layer, 0], scale1), (w_out.at[layer], wout), (q_in.at[layer], q), (k_in.at[layer], k),
            (v_in.at[layer], v),
        )
        copies = [pltpu.make_async_copy(src, dst.at[layer % 2], load_sem.at[layer, i]) for i, (src, dst) in enumerate(pairs)]
        return copies + [
            pltpu.make_async_copy(w_qkv.at[layer], wqkv, load_sem.at[layer, 8]),
            pltpu.make_async_copy(context_in.at[layer], saved, load_sem.at[layer, 9]),
        ]

    def ffn_loads(layer, i):
        slot = lax.rem(i, 2)
        units = pl.ds(pl.multiple_of(i * SPAN, SPAN), SPAN)
        return [
            pltpu.make_async_copy(full.at[layer, 1, units], down.at[slot], ffn_sem.at[slot, 0]),
            pltpu.make_async_copy(slope_in.at[layer, i], slope.at[slot], ffn_sem.at[slot, 1]),
            pltpu.make_async_copy(full.at[layer, 0, units], up.at[slot], ffn_sem.at[slot, 2]),
        ]

    order = list(reversed(range(layers)))
    for copy in loads(order[0])[:2]:
        copy.start()
    for i in range(2):
        for copy in ffn_loads(order[0], i):
            copy.start()
    for copy in loads(order[0])[2:]:
        copy.start()
    half = width // 2
    fill_hide(place, rim, segments, hide)
    for layer in order:
        here = layer % 2
        mine = loads(layer)
        if layer == order[0]:
            cot_copy.wait()
        if layer > 0:
            for copy in loads(layer - 1)[:8]:
                copy.start()
        if layer < order[0]:
            mine[8].start()
            mine[9].start()
        mine[0].wait()
        mine[1].wait()

        def second_norm(at):
            grad = cot[at].astype(jnp.float32) if layer == order[0] else acc[at]
            grad = norm_grad(grad, unit2[here, at].astype(jnp.float32), scale2[here, at, :1], gains[layer, 1:])
            acc[at] = grad
            low[at] = grad.astype(jnp.bfloat16)

        each(rows // 64, 64, second_norm)
        if fast and layer + 1 < layers:
            prefix_sum.middle(layer + 1)

        @pl.loop(0, spans)
        def _(i):
            slot = lax.rem(i, 2)
            for copy in ffn_loads(layer, i):
                copy.wait()
            for part in range(2):
                at = pl.ds(part * (rows // 2), rows // 2)
                grad = multiply_back(low[at], down[slot]) * slope[slot, at].astype(jnp.float32)
                acc[at] += multiply(grad.astype(jnp.bfloat16), up[slot])

            @pl.when(i + 2 < spans)
            def _():
                for copy in ffn_loads(layer, i + 2):
                    copy.start()

        if layer > 0:
            for i in range(2):
                for copy in ffn_loads(layer - 1, i):
                    copy.start()
        mine[2].wait()
        mine[3].wait()

        def first_norm(at):
            grad = norm_grad(acc[at], unit1[here, at].astype(jnp.float32), scale1[here, at, :1], gains[layer, :1])
            acc[at] = grad
            low[at] = grad.astype(jnp.bfloat16)

        each(rows // 64, 64, first_norm)
        if fast and layer + 1 < layers:
            prefix_sum.last(layer + 1)
        mine[4].wait()
        for part in range(2):
            span = pl.ds(part * half, half)
            context[:, span] = multiply_back(low[...], wout[here, span]).astype(jnp.bfloat16)
        for copy in mine[5:8] + mine[9:]:
            copy.wait()

        @pl.loop(0, width // LANES)
        def _(pair):
            attend_back(
                seqs, tok, rim, pair, q.at[here], k.at[here], v.at[here], prefix.at[layer], hide, lse.at[layer], saved, context,
                made, dk, dv, prefix_parts.at[layer], 1.0 / math.sqrt(width // HEADS),
            )

        if fast:
            prefix_sum.start(layer)

        low_edge, high_edge, own_rows = pl.ds(0, rim), pl.ds(rim + rows, rim), pl.ds(rim, rows)
        for member, ref in enumerate((dk, dv)):
            lanes = pl.ds(member * width, width)
            edge[layer, 0, :, lanes] = ref[low_edge].astype(jnp.bfloat16)
            edge[layer, 1, :, lanes] = ref[high_edge].astype(jnp.bfloat16)

        def edge_copy(side, wide):
            return place.remote(
                edge.at[layer, side], edge_in.at[layer, side], edge_send.at[layer, side], edge_recv.at[layer, side], (place.row, wide)
            )

        mine[8].wait()
        for part in range(2):
            span = pl.ds(part * half, half)
            acc[:, span] += multiply_back(made[:, pl.ds(0, width)], wqkv[span, pl.ds(0, width)])
            if part == 0:
                @pl.when(place.part > 0)
                def _():
                    edge_copy(0, place.wide - 1).start()

                @pl.when(place.part < place.parts - 1)
                def _():
                    edge_copy(1, place.wide + 1).start()

        @pl.when(place.part < place.parts - 1)
        def _():
            edge_copy(0, place.wide).wait_recv()
            for member, ref in enumerate((dk, dv)):
                ref[pl.ds(rows, rim)] += edge_in[layer, 0, :, pl.ds(member * width, width)].astype(jnp.float32)

        @pl.when(place.part > 0)
        def _():
            edge_copy(1, place.wide).wait_recv()
            for member, ref in enumerate((dk, dv)):
                ref[pl.ds(rim, rim)] += edge_in[layer, 1, :, pl.ds(member * width, width)].astype(jnp.float32)

        for member, ref in enumerate((dk, dv)):
            def lower(at):
                made[at, pl.ds((1 + member) * width, width)] = ref[pl.ds(pl.multiple_of(at.start + rim, 64), 64)].astype(jnp.bfloat16)

            each(rows // 64, 64, lower)

        @pl.when(place.part > 0)
        def _():
            edge_copy(0, place.wide).wait_send()

        @pl.when(place.part < place.parts - 1)
        def _():
            edge_copy(1, place.wide).wait_send()

        others = pl.ds(width, 2 * width)
        if layer > 0:
            for part in range(2):
                span = pl.ds(part * half, half)
                acc[:, span] += multiply_back(made[:, others], wqkv[span, others])

    home_args = (lambda s: grads.at[s], home_send, home_recv)
    for part in range(2):
        at = pl.ds(part * (rows // 2), rows // 2)
        low[at] = (acc[at] + multiply_back(made[at, others], wqkv[:, others])).astype(jnp.bfloat16)
        for b in range(part * (seqs // 2), (part + 1) * (seqs // 2)):
            place.send_home_block(b, low.at[pl.ds(b * tok, tok)], *home_args, home_own)
        if fast and part == 0:
            prefix_sum.middle(0)
    if fast:
        prefix_sum.last(0)
    for s in range(seqs):
        place.got_home(s, low.at[pl.ds(0, tok)], *home_args, home_own)
        place.got_home(s, out_rows(0), *out_args, out_own)
    place.sent_home(low.at[pl.ds(0, tok)], *home_args)
    place.sent_home(out_rows(0), *out_args)
    if fast:
        for layer in order:
            prefix_sum.finish(layer)


def backward(fast, y_low, cot, full, w_qkv, w_out, q, k, v, unit, scale, slope, context, lse, segments, gains, prefix, seqs):
    rows, width = y_low.shape
    layers, rim, tok = w_qkv.shape[0], PAIR_MAX, rows // seqs
    low, full_type = jnp.bfloat16, jnp.float32
    shape = jax.ShapeDtypeStruct
    dma = pltpu.SemaphoreType.DMA
    vmem = pltpu.VMEM
    return pl.pallas_call(
        functools.partial(backward_kernel, fast, seqs, tok, rim),
        out_shape=(shape((seqs, tok, width), low), shape((seqs, tok, width), low), shape(prefix.shape, full_type)),
        in_specs=[pl.BlockSpec(memory_space=pl.ANY)] * 12 + [pl.BlockSpec(memory_space=pltpu.VMEM)] * 4,
        out_specs=(pl.BlockSpec(memory_space=pl.ANY),) * 2 + (pl.BlockSpec(memory_space=pltpu.VMEM),),
        scratch_shapes=[
            vmem(w_qkv.shape[1:], low), vmem((2,) + w_out.shape[1:], low), vmem((2, rows, width), low),
            vmem((2, rows + 2 * rim, width), low), vmem((2, rows + 2 * rim, width), low),
            vmem((2, rows, width), low), vmem((2, rows, width), low), vmem((2, rows, LANES), full_type), vmem((2, rows, LANES), full_type),
            vmem((2, SPAN, width), low), vmem((2, SPAN, width), low), vmem((2, rows, SPAN), low),
            vmem((rows, width), low), vmem((rows, width), full_type), vmem((rows, width), low), vmem((rows, width), low),
            vmem((rows, 3 * width), low), vmem((rows + 2 * rim, width), full_type), vmem((rows + 2 * rim, width), full_type),
            vmem((layers, 2, rim, 2 * width), low), vmem((layers, 2, rim, 2 * width), low), vmem((rows, width), low),
            vmem((seqs, prefix.shape[2] + tok + 2 * rim, tok), full_type),
            dma((layers + 1, 10)), dma((2, 3)), dma, dma((seqs,)), dma, dma, dma((seqs,)), dma, dma((layers, 2)), dma((layers, 2)),
        ] + (prefix_scratch(prefix.shape) if fast else []),
        compiler_params=pltpu.CompilerParams(collective_id=1, has_side_effects=True, vmem_limit_bytes=67043328),
    )(y_low, cot, full, w_qkv, w_out, q, k, v, unit, scale, slope, context, lse, segments, gains, prefix)


def local(
    tokens,
    segments,
    w_qkv,
    b_qkv,
    w_out,
    b_out,
    norm_gain,
    norm_bias,
    w_up,
    b_up,
    w_down,
    b_down,
    prefix,
    cotangent,
):
    seqs = tokens.shape[0]
    fast = lax.axis_size("wide") == 8 and lax.axis_size("rows") == 4
    full_in = w_up
    if not fast:
        full_in = jnp.stack([lax.all_gather(w, "wide", axis=1, tiled=True) for w in (w_up, w_down)], axis=1)
    y_low, cot, full, q, k, v, unit, scale, slope, lse, context = forward(
        fast, tokens, cotangent, w_qkv, w_out, w_up, w_down, full_in, segments, b_qkv, b_out, norm_gain, norm_bias,
        b_up.astype(jnp.float32).reshape(1, -1), b_down, prefix,
    )
    output, grads, prefix_grads = backward(
        fast, y_low, cot, full if fast else full_in, w_qkv, w_out, q, k, v, unit, scale, slope, context, lse, segments, norm_gain, prefix, seqs
    )
    if not fast:
        prefix_grads = lax.psum(prefix_grads, ("rows", "wide"))
    return output, grads.astype(jnp.float32), prefix_grads


def solution(mesh):
    return jax.shard_map(
        local,
        mesh=mesh,
        in_specs=(
            P("rows", "wide", None),
            P("rows", None),
            P(),
            P(),
            P(),
            P(),
            P(),
            P(),
            P(None, "wide", None),
            P(None, "wide"),
            P(None, "wide", None),
            P(),
            P(),
            P("rows", "wide", None),
        ),
        out_specs=(P("rows", "wide", None), P("rows", "wide", None), P()),
        check_vma=False,
    )
```

```python
import functools
import math

import jax
import jax.numpy as jnp
from jax import lax
from jax.experimental import pallas as pl
from jax.experimental.pallas import tpu as pltpu
from jax.sharding import PartitionSpec as P

HEADS = 16
PAIR_MAX = 128
MESH = pl.DeviceIdType.MESH
LANES = 128
SPAN = 1024
ROOT_HALF = math.sqrt(0.5)


def multiply(left, right):
    return jnp.dot(left, right, preferred_element_type=jnp.float32)


def multiply_back(left, right):
    return lax.dot_general(left, right, (((1,), (1,)), ((), ())), preferred_element_type=jnp.float32)


def multiply_first(left, right):
    return lax.dot_general(left, right, (((0,), (0,)), ((), ())), preferred_element_type=jnp.float32)


def two_heads(rows):
    half = rows.shape[1] // 2
    lane = lax.broadcasted_iota(jnp.int32, rows.shape, 1)
    nothing = jnp.zeros_like(rows)
    return jnp.concatenate([jnp.where(lane < half, rows, nothing), jnp.where(lane >= half, rows, nothing)], axis=0)


def own_heads(columns):
    half, count = columns.shape[0] // 2, columns.shape[1] // 2
    place = lax.broadcasted_iota(jnp.int32, (columns.shape[0], count), 0)
    return jnp.where(place < half, columns[:, :count], columns[:, count:]).T


def attend(blocks, rows, rim, pair, q_ref, k_ref, v_ref, prefix_ref, hide_ref, context_ref, lse_ref):
    lanes = pl.ds(pl.multiple_of(pair * 128, 128), 128)
    for block in range(blocks):
        here = pl.ds(block * rows, rows)
        window = pl.ds(block * rows, rows + 2 * rim)
        queries = two_heads(q_ref[here, lanes])
        hide = hide_ref[block]
        keys = jnp.concatenate([prefix_ref[0, :, lanes], k_ref[window, lanes]], axis=0)
        values = jnp.concatenate([prefix_ref[1, :, lanes], v_ref[window, lanes]], axis=0)
        scores = multiply_back(keys, queries) + jnp.concatenate([hide, hide], axis=1)
        top = jnp.max(scores, axis=0, keepdims=True)
        scores = jnp.exp(scores - top)
        total = jnp.sum(scores, axis=0, keepdims=True)
        share = 1.0 / total
        columns = multiply_first(values, scores.astype(jnp.bfloat16))
        context_ref[here, lanes] = own_heads(columns * share).astype(jnp.bfloat16)
        lse_ref[pair * blocks + block] = top + jnp.log(total)


def attend_back(
    blocks, rows, rim, pair, q_ref, k_ref, v_ref, prefix_ref, hide_ref, lse_ref, context_ref, grad_ref, dq_ref, dk_ref, dv_ref, dp_ref, scale
):
    lanes = pl.ds(pl.multiple_of(pair * 128, 128), 128)
    for block in range(blocks):
        here = pl.ds(block * rows, rows)
        grad = grad_ref[here, lanes]
        queries, grads = two_heads(q_ref[here, lanes]), two_heads(grad)
        shared = (grad.astype(jnp.float32) * context_ref[here, lanes].astype(jnp.float32)).T
        half = shared.shape[0] // 2
        dots = jnp.concatenate(
            [jnp.sum(shared[:half], axis=0, keepdims=True), jnp.sum(shared[half:], axis=0, keepdims=True)], axis=1
        )
        lse = lse_ref[pair * blocks + block]
        window = pl.ds(block * rows, rows + 2 * rim)
        keys = jnp.concatenate([prefix_ref[0, :, lanes], k_ref[window, lanes]], axis=0)
        values = jnp.concatenate([prefix_ref[1, :, lanes], v_ref[window, lanes]], axis=0)
        hide = hide_ref[block]
        probs = jnp.exp(multiply_back(keys, queries) + (jnp.concatenate([hide, hide], axis=1) - lse))
        grad_scores = (probs * (multiply_back(values, grads) - dots)).astype(jnp.bfloat16)
        new_values = multiply(probs.astype(jnp.bfloat16), grads)
        new_keys = multiply(grad_scores, queries)
        columns = multiply_first(keys, grad_scores)
        count = prefix_ref.shape[1]
        old, fresh = pl.ds(block * rows, 2 * rim), pl.ds(block * rows + 2 * rim, rows)
        if block == 0:
            dk_ref[window, lanes], dv_ref[window, lanes] = new_keys[count:], new_values[count:]
            dp_ref[0, :, lanes], dp_ref[1, :, lanes] = new_keys[:count], new_values[:count]
        else:
            dk_ref[old, lanes] += new_keys[count : count + 2 * rim]
            dv_ref[old, lanes] += new_values[count : count + 2 * rim]
            dk_ref[fresh, lanes], dv_ref[fresh, lanes] = new_keys[count + 2 * rim :], new_values[count + 2 * rim :]
            dp_ref[0, :, lanes] += new_keys[:count]
            dp_ref[1, :, lanes] += new_values[:count]
        dq_ref[here, lanes] = (own_heads(columns) * scale).astype(jnp.bfloat16)


def gelu_pair(values):
    size = jnp.abs(values) * ROOT_HALF
    bell = jnp.exp(values * values * -0.5)
    t = 1.0 / (1.0 + 0.3275911 * size)
    series = ((((1.061405429 * t - 1.453152027) * t + 1.421413741) * t - 0.284496736) * t + 0.254829592) * t
    tail = 0.5 * series * bell
    below = jnp.where(values < 0, tail, 1.0 - tail)
    return values * below, below + values * bell * (1.0 / math.sqrt(2.0 * math.pi))


def normalize(values):
    center = values - jnp.mean(values, axis=-1, keepdims=True)
    scale = lax.rsqrt(jnp.mean(center * center, axis=-1, keepdims=True) + 1e-05)
    return center * scale, scale


def norm_grad(grad, unit, scale, gain):
    inner = grad * gain
    first = jnp.mean(inner, axis=-1, keepdims=True)
    second = jnp.mean(inner * unit, axis=-1, keepdims=True)
    return scale * (inner - first - unit * second)


def each(count, step, body):
    @pl.loop(0, count)
    def _(i):
        body(pl.ds(pl.multiple_of(i * step, step), step))


class Place:
    def __init__(self, seqs, tok):
        self.seqs, self.tok, self.rows = seqs, tok, seqs * tok
        self.wide_size = lax.axis_size("wide")
        self.parts = self.wide_size // seqs
        self.row, self.wide = lax.axis_index("rows"), lax.axis_index("wide")
        self.seq, self.part = lax.div(self.wide, self.parts), lax.rem(self.wide, self.parts)

    def others(self, body):
        @pl.loop(1, self.wide_size)
        def _(step):
            body(lax.rem(self.wide + step, self.wide_size))

    def barrier(self, more):
        sem = pltpu.get_barrier_semaphore()
        self.others(lambda other: pl.semaphore_signal(sem, inc=1, device_id=(self.row, other), device_id_type=MESH))
        for device in more:
            pl.semaphore_signal(sem, inc=1, device_id=device, device_id_type=MESH)
        pl.semaphore_wait(sem, self.wide_size - 1 + len(more))

    def remote(self, src, dst, send, recv, device):
        return pltpu.make_async_remote_copy(
            src_ref=src, dst_ref=dst, send_sem=send, recv_sem=recv, device_id=device, device_id_type=MESH
        )

    def send_out(self, parts, target, send, recv, own):
        block = lax.rem(self.wide, self.seqs)
        for s in range(self.seqs):
            goal = s * self.parts + lax.div(self.wide, self.seqs)

            @pl.when(goal != self.wide)
            def _():
                self.remote(parts(s), target(block), send, recv.at[block], (self.row, goal)).start()

            @pl.when(goal == self.wide)
            def _():
                pltpu.make_async_copy(parts(s), target(block), own).start()

    def sent_out(self, parts, target, send, recv, own):
        block = lax.rem(self.wide, self.seqs)
        for s in range(self.seqs):
            goal = s * self.parts + lax.div(self.wide, self.seqs)

            @pl.when(goal != self.wide)
            def _():
                self.remote(parts(s), target(block), send, recv.at[block], (self.row, goal)).wait_send()

    def got_out(self, parts, target, send, recv, own):
        for b in range(self.seqs):
            source = self.part * self.seqs + b

            @pl.when(source != self.wide)
            def _():
                self.remote(parts(0), target(b), send, recv.at[b], (self.row, self.wide)).wait_recv()

            @pl.when(source == self.wide)
            def _():
                pltpu.make_async_copy(parts(0), target(b), own).wait()

    def send_home_block(self, b, part, target, send, recv, own):
        goal = self.part * self.seqs + b

        @pl.when(goal != self.wide)
        def _():
            self.remote(part, target(self.seq), send, recv.at[self.seq], (self.row, goal)).start()

        @pl.when(goal == self.wide)
        def _():
            pltpu.make_async_copy(part, target(self.seq), own).start()

    def sent_home(self, part, target, send, recv):
        for b in range(self.seqs):
            goal = self.part * self.seqs + b

            @pl.when(goal != self.wide)
            def _():
                self.remote(part, target(self.seq), send, recv.at[self.seq], (self.row, goal)).wait_send()

    def got_home(self, s, part, target, send, recv, own):
        source = s * self.parts + lax.div(self.wide, self.seqs)

        @pl.when(source != self.wide)
        def _():
            self.remote(part, target(s), send, recv.at[s], (self.row, self.wide)).wait_recv()

        @pl.when(source == self.wide)
        def _():
            pltpu.make_async_copy(part, target(s), own).wait()


def fill_hide(place, rim, segments, hide):
    count = hide.shape[1] - place.tok - 2 * rim
    base = place.part * place.rows

    def ids(start):
        start = pl.multiple_of(start, LANES)
        rows = segments[:, pl.ds(start, LANES)].astype(jnp.float32)
        here = lax.broadcasted_iota(jnp.int32, rows.shape, 0) == place.seq
        return jnp.sum(jnp.where(here, rows, 0.0), axis=0, keepdims=True)

    for b in range(place.seqs):
        hide[b, pl.ds(0, count)] = jnp.zeros((count, place.tok), jnp.float32)
        own = ids(base + b * place.tok)
        for chunk in range((place.tok + 2 * rim) // LANES):
            start = base + b * place.tok - rim + chunk * LANES
            safe = jnp.clip(start, 0, segments.shape[1] - LANES)
            keys = jnp.where(start == safe, ids(safe), -1.0)
            keys = jnp.broadcast_to(keys, (LANES, LANES)).T
            hide[b, pl.ds(count + chunk * LANES, LANES)] = jnp.where(keys == own, 0.0, -1e30)


class Gather:
    def __init__(self, shards, full, sems):
        self.shards = shards
        self.full = full
        self.send_sem, self.zs, self.xs, self.ys, self.ds, self.cz, self.cx, self.cy, self.cd, self.cown, self.own = sems
        self.row = lax.axis_index("rows")
        self.wide = lax.axis_index("wide")
        self.z, self.core = lax.div(self.wide, 2), lax.rem(self.wide, 2)
        self.shard_rows = shards[0].shape[1]
        self.unit_rows = self.shard_rows // 4
        self.row_x = self.row + 1 - 2 * lax.rem(self.row, 2)
        self.row_y = lax.rem(self.row + 2, 4)
        self.row_d = 3 - self.row

    def unit(self, layer, member, z, core, quarter):
        start = (z * 2 + core) * self.shard_rows + quarter * self.unit_rows
        return self.full.at[layer, member, pl.ds(pl.multiple_of(start, self.unit_rows), self.unit_rows)]

    def shard(self, layer, member, z, core):
        start = (z * 2 + core) * self.shard_rows
        return self.full.at[layer, member, pl.ds(pl.multiple_of(start, self.shard_rows), self.shard_rows)]

    def copy(self, src, dst, recv, kind):
        if kind == "x":
            device = (self.row_x, self.wide)
        elif kind == "y":
            device = (self.row_y, self.wide)
        elif kind == "core":
            device = (self.row, self.z * 2 + 1 - self.core)
        else:
            device = (self.row, self.wide + 2 - 4 * kind)
        return pltpu.make_async_remote_copy(
            src_ref=src, dst_ref=dst, send_sem=self.send_sem, recv_sem=recv, device_id=device, device_id_type=MESH
        )

    def start_z(self, layer):
        for member in range(2):
            start = pl.multiple_of(self.row * self.unit_rows, self.unit_rows)
            mine = self.shards[member].at[layer, pl.ds(start, self.unit_rows)]
            here = self.unit(layer, member, self.z, self.core, self.row)

            @pl.when(self.z < 3)
            def _():
                self.copy(mine, here, self.zs.at[layer, member, 0, 0], 0).start()

            @pl.when(self.z > 0)
            def _():
                self.copy(mine, here, self.zs.at[layer, member, 0, 1], 1).start()

    def start_core(self, layer):
        for member in range(2):
            place = self.shard(layer, member, self.z, self.core)
            pltpu.make_async_copy(self.shards[member].at[layer], place, self.own.at[layer, member]).start()
            self.copy(self.shards[member].at[layer], place, self.cown.at[layer, member], "core").start()

    def slot(self, i):
        near = jnp.minimum(self.z, 3 - self.z)
        far_side = 1 - lax.div(self.z, 2)
        both = jnp.minimum(lax.div(i, jnp.maximum(2 * near, 1)), 1) + (1 - jnp.minimum(near, 1))
        both = 1 - jnp.minimum(both, 1)
        step = both * lax.div(i, 2) + (1 - both) * (i - near)
        side = both * lax.rem(i, 2) + (1 - both) * far_side
        return step, side, self.z + (1 + step) * (2 * side - 1)

    def on_z(self, layer, i):
        step, side, origin = self.slot(i)
        for member in range(2):
            unit = self.unit(layer, member, origin, self.core, self.row)
            self.copy(unit, unit, self.zs.at[layer, member, step, side], "x").wait_recv()
            target = self.z + 1 - 2 * side

            @pl.when((target >= 0) & (target < 4))
            def _():
                self.copy(unit, unit, self.zs.at[layer, member, step + 1, side], side).start()

            self.copy(unit, unit, self.xs.at[layer, member, step, side], "x").start()
            self.copy(unit, unit, self.ys.at[layer, member, step, side], "y").start()
            self.copy(unit, unit, self.cz.at[layer, member, step, side], "core").start()

    def on_first(self, layer, _):
        self.on_z(layer, 0)

        @pl.when((self.z > 0) & (self.z < 3))
        def _():
            self.on_z(layer, 1)

    def on_second(self, layer, _):
        self.on_z(layer, 1 + jnp.minimum(self.z, 1) * jnp.minimum(3 - self.z, 1))

    def on_third(self, layer, _):
        @pl.when((self.z == 0) | (self.z == 3))
        def _():
            self.on_z(layer, 2)

    def on_xy(self, layer, i):
        step, side, origin = self.slot(i)
        for member in range(2):
            unit = self.unit(layer, member, origin, self.core, self.row_x)
            self.copy(unit, unit, self.xs.at[layer, member, step, side], "x").wait_recv()
            if member == 0:
                self.copy(unit, unit, self.ds.at[layer, member, step, side], "y").start()
            self.copy(unit, unit, self.cx.at[layer, member, step, side], "core").start()
            unit = self.unit(layer, member, origin, self.core, self.row_y)
            self.copy(unit, unit, self.ys.at[layer, member, step, side], "y").wait_recv()
            if member == 1:
                self.copy(unit, unit, self.ds.at[layer, member, step, side], "x").start()
            self.copy(unit, unit, self.cy.at[layer, member, step, side], "core").start()

    def on_d(self, layer, i):
        step, side, origin = self.slot(i)
        for member in range(2):
            unit = self.unit(layer, member, origin, self.core, self.row_d)
            self.copy(unit, unit, self.ds.at[layer, member, step, side], "x").wait_recv()
            self.copy(unit, unit, self.cd.at[layer, member, step, side], "core").start()

    def on_core(self, layer, i):
        step, side, origin = self.slot(i)
        for member in range(2):
            for sem, quarter in ((self.cz, self.row), (self.cx, self.row_x), (self.cy, self.row_y), (self.cd, self.row_d)):
                unit = self.unit(layer, member, origin, 1 - self.core, quarter)
                self.copy(unit, unit, sem.at[layer, member, step, side], "core").wait_recv()

    def on_own(self, layer):
        for member in range(2):
            place = self.shard(layer, member, self.z, self.core)
            pltpu.make_async_copy(self.shards[member].at[layer], place, self.own.at[layer, member]).wait()
            place = self.shard(layer, member, self.z, 1 - self.core)
            self.copy(place, place, self.cown.at[layer, member], "core").wait_recv()

    def drain(self, layers):
        def wait(units):
            span = self.full.at[0, 0, pl.ds(0, units * self.unit_rows)]
            self.copy(span, span, self.own.at[0, 0], "core").wait_send()

        @pl.loop(0, layers)
        def _(layer):
            wait(8)

            @pl.when(self.z < 3)
            def _():
                wait(2)

            @pl.when(self.z > 0)
            def _():
                wait(2)

            @pl.loop(0, 3)
            def _(i):
                step, side, origin = self.slot(i)
                target = self.z + 1 - 2 * side

                @pl.when((target >= 0) & (target < 4))
                def _():
                    wait(2)

                wait(14)


class PrefixSum:
    def __init__(self, place, parts, rounded, inbox, planes, total, sems):
        self.parts, self.rounded, self.inbox, self.planes, self.total = parts, rounded, inbox, planes, total
        self.send_sem, self.in_sem, self.plane_sem, self.total_sem = sems
        self.row = place.row
        self.z, self.core = lax.div(place.wide, 2), lax.rem(place.wide, 2)
        self.me = self.row * 2 + self.core
        self.size = inbox.shape[2]

    def peers(self, body):
        @pl.loop(1, 8)
        def _(step):
            body(lax.rem(self.me + step, 8))

    def others(self):
        return [(lax.rem(self.row + step, 4), self.z * 2 + core) for step in range(1, 4) for core in range(2)]

    def piece(self, ref, layer, index):
        start = lax.rem(index, 4) * self.size
        return ref.at[layer, lax.div(index, 4), pl.ds(pl.multiple_of(start, self.size), self.size)]

    def copy(self, src, dst, recv, row, wide):
        return pltpu.make_async_remote_copy(
            src_ref=src, dst_ref=dst, send_sem=self.send_sem, recv_sem=recv, device_id=(row, wide), device_id_type=MESH
        )

    def in_copy(self, layer, peer, origin):
        return self.copy(
            self.piece(self.rounded, layer, peer), self.inbox.at[layer, origin], self.in_sem.at[layer, origin],
            lax.div(peer, 2), self.z * 2 + lax.rem(peer, 2),
        )

    def plane_copy(self, layer, z, origin):
        place = self.planes.at[layer, origin]
        return self.copy(place, place, self.plane_sem.at[layer, origin], self.row, z * 2 + self.core)

    def total_copy(self, layer, peer, origin):
        place = self.piece(self.total, layer, origin)
        return self.copy(place, place, self.total_sem.at[layer, origin], lax.div(peer, 2), self.z * 2 + lax.rem(peer, 2))

    def planes_others(self, body):
        @pl.loop(1, 4)
        def _(step):
            body(lax.rem(self.z + step, 4))

    def start(self, layer):
        self.rounded[layer] = self.parts[layer].astype(jnp.bfloat16)
        self.peers(lambda peer: self.in_copy(layer, peer, self.me).start())

    def middle(self, layer):
        self.peers(lambda peer: self.in_copy(layer, self.me, peer).wait_recv())
        value = self.piece(self.parts, layer, self.me)[...]
        for step in range(1, 8):
            value += self.inbox[layer, lax.rem(self.me + step, 8)].astype(jnp.float32)
        self.planes[layer, self.z] = value
        self.planes_others(lambda z: self.plane_copy(layer, z, self.z).start())

    def last(self, layer):
        self.planes_others(lambda z: self.plane_copy(layer, self.z, z).wait_recv())
        value = self.planes[layer, 0]
        for z in range(1, 4):
            value += self.planes[layer, z]
        self.piece(self.total, layer, self.me)[...] = value
        self.peers(lambda peer: self.total_copy(layer, peer, self.me).start())

    def finish(self, layer):
        self.peers(lambda peer: self.total_copy(layer, self.me, peer).wait_recv())
        self.peers(lambda peer: self.in_copy(layer, peer, self.me).wait_send())
        self.planes_others(lambda z: self.plane_copy(layer, z, self.z).wait_send())
        self.peers(lambda peer: self.total_copy(layer, peer, self.me).wait_send())


def prefix_scratch(shape):
    layers, members, count, width = shape
    size = members * count // 8
    dma = pltpu.SemaphoreType.DMA
    return [
        pltpu.VMEM(shape, jnp.float32), pltpu.VMEM(shape, jnp.bfloat16), pltpu.VMEM((layers, 8, size, width), jnp.bfloat16),
        pltpu.VMEM((layers, 4, size, width), jnp.float32), dma, dma((layers, 8)), dma((layers, 4)), dma((layers, 8)),
    ]


def gather_sems(layers):
    return (
        [pltpu.SemaphoreType.DMA]
        + [pltpu.SemaphoreType.DMA((layers, 2, 3, 2))] * 8
        + [pltpu.SemaphoreType.DMA((layers, 2))] * 2
    )


def forward_kernel(
    fast, seqs, tok, rim,
    tokens, cotangent, w_qkv, w_out, w_up, w_down, full_in,
    segments, b_qkv, b_out, gains, shifts, b_up, b_down, prefix,
    y_low, cot_out, full_out, q_out, k_out, v_out, unit_out, scale_out, slope_out, lse_out, context_out,
    full, wqkv, wout, x, low, acc, q, k, v, halo, context, slope, unit1, unit2, scale1, scale2, lse, bias, hide,
    load_sem, store_sem, slope_sem, full_sem, tok_send, tok_recv, tok_own, cot_send, cot_recv, cot_own,
    halo_send, halo_recv, bias_send, bias_recv, bias_own,
    *gather_sem,
):
    layers, width = w_qkv.shape[0], tokens.shape[2]
    place = Place(seqs, tok)
    rows = place.rows
    gather = Gather((w_up, w_down), full, gather_sem) if fast else None
    place.barrier(((gather.row_x, place.wide), (gather.row_y, place.wide)) if fast else ())
    own_bias = bias.at[place.wide]

    def load(layer):
        return (
            pltpu.make_async_copy(w_qkv.at[layer], wqkv, load_sem.at[0]),
            pltpu.make_async_copy(w_out.at[layer], wout, load_sem.at[1]),
        )

    def put_bias(other):
        return place.remote(b_up, own_bias, bias_send, bias_recv.at[place.wide], (place.row, other))

    def got_bias(other):
        return place.remote(b_up, bias.at[other], bias_send, bias_recv.at[other], (place.row, other))

    if fast:
        gather.start_z(0)
        gather.start_core(0)
    else:
        pltpu.make_async_copy(full_in, full, full_sem.at[0]).start()
    for copy in load(0):
        copy.start()
    place.others(lambda other: put_bias(other).start())
    pltpu.make_async_copy(b_up, own_bias, bias_own).start()

    tok_args = (lambda s: tokens.at[s], lambda b: low.at[pl.ds(pl.multiple_of(b * tok, tok), tok)], tok_send, tok_recv, tok_own)
    cot_args = (lambda s: cotangent.at[s], lambda b: cot_out.at[pl.ds(pl.multiple_of(b * tok, tok), tok)], cot_send, cot_recv, cot_own)
    events = {}
    if fast:
        gather.on_first(0, 0)
        place.send_out(*tok_args)
        gather.on_second(0, 0)
        gather.on_xy(0, 0)
        events = {
            (0, "queries"): [(gather.on_third, 0, 0)],
            (0, "pair", 1): [(gather.on_xy, 0, 1)],
            (0, "pair", 4): [(gather.on_first, 1, 0), (gather.on_d, 0, 0)],
            (0, "pair", 7): [(gather.on_xy, 0, 2)],
            (0, "projected"): [(gather.on_d, 0, 1)],
            (0, "normed"): [(gather.on_second, 1, 0)],
            (0, "step", 1): [(gather.on_core, 0, 0)],
            (0, "step", 2): [(gather.on_xy, 1, 0), (gather.on_core, 0, 1), (gather.on_d, 0, 2)],
            (0, "step", 3): [(gather.on_core, 0, 2), (gather.on_third, 1, 0)],
            (1, "queries"): [(gather.on_xy, 1, 1)],
            (1, "pair", 7): [(gather.on_xy, 1, 2)],
            (1, "projected"): [(gather.on_d, 1, 0)],
            (1, "normed"): [(gather.on_d, 1, 1)],
            (1, "step", 1): [(gather.on_core, 1, 0)],
            (1, "step", 2): [(gather.on_d, 1, 2), (gather.on_core, 1, 1)],
            (1, "step", 3): [(gather.on_core, 1, 2)],
        }
    else:
        place.send_out(*tok_args)

    def tick(*when):
        for event, layer, i in events.get(when, ()):
            event(layer, i)

    def loop_tick(layer, kind, index, count):
        for n in range(count):
            if (layer, kind, n) in events:
                @pl.when(index == n)
                def _():
                    tick(layer, kind, n)

    blank = jnp.zeros((rim, width), jnp.bfloat16)

    @pl.when(place.part == 0)
    def _():
        k[pl.ds(0, rim)] = blank
        v[pl.ds(0, rim)] = blank

    @pl.when(place.part == place.parts - 1)
    def _():
        k[pl.ds(rim + rows, rim)] = blank
        v[pl.ds(rim + rows, rim)] = blank

    fill_hide(place, rim, segments, hide)
    place.got_out(*tok_args)
    if fast:
        gather.start_z(1)
        gather.start_core(1)

    def halo_copy(layer, member, side, wide):
        ref = (k, v)[member]
        return place.remote(
            ref.at[pl.ds((rows, rim)[side], rim)], halo.at[layer, member, side],
            halo_send.at[member, side], halo_recv.at[layer, member, side], (place.row, wide),
        )

    def halos(body, to):
        for side in range(2):
            @pl.when(place.part < place.parts - 1 if (side == 0) == to else place.part > 0)
            def _():
                for member in range(2):
                    body(member, side, jnp.clip(place.wide + (1 - 2 * side), 0, place.wide_size - 1))

    def got_halo(layer, member, side, wide):
        halo_copy(layer, member, side, place.wide).wait_recv()
        (k, v)[member][pl.ds((0, rim + rows)[side], rim)] = halo[layer, member, side]

    def kept(layer):
        return [
            pltpu.make_async_copy(src, dst.at[layer], store_sem.at[i])
            for i, (src, dst) in enumerate(((q, q_out), (k, k_out), (v, v_out)))
        ]

    def kept_context(layer):
        return [pltpu.make_async_copy(context, context_out.at[layer], store_sem.at[9])]

    def kept_norm(layer, which):
        unit, scale = ((unit1, scale1), (unit2, scale2))[which]
        return [
            pltpu.make_async_copy(unit, unit_out.at[layer, which], store_sem.at[3 + which]),
            pltpu.make_async_copy(scale, scale_out.at[layer, which], store_sem.at[5 + which]),
        ]

    half = width // 2
    for layer in range(layers):
        if layer > 0:
            for copy in kept(layer - 1) + kept_context(layer - 1) + kept_norm(layer - 1, 0) + kept_norm(layer - 1, 1):
                copy.wait()
        load(layer)[0].wait()
        for part in (2, 3, 4, 5, 0, 1):
            lanes = pl.ds(part * half, half)
            made = multiply(low[...], wqkv[:, lanes]) + b_qkv[layer : layer + 1, lanes]
            kind, side = part // 2, pl.ds((part % 2) * half, half)
            if kind == 0:
                q[:, side] = made.astype(jnp.bfloat16) * (1.0 / math.sqrt(width // HEADS))
            else:
                (k, v)[kind - 1][pl.ds(rim, rows), side] = made.astype(jnp.bfloat16)
            if part == 5:
                halos(lambda *at: halo_copy(layer, *at).start(), True)
        if layer + 1 < layers:
            load(layer + 1)[0].start()
        tick(layer, "queries")
        halos(lambda *at: got_halo(layer, *at), False)
        halos(lambda *at: halo_copy(layer, *at).wait_send(), True)
        for copy in kept(layer):
            copy.start()

        @pl.loop(0, width // LANES)
        def _(pair):
            attend(seqs, tok, rim, pair, q, k, v, prefix.at[layer], hide, context, lse.at[layer])
            loop_tick(layer, "pair", pair, width // LANES)

        for copy in kept_context(layer):
            copy.start()
        load(layer)[1].wait()
        for part in range(2):
            lanes = pl.ds(part * half, half)
            acc[:, lanes] = multiply(context[...], wout[:, lanes])
        if layer + 1 < layers:
            load(layer + 1)[1].start()
        tick(layer, "projected")

        def first_norm(at):
            before = low[at].astype(jnp.float32) if layer == 0 else x[at]
            unit, scale = normalize(before + acc[at] + b_out[layer : layer + 1])
            unit1[at] = unit.astype(jnp.bfloat16)
            scale1[at] = jnp.broadcast_to(scale, (scale.shape[0], LANES))
            normed = unit * gains[layer, :1] + shifts[layer, :1]
            low[at] = normed.astype(jnp.bfloat16)
            acc[at] = normed + b_down[layer : layer + 1]

        each(rows // 64, 64, first_norm)
        for copy in kept_norm(layer, 0):
            copy.start()
        tick(layer, "normed")
        if layer == 0:
            pltpu.make_async_copy(b_up, own_bias, bias_own).wait()
            place.others(lambda other: got_bias(other).wait_recv())

            place.others(lambda other: put_bias(other).wait_send())
            if not fast:
                pltpu.make_async_copy(full_in, full, full_sem.at[0]).wait()

        hidden = b_up.shape[1] // layers

        @pl.loop(0, full.shape[2] // SPAN)
        def _(i):
            spot = i
            if fast:
                @pl.when(i == 0)
                def _():
                    gather.on_own(layer)

                loop_tick(layer, "step", i, full.shape[2] // SPAN)
                origin = gather.slot(jnp.maximum(i - 1, 0))[2]
                started = jnp.minimum(i, 1)
                spot = started * origin + (1 - started) * gather.z
            units = pl.ds(pl.multiple_of(spot * SPAN, SPAN), SPAN)
            slot = lax.rem(i, 2)
            step_bias = jnp.concatenate(
                [bias[spot * (SPAN // hidden) + n, :, pl.ds(layer * hidden, hidden)] for n in range(SPAN // hidden)], axis=1
            )

            @pl.when(i > 1)
            def _():
                pltpu.make_async_copy(slope.at[slot], slope_out.at[layer, spot], slope_sem.at[slot]).wait()

            for part in range(2):
                at = pl.ds(part * (rows // 2), rows // 2)
                act, rise = gelu_pair(multiply_back(low[at], full[layer, 0, units]) + step_bias)
                slope[slot, at] = rise.astype(jnp.bfloat16)
                acc[at] += multiply(act.astype(jnp.bfloat16), full[layer, 1, units])
            pltpu.make_async_copy(slope.at[slot], slope_out.at[layer, spot], slope_sem.at[slot]).start()
            if fast:
                pltpu.make_async_copy(full.at[layer, :, units], full_out.at[layer, :, units], full_sem.at[layer]).start()

        for slot in range(2):
            pltpu.make_async_copy(slope.at[slot], slope_out.at[layer, 0], slope_sem.at[slot]).wait()

        def second_norm(at):
            unit, scale = normalize(acc[at])
            unit2[at] = unit.astype(jnp.bfloat16)
            scale2[at] = jnp.broadcast_to(scale, (scale.shape[0], LANES))
            after = unit * gains[layer, 1:] + shifts[layer, 1:]
            low[at] = after.astype(jnp.bfloat16)
            if layer + 1 < layers:
                x[at] = after

        each(rows // 64, 64, second_norm)
        for copy in kept_norm(layer, 1):
            copy.start()
        if layer == 0:
            place.send_out(*cot_args)
            tick(0, "done")
    last = [pltpu.make_async_copy(low, y_low, store_sem.at[7]), pltpu.make_async_copy(lse, lse_out, store_sem.at[8])]
    for copy in last:
        copy.start()
    place.sent_out(*tok_args)
    place.got_out(*cot_args)
    place.sent_out(*cot_args)
    for copy in last + kept(layers - 1) + kept_context(layers - 1) + kept_norm(layers - 1, 0) + kept_norm(layers - 1, 1):
        copy.wait()
    if fast:
        gather.drain(layers)
        for layer in range(layers):
            pltpu.make_async_copy(full.at[layer], full_out.at[layer], full_sem.at[layer]).wait()


def forward(fast, tokens, cotangent, w_qkv, w_out, w_up, w_down, full_in, segments, b_qkv, b_out, gains, shifts, b_up, b_down, prefix):
    seqs, tok, width = tokens.shape
    layers, rim, rows = w_qkv.shape[0], PAIR_MAX, seqs * tok
    wides = lax.axis_size("wide")
    units = w_up.shape[1] * wides
    low, full_type = jnp.bfloat16, jnp.float32
    spans = units // SPAN
    shape = jax.ShapeDtypeStruct
    dma = pltpu.SemaphoreType.DMA
    scores = (layers, width // LANES * seqs, 1, 2 * tok)
    return pl.pallas_call(
        functools.partial(forward_kernel, fast, seqs, tok, rim),
        out_shape=(
            shape((rows, width), low), shape((rows, width), low), shape((layers, 2, units, width), low),
            shape((layers, rows, width), low), shape((layers, rows + 2 * rim, width), low),
            shape((layers, rows + 2 * rim, width), low), shape((layers, 2, rows, width), low),
            shape((layers, 2, rows, LANES), full_type), shape((layers, spans, rows, SPAN), low), shape(scores, full_type),
            shape((layers, rows, width), low),
        ),
        in_specs=[pl.BlockSpec(memory_space=pl.ANY)] * 7 + [pl.BlockSpec(memory_space=pltpu.VMEM)] * 8,
        out_specs=(pl.BlockSpec(memory_space=pl.ANY),) * 11,
        scratch_shapes=[
            pltpu.VMEM((layers, 2, units, width), low), pltpu.VMEM(w_qkv.shape[1:], low), pltpu.VMEM(w_out.shape[1:], low),
            pltpu.VMEM((rows, width), full_type), pltpu.VMEM((rows, width), low), pltpu.VMEM((rows, width), full_type),
            pltpu.VMEM((rows, width), low), pltpu.VMEM((rows + 2 * rim, width), low), pltpu.VMEM((rows + 2 * rim, width), low),
            pltpu.VMEM((layers, 2, 2, rim, width), low), pltpu.VMEM((rows, width), low), pltpu.VMEM((2, rows, SPAN), low),
            pltpu.VMEM((rows, width), low), pltpu.VMEM((rows, width), low),
            pltpu.VMEM((rows, LANES), full_type), pltpu.VMEM((rows, LANES), full_type),
            pltpu.VMEM(scores, full_type), pltpu.VMEM((wides,) + b_up.shape, full_type),
            pltpu.VMEM((seqs, prefix.shape[2] + tok + 2 * rim, tok), full_type),
            dma((2,)), dma((10,)), dma((2,)), dma((layers,)), dma, dma((seqs,)), dma, dma, dma((seqs,)), dma,
            dma((2, 2)), dma((layers, 2, 2)), dma, dma((wides,)), dma,
        ] + (gather_sems(layers) if fast else []),
        compiler_params=pltpu.CompilerParams(collective_id=0, has_side_effects=True, vmem_limit_bytes=67043328),
    )(tokens, cotangent, w_qkv, w_out, w_up, w_down, full_in, segments, b_qkv, b_out, gains, shifts, b_up, b_down, prefix)


def backward_kernel(
    fast, seqs, tok, rim,
    y_low, cot_in, full, w_qkv, w_out, q_in, k_in, v_in, unit_in, scale_in, slope_in, context_in,
    lse, segments, gains, prefix,
    out, grads, prefix_grads,
    wqkv, wout, q, k, v, unit1, unit2, scale1, scale2, up, down, slope, cot, acc, low, context, made, dk, dv, edge, edge_in, saved, hide,
    load_sem, ffn_sem, out_send, out_recv, out_own, home_send, home_recv, home_own, edge_send, edge_recv,
    *sums,
):
    layers, width = w_qkv.shape[0], w_qkv.shape[1]
    place = Place(seqs, tok)
    rows = place.rows
    prefix_sum, prefix_parts = None, prefix_grads
    if fast:
        prefix_parts = sums[0]
        prefix_sum = PrefixSum(place, *sums[:4], prefix_grads, sums[4:])
    place.barrier(prefix_sum.others() if fast else ())
    spans = slope_in.shape[1]

    def out_rows(b):
        return y_low.at[pl.ds(b * tok, tok)]

    out_args = (lambda s: out.at[s], out_send, out_recv)
    for b in range(seqs):
        place.send_home_block(b, out_rows(b), *out_args, out_own)

    cot_copy = pltpu.make_async_copy(cot_in, cot, load_sem.at[layers, 0])
    cot_copy.start()

    def loads(layer):
        pairs = (
            (unit_in.at[layer, 1], unit2), (scale_in.at[layer, 1], scale2), (unit_in.at[layer, 0], unit1),
            (scale_in.at[layer, 0], scale1), (w_out.at[layer], wout), (q_in.at[layer], q), (k_in.at[layer], k),
            (v_in.at[layer], v),
        )
        copies = [pltpu.make_async_copy(src, dst.at[layer % 2], load_sem.at[layer, i]) for i, (src, dst) in enumerate(pairs)]
        return copies + [
            pltpu.make_async_copy(w_qkv.at[layer], wqkv, load_sem.at[layer, 8]),
            pltpu.make_async_copy(context_in.at[layer], saved, load_sem.at[layer, 9]),
        ]

    def ffn_loads(layer, i):
        slot = lax.rem(i, 2)
        units = pl.ds(pl.multiple_of(i * SPAN, SPAN), SPAN)
        return [
            pltpu.make_async_copy(full.at[layer, 1, units], down.at[slot], ffn_sem.at[slot, 0]),
            pltpu.make_async_copy(slope_in.at[layer, i], slope.at[slot], ffn_sem.at[slot, 1]),
            pltpu.make_async_copy(full.at[layer, 0, units], up.at[slot], ffn_sem.at[slot, 2]),
        ]

    order = list(reversed(range(layers)))
    for copy in loads(order[0])[:2]:
        copy.start()
    for i in range(2):
        for copy in ffn_loads(order[0], i):
            copy.start()
    for copy in loads(order[0])[2:]:
        copy.start()
    half = width // 2
    fill_hide(place, rim, segments, hide)
    for layer in order:
        here = layer % 2
        mine = loads(layer)
        if layer == order[0]:
            cot_copy.wait()
        if layer > 0:
            for copy in loads(layer - 1)[:8]:
                copy.start()
        if layer < order[0]:
            mine[8].start()
            mine[9].start()
        mine[0].wait()
        mine[1].wait()

        def second_norm(at):
            grad = cot[at].astype(jnp.float32) if layer == order[0] else acc[at]
            grad = norm_grad(grad, unit2[here, at].astype(jnp.float32), scale2[here, at, :1], gains[layer, 1:])
            acc[at] = grad
            low[at] = grad.astype(jnp.bfloat16)

        each(rows // 64, 64, second_norm)
        if fast and layer + 1 < layers:
            prefix_sum.middle(layer + 1)

        @pl.loop(0, spans)
        def _(i):
            slot = lax.rem(i, 2)
            for copy in ffn_loads(layer, i):
                copy.wait()
            for part in range(2):
                at = pl.ds(part * (rows // 2), rows // 2)
                grad = multiply_back(low[at], down[slot]) * slope[slot, at].astype(jnp.float32)
                acc[at] += multiply(grad.astype(jnp.bfloat16), up[slot])

            @pl.when(i + 2 < spans)
            def _():
                for copy in ffn_loads(layer, i + 2):
                    copy.start()

        if layer > 0:
            for i in range(2):
                for copy in ffn_loads(layer - 1, i):
                    copy.start()
        mine[2].wait()
        mine[3].wait()

        def first_norm(at):
            grad = norm_grad(acc[at], unit1[here, at].astype(jnp.float32), scale1[here, at, :1], gains[layer, :1])
            acc[at] = grad
            low[at] = grad.astype(jnp.bfloat16)

        each(rows // 64, 64, first_norm)
        if fast and layer + 1 < layers:
            prefix_sum.last(layer + 1)
        mine[4].wait()
        for part in range(2):
            span = pl.ds(part * half, half)
            context[:, span] = multiply_back(low[...], wout[here, span]).astype(jnp.bfloat16)
        for copy in mine[5:8] + mine[9:]:
            copy.wait()

        @pl.loop(0, width // LANES)
        def _(pair):
            attend_back(
                seqs, tok, rim, pair, q.at[here], k.at[here], v.at[here], prefix.at[layer], hide, lse.at[layer], saved, context,
                made, dk, dv, prefix_parts.at[layer], 1.0 / math.sqrt(width // HEADS),
            )

        if fast:
            prefix_sum.start(layer)

        low_edge, high_edge, own_rows = pl.ds(0, rim), pl.ds(rim + rows, rim), pl.ds(rim, rows)
        for member, ref in enumerate((dk, dv)):
            lanes = pl.ds(member * width, width)
            edge[layer, 0, :, lanes] = ref[low_edge].astype(jnp.bfloat16)
            edge[layer, 1, :, lanes] = ref[high_edge].astype(jnp.bfloat16)

        def edge_copy(side, wide):
            return place.remote(
                edge.at[layer, side], edge_in.at[layer, side], edge_send.at[layer, side], edge_recv.at[layer, side], (place.row, wide)
            )

        mine[8].wait()
        for part in range(2):
            span = pl.ds(part * half, half)
            acc[:, span] += multiply_back(made[:, pl.ds(0, width)], wqkv[span, pl.ds(0, width)])
            if part == 0:
                @pl.when(place.part > 0)
                def _():
                    edge_copy(0, place.wide - 1).start()

                @pl.when(place.part < place.parts - 1)
                def _():
                    edge_copy(1, place.wide + 1).start()

        @pl.when(place.part < place.parts - 1)
        def _():
            edge_copy(0, place.wide).wait_recv()
            for member, ref in enumerate((dk, dv)):
                ref[pl.ds(rows, rim)] += edge_in[layer, 0, :, pl.ds(member * width, width)].astype(jnp.float32)

        @pl.when(place.part > 0)
        def _():
            edge_copy(1, place.wide).wait_recv()
            for member, ref in enumerate((dk, dv)):
                ref[pl.ds(rim, rim)] += edge_in[layer, 1, :, pl.ds(member * width, width)].astype(jnp.float32)

        for member, ref in enumerate((dk, dv)):
            def lower(at):
                made[at, pl.ds((1 + member) * width, width)] = ref[pl.ds(pl.multiple_of(at.start + rim, 64), 64)].astype(jnp.bfloat16)

            each(rows // 64, 64, lower)

        @pl.when(place.part > 0)
        def _():
            edge_copy(0, place.wide).wait_send()

        @pl.when(place.part < place.parts - 1)
        def _():
            edge_copy(1, place.wide).wait_send()

        others = pl.ds(width, 2 * width)
        if layer > 0:
            for part in range(2):
                span = pl.ds(part * half, half)
                acc[:, span] += multiply_back(made[:, others], wqkv[span, others])

    home_args = (lambda s: grads.at[s], home_send, home_recv)
    for part in range(2):
        at = pl.ds(part * (rows // 2), rows // 2)
        low[at] = (acc[at] + multiply_back(made[at, others], wqkv[:, others])).astype(jnp.bfloat16)
        for b in range(part * (seqs // 2), (part + 1) * (seqs // 2)):
            place.send_home_block(b, low.at[pl.ds(b * tok, tok)], *home_args, home_own)
        if fast and part == 0:
            prefix_sum.middle(0)
    if fast:
        prefix_sum.last(0)
    for s in range(seqs):
        place.got_home(s, low.at[pl.ds(0, tok)], *home_args, home_own)
        place.got_home(s, out_rows(0), *out_args, out_own)
    place.sent_home(low.at[pl.ds(0, tok)], *home_args)
    place.sent_home(out_rows(0), *out_args)
    if fast:
        for layer in order:
            prefix_sum.finish(layer)


def backward(fast, y_low, cot, full, w_qkv, w_out, q, k, v, unit, scale, slope, context, lse, segments, gains, prefix, seqs):
    rows, width = y_low.shape
    layers, rim, tok = w_qkv.shape[0], PAIR_MAX, rows // seqs
    low, full_type = jnp.bfloat16, jnp.float32
    shape = jax.ShapeDtypeStruct
    dma = pltpu.SemaphoreType.DMA
    vmem = pltpu.VMEM
    return pl.pallas_call(
        functools.partial(backward_kernel, fast, seqs, tok, rim),
        out_shape=(shape((seqs, tok, width), low), shape((seqs, tok, width), low), shape(prefix.shape, full_type)),
        in_specs=[pl.BlockSpec(memory_space=pl.ANY)] * 12 + [pl.BlockSpec(memory_space=pltpu.VMEM)] * 4,
        out_specs=(pl.BlockSpec(memory_space=pl.ANY),) * 2 + (pl.BlockSpec(memory_space=pltpu.VMEM),),
        scratch_shapes=[
            vmem(w_qkv.shape[1:], low), vmem((2,) + w_out.shape[1:], low), vmem((2, rows, width), low),
            vmem((2, rows + 2 * rim, width), low), vmem((2, rows + 2 * rim, width), low),
            vmem((2, rows, width), low), vmem((2, rows, width), low), vmem((2, rows, LANES), full_type), vmem((2, rows, LANES), full_type),
            vmem((2, SPAN, width), low), vmem((2, SPAN, width), low), vmem((2, rows, SPAN), low),
            vmem((rows, width), low), vmem((rows, width), full_type), vmem((rows, width), low), vmem((rows, width), low),
            vmem((rows, 3 * width), low), vmem((rows + 2 * rim, width), full_type), vmem((rows + 2 * rim, width), full_type),
            vmem((layers, 2, rim, 2 * width), low), vmem((layers, 2, rim, 2 * width), low), vmem((rows, width), low),
            vmem((seqs, prefix.shape[2] + tok + 2 * rim, tok), full_type),
            dma((layers + 1, 10)), dma((2, 3)), dma, dma((seqs,)), dma, dma, dma((seqs,)), dma, dma((layers, 2)), dma((layers, 2)),
        ] + (prefix_scratch(prefix.shape) if fast else []),
        compiler_params=pltpu.CompilerParams(collective_id=1, has_side_effects=True, vmem_limit_bytes=67043328),
    )(y_low, cot, full, w_qkv, w_out, q, k, v, unit, scale, slope, context, lse, segments, gains, prefix)


def local(
    tokens,
    segments,
    w_qkv,
    b_qkv,
    w_out,
    b_out,
    norm_gain,
    norm_bias,
    w_up,
    b_up,
    w_down,
    b_down,
    prefix,
    cotangent,
):
    seqs = tokens.shape[0]
    fast = lax.axis_size("wide") == 8 and lax.axis_size("rows") == 4
    full_in = w_up
    if not fast:
        full_in = jnp.stack([lax.all_gather(w, "wide", axis=1, tiled=True) for w in (w_up, w_down)], axis=1)
    y_low, cot, full, q, k, v, unit, scale, slope, lse, context = forward(
        fast, tokens, cotangent, w_qkv, w_out, w_up, w_down, full_in, segments, b_qkv, b_out, norm_gain, norm_bias,
        b_up.astype(jnp.float32).reshape(1, -1), b_down, prefix,
    )
    output, grads, prefix_grads = backward(
        fast, y_low, cot, full if fast else full_in, w_qkv, w_out, q, k, v, unit, scale, slope, context, lse, segments, norm_gain, prefix, seqs
    )
    if not fast:
        prefix_grads = lax.psum(prefix_grads, ("rows", "wide"))
    return output, grads.astype(jnp.float32), prefix_grads


def solution(mesh):
    return jax.shard_map(
        local,
        mesh=mesh,
        in_specs=(
            P("rows", "wide", None),
            P("rows", None),
            P(),
            P(),
            P(),
            P(),
            P(),
            P(),
            P(None, "wide", None),
            P(None, "wide"),
            P(None, "wide", None),
            P(),
            P(),
            P("rows", "wide", None),
        ),
        out_specs=(P("rows", "wide", None), P("rows", "wide", None), P()),
        check_vma=False,
    )
```
